32 devices in a mesh: gx: 4 (over y, core), gy: 8 (over z, x).
Axes of the slice: x: 2, y: 2, z: 4, core: 2. Of those that a mesh axis runs over, the one named last changes fastest.
Arguments:
- forcing: float32 [2, 20, 64, 1024], P(None, None, 'gx', 'gy'), may hold values from -6 to 6
- viscosity: float32 [20, 64, 1024], P(None, 'gx', 'gy'), may hold values from 0.5 to 8
- spread: float32 [20, 64, 1024], P(None, 'gx', 'gy'), may hold values from 0.2 to 2
- coupling: float32 [64, 1024], P('gx', 'gy'), may hold values from -0.5 to 0.5
- friction: float32 [64, 1024], P('gx', 'gy'), may hold values from 0.05 to 5
- ice_mask: int32 [64, 1024], P('gx', 'gy'), may hold values 0 or 1
- aggregates: int32 [64, 1024], P('gx', 'gy'), may hold values from 0 to 127, as said below
Outputs:
- solution: float32 [2, 20, 64, 1024], P(None, None, 'gx', 'gy')
- residual: float32 [2, 20, 64, 1024], P(None, None, 'gx', 'gy')
The draws below stay inside these ranges and needn't reach their ends.
Inputs may be any that keep to these rules, and one draw needn't show every extreme that they name: `aggregates`: within each device block of 16 x 128 columns, every number from 0 to 127 names some columns of that block.
All inputs are finite; a program needn't handle non-finite values. No bound on the sum of `ice_mask` on one device may be relied on, other than what follows from the above.
Results may differ from the reference program's by a relative error of at most 0.0013.
Values sent between devices are 32-bit elements; how exact they have to be, the bound alone decides.
A program may use at most 128 MiB of HBM per device.

```python
import math
import jax
import jax.numpy as jnp
from jax import lax

CX = 16
CY = 128
L = 20
ITERS = 3
SWEEPS = 2
CSWEEPS = 4
AGG_DEV = 128
NX = 64
NY = 1024
N_GX = 4
N_GY = 8


def draw_aggregates(key, part):
    local_rows = lax.broadcasted_iota(jnp.int32, (NX, NY), 0) % CX
    local_cols = lax.broadcasted_iota(jnp.int32, (NX, NY), 1) % CY
    move_code = jax.random.randint(key, (NX, NY), 0, 12)
    row_step = jnp.where(move_code == 0, 4, jnp.where(move_code == 1, -4, 0))
    col_step = jnp.where(move_code == 2, 4, jnp.where(move_code == 3, -4, 0))
    centre = (local_rows % 4 == 1) & (local_cols % 4 == 1)
    row_step = jnp.where(centre, 0, row_step)
    col_step = jnp.where(centre, 0, col_step)
    moved_row = jnp.clip(local_rows + row_step, 0, CX - 1)
    moved_col = jnp.clip(local_cols + col_step, 0, CY - 1)
    return (moved_row // 4 * (CY // 4) + moved_col // 4).astype(jnp.int32)


def draw_forcing(key, part):
    rough_key = jax.random.fold_in(key, 11)
    phase_key = jax.random.fold_in(key, 12)
    amp_key = jax.random.fold_in(key, 13)
    first = (lax.broadcasted_iota(jnp.float32, (NX, NY), 0) + 0.5) / NX
    second = (lax.broadcasted_iota(jnp.float32, (NX, NY), 1) + 0.5) / NY
    phases = jax.random.uniform(phase_key, (2, 2), jnp.float32, 0.0, 2.0 * math.pi)
    amounts = jax.random.uniform(amp_key, (2,), jnp.float32, 0.5, 1.0)
    shape_first = jnp.cos(2.0 * math.pi * first + phases[0, 0]) * jnp.cos(2.0 * math.pi * second + phases[0, 1])
    shape_second = jnp.cos(2.0 * math.pi * first + phases[1, 0]) * jnp.cos(4.0 * math.pi * second + phases[1, 1])
    rough = jax.random.truncated_normal(rough_key, -5.0, 5.0, (2, L, NX, NY), jnp.float32)
    smooth = jnp.stack([amounts[0] * 0.6 * (1.0 + 0.5 * shape_first), amounts[1] * 0.4 * shape_second])
    return (rough + smooth[:, None]).astype(jnp.float32)


def place_ends(drawn, rng, low, high):
    longest = drawn.shape.index(max(drawn.shape))
    spots = []
    for shift in (0, 1):
        where = [jax.random.randint(jax.random.fold_in(rng, axis), (), 0, length) for axis, length in enumerate(drawn.shape)]
        where[longest] = (where[longest] + shift) % drawn.shape[longest]
        spots.append(tuple(where))
    return drawn.at[spots[0]].set(low).at[spots[1]].set(high)


def level_of(key, extent, pieces, low, high):
    def one(position, blocks):
        heights = jax.random.uniform(jax.random.fold_in(jax.random.fold_in(key, 6), position), (blocks,), jnp.float32, low / len(pieces), high / len(pieces))
        return jnp.repeat(jnp.exp(heights), extent[position] // blocks).reshape((-1,) + (1,) * (len(extent) - position - 1))

    factor_of = one(*pieces[0])
    for cut in pieces[1:]:
        factor_of = factor_of * one(*cut)
    return factor_of


def setup_inputs(seed: int = 0) -> dict:
    splits = jax.random.split(jax.random.key(seed), 8)
    return {
        "forcing": draw_forcing(jax.random.fold_in(splits[7], 71), 0),
        "viscosity": jnp.clip(jnp.exp(math.log(8.0) - 2.7725887 * jax.random.uniform(splits[1], (L, NX, NY), jnp.float32) ** level_of(splits[1], (L, NX, NY), ((1, 4), (2, 8)), -0.2, 0.2)), 0.5, 8.0),
        "spread": jnp.clip(jnp.exp(math.log(2.0) - 2.3025851 * jax.random.uniform(splits[2], (L, NX, NY), jnp.float32) ** level_of(splits[2], (L, NX, NY), ((1, 4), (2, 8)), -0.2, 0.2)), 0.2, 2.0),
        "coupling": jnp.clip(jax.random.uniform(splits[3], (NX, NY), jnp.float32, -0.5, 0.5) * level_of(splits[3], (NX, NY), ((0, 4), (1, 8)), -0.4, 0.0), -0.5, 0.5),
        "friction": jnp.clip(jnp.exp(math.log(5.0) - 4.6051702 * jax.random.uniform(splits[4], (NX, NY), jnp.float32) ** level_of(splits[4], (NX, NY), ((0, 4), (1, 8)), -0.2, 0.2)), 0.05, 5.0),
        "ice_mask": place_ends((jax.random.randint(splits[5], (NX, NY), 0, 32) < 31).astype(jnp.int32), jax.random.fold_in(splits[5], 1), 0, 1),
        "aggregates": draw_aggregates(jax.random.fold_in(splits[7], 71), 0),
    }


LINE_WEIGHT = 0.8
POINT_WEIGHT = 0.7
COARSE_WEIGHT = 0.7

def beside_all(padded):
    return (padded[..., 2:, 1:-1], padded[..., :-2, 1:-1], padded[..., 1:-1, 2:], padded[..., 1:-1, :-2])

def fine_coefficients(viscosity, spread, coupling, friction, ice_float, mask_padded):
    east_mask, west_mask, north_mask, south_mask = beside_all(mask_padded)
    vertical = 0.5 * (viscosity[:-1] + viscosity[1:]) * ice_float
    face_total = jnp.pad(vertical, ((0, 1), (0, 0), (0, 0))) + jnp.pad(vertical, ((1, 0), (0, 0), (0, 0)))
    bottom = jnp.pad(friction[None], ((0, viscosity.shape[0] - 1), (0, 0), (0, 0)))
    diagonal = ice_float * (face_total + 4.0 * spread + bottom) + (1.0 - ice_float)
    owned_spread = spread * ice_float
    return (diagonal, vertical, owned_spread * east_mask, owned_spread * west_mask, owned_spread * north_mask, owned_spread * south_mask, bottom * coupling * ice_float)

def group_layers(level_coefs, group_size):
    diagonal, vertical, to_east, to_west, to_north, to_south, crossed = level_coefs
    group_count = diagonal.shape[0] // group_size

    def fold_layers(values):
        return values.reshape((group_count, group_size) + values.shape[1:]).sum(axis=1)
    padded = jnp.concatenate([vertical, jnp.zeros_like(diagonal[:1])], axis=0)
    blocks = padded.reshape((group_count, group_size) + padded.shape[1:])
    inner_sum = blocks[:, :group_size - 1].sum(axis=1)
    return (fold_layers(diagonal) - 2.0 * inner_sum, blocks[:-1, group_size - 1], fold_layers(to_east), fold_layers(to_west), fold_layers(to_north), fold_layers(to_south), fold_layers(crossed))

def apply_stencil(level_coefs, grid_field, padded):
    diagonal, vertical, to_east, to_west, to_north, to_south, crossed = level_coefs
    east_value, west_value, north_value, south_value = beside_all(padded)
    result = diagonal * grid_field + crossed * grid_field[::-1] - (to_east * east_value + to_west * west_value + to_north * north_value + to_south * south_value)
    if vertical.shape[0] > 0:
        upward = vertical * grid_field[:, 1:]
        downward = vertical * grid_field[:, :-1]
        result = result - (jnp.pad(upward, ((0, 0), (0, 1), (0, 0), (0, 0))) + jnp.pad(downward, ((0, 0), (1, 0), (0, 0), (0, 0))))
    return result

def line_factor(level_coefs):
    diagonal, vertical = (level_coefs[0], level_coefs[1])
    inverse = [1.0 / diagonal[0]]
    upper = []
    for layer_at in range(1, diagonal.shape[0]):
        ratio_value = -vertical[layer_at - 1] * inverse[-1]
        upper.append(ratio_value)
        inverse.append(1.0 / (diagonal[layer_at] + vertical[layer_at - 1] * ratio_value))
    return (inverse, upper, vertical)

def line_solve(factor, right_side):
    inverse, upper, vertical = factor
    layers = len(inverse)
    forward = [right_side[:, 0] * inverse[0]]
    for layer_at in range(1, layers):
        forward.append((right_side[:, layer_at] + vertical[layer_at - 1] * forward[-1]) * inverse[layer_at])
    backward = [forward[-1]]
    for layer_at in range(layers - 2, -1, -1):
        backward.append(forward[layer_at] - upper[layer_at] * backward[-1])
    return jnp.stack(backward[::-1], axis=1)

def group_sum(grid_field, group_size):
    return grid_field.reshape((2, grid_field.shape[1] // group_size, group_size) + grid_field.shape[2:]).sum(axis=2)

def expand_layers(grid_field, group_size):
    return jnp.repeat(grid_field, group_size, axis=1)

def point_diagonal(column_coefs, group_ids, group_count):
    ids_padded = jnp.pad(group_ids, 1, constant_values=-1)
    east_id, west_id, north_id, south_id = beside_all(ids_padded)
    inner_sum = jnp.where(east_id == group_ids, column_coefs[2][0], 0.0) + jnp.where(west_id == group_ids, column_coefs[3][0], 0.0) + jnp.where(north_id == group_ids, column_coefs[4][0], 0.0) + jnp.where(south_id == group_ids, column_coefs[5][0], 0.0)
    return jax.ops.segment_sum((column_coefs[0][0] - inner_sum).reshape(-1), group_ids.reshape(-1), num_segments=group_count)

def coarse_coefficients(column_coefs, blocks_first, blocks_second):
    diagonal, vertical, to_east, to_west, to_north, to_south, crossed = column_coefs

    def split_block(values):
        plane = values[0]
        return plane.reshape(blocks_first, plane.shape[0] // blocks_first, blocks_second, plane.shape[1] // blocks_second)
    east_block = split_block(to_east)
    west_block = split_block(to_west)
    north_block = split_block(to_north)
    south_block = split_block(to_south)
    inner_sum = east_block[:, :-1].sum(axis=(1, 3)) + west_block[:, 1:].sum(axis=(1, 3)) + north_block[:, :, :, :-1].sum(axis=(1, 3)) + south_block[:, :, :, 1:].sum(axis=(1, 3))
    return (split_block(diagonal).sum(axis=(1, 3)) - inner_sum, split_block(crossed).sum(axis=(1, 3)), east_block[:, -1].sum(axis=2), west_block[:, 0].sum(axis=2), north_block[:, :, :, -1].sum(axis=1), south_block[:, :, :, 0].sum(axis=1))

def coarse_apply(block_table, grid_field, padded):
    diagonal, crossed, to_east, to_west, to_north, to_south = block_table
    east_value, west_value, north_value, south_value = beside_all(padded)
    return diagonal * grid_field + crossed * grid_field[::-1] - (to_east * east_value + to_west * west_value + to_north * north_value + to_south * south_value)

def coarse_jacobi(block_table, right_side, widen_rim):
    answer = COARSE_WEIGHT * right_side / block_table[0]
    for sweep_at in range(CSWEEPS - 1):
        answer = answer + COARSE_WEIGHT * (right_side - coarse_apply(block_table, answer, widen_rim(answer))) / block_table[0]
    return answer

def least_squares(columns, initial_norm):
    steps_count = len(columns)
    matrix_rows = [[columns[column_at][row_at] for column_at in range(steps_count)] for row_at in range(steps_count + 1)]
    target = [initial_norm] + [jnp.zeros_like(initial_norm) for row_at in range(steps_count)]
    for pivot_at in range(steps_count):
        top_value = matrix_rows[pivot_at][pivot_at]
        low_value = matrix_rows[pivot_at + 1][pivot_at]
        radius = jnp.sqrt(top_value * top_value + low_value * low_value)
        cosine = top_value / radius
        sine_value = low_value / radius
        for column_at in range(pivot_at, steps_count):
            upper_entry = matrix_rows[pivot_at][column_at]
            lower_entry = matrix_rows[pivot_at + 1][column_at]
            matrix_rows[pivot_at][column_at] = cosine * upper_entry + sine_value * lower_entry
            matrix_rows[pivot_at + 1][column_at] = cosine * lower_entry - sine_value * upper_entry
        upper_entry = target[pivot_at]
        lower_entry = target[pivot_at + 1]
        target[pivot_at] = cosine * upper_entry + sine_value * lower_entry
        target[pivot_at + 1] = cosine * lower_entry - sine_value * upper_entry
    weights = [None] * steps_count
    for pivot_at in reversed(range(steps_count)):
        partial_sum = target[pivot_at]
        for column_at in range(pivot_at + 1, steps_count):
            partial_sum = partial_sum - matrix_rows[pivot_at][column_at] * weights[column_at]
        weights[pivot_at] = partial_sum / matrix_rows[pivot_at][pivot_at]
    return weights

def reference(forcing, viscosity, spread, coupling, friction, ice_mask, aggregates):
    ice_float = ice_mask.astype(jnp.float32)
    fine_coefs = fine_coefficients(viscosity, spread, coupling, friction, ice_float, jnp.pad(ice_float, 1))
    middle = group_layers(fine_coefs, 2)
    column = group_layers(middle, L // 2)
    stencils = [fine_coefs, middle, column]
    factors = [line_factor(level_coefs) for level_coefs in stencils]
    device_rows = lax.broadcasted_iota(jnp.int32, (NX, NY), 0) // CX
    device_cols = lax.broadcasted_iota(jnp.int32, (NX, NY), 1) // CY
    group_ids = (aggregates + (device_rows * N_GY + device_cols) * AGG_DEV).astype(jnp.int32)
    total_groups = N_GX * N_GY * AGG_DEV
    ids_flat = group_ids.reshape(-1)
    point_diag = point_diagonal(column, group_ids, total_groups)
    block_table = coarse_coefficients(column, N_GX, N_GY)

    def apply_level(level_number, grid_field):
        padded = jnp.pad(grid_field, ((0, 0), (0, 0), (1, 1), (1, 1)))
        return apply_stencil(stencils[level_number], grid_field, padded)

    def restrict_points(grid_field):
        flattened = grid_field.reshape(2, -1)
        return jnp.stack([jax.ops.segment_sum(flattened[0], ids_flat, num_segments=total_groups), jax.ops.segment_sum(flattened[1], ids_flat, num_segments=total_groups)])

    def prolong_points(values):
        return values[:, ids_flat].reshape(2, 1, NX, NY)

    def point_apply(values):
        return restrict_points(apply_level(2, prolong_points(values)))

    def local_widen(values):
        return jnp.pad(values, ((0, 0), (1, 1), (1, 1)))

    def coarse_correction(values):
        coarse_rhs = values.reshape(2, N_GX, N_GY, AGG_DEV).sum(axis=3)
        answer = coarse_jacobi(block_table, coarse_rhs, local_widen)
        return jnp.repeat(answer.reshape(2, -1), AGG_DEV, axis=1)

    def point_cycle(right_side):
        answer = POINT_WEIGHT * right_side / point_diag
        for sweep_at in range(SWEEPS - 1):
            answer = answer + POINT_WEIGHT * (right_side - point_apply(answer)) / point_diag
        answer = answer + coarse_correction(right_side - point_apply(answer))
        for sweep_at in range(SWEEPS):
            answer = answer + POINT_WEIGHT * (right_side - point_apply(answer)) / point_diag
        return answer

    def line_cycle(level_number, right_side):
        factor = factors[level_number]
        answer = LINE_WEIGHT * line_solve(factor, right_side)
        for sweep_at in range(SWEEPS - 1):
            answer = answer + LINE_WEIGHT * line_solve(factor, right_side - apply_level(level_number, answer))
        leftover = right_side - apply_level(level_number, answer)
        if level_number == 0:
            answer = answer + expand_layers(line_cycle(1, group_sum(leftover, 2)), 2)
        elif level_number == 1:
            depth_count = leftover.shape[1]
            answer = answer + expand_layers(line_cycle(2, group_sum(leftover, depth_count)), depth_count)
        else:
            answer = answer + prolong_points(point_cycle(restrict_points(leftover)))
        for sweep_at in range(SWEEPS):
            answer = answer + LINE_WEIGHT * line_solve(factor, right_side - apply_level(level_number, answer))
        return answer
    initial_norm = jnp.sqrt(jnp.sum(forcing * forcing))
    basis = [forcing / initial_norm]
    stored = []
    columns = []
    for step_at in range(ITERS):
        search = line_cycle(0, basis[step_at])
        stored.append(search)
        image = apply_level(0, search)
        projected = [jnp.sum(vector * image) for vector in basis]
        for index_at in range(len(basis)):
            image = image - projected[index_at] * basis[index_at]
        height = jnp.sqrt(jnp.sum(image * image))
        columns.append(projected + [height] + [jnp.zeros_like(height) for row_at in range(ITERS - 1 - step_at)])
        if step_at + 1 < ITERS:
            basis.append(image / height)
    weights = least_squares(columns, initial_norm)
    solution = weights[0] * stored[0]
    for index_at in range(1, ITERS):
        solution = solution + weights[index_at] * stored[index_at]
    residual = forcing - apply_level(0, solution)
    return (solution, residual)
```

```python
import jax
import jax.numpy as jnp
from jax import lax
from jax.experimental import pallas as pl
from jax.experimental.pallas import tpu as pltpu
from jax.sharding import PartitionSpec as P

ITERS = 3
CSWEEPS = 4
LINE_WEIGHT = 0.8
POINT_WEIGHT = 0.7
COARSE_WEIGHT = 0.7
MESH = pl.DeviceIdType.MESH
F32 = jnp.float32
BF16 = jnp.bfloat16
TOP = 8
HALO = 8
SLOT = 2 * HALO
STEPS = ((1, 0), (-1, 0), (0, 1), (0, -1), (1, 1), (1, -1), (-1, 1), (-1, -1))
BACK = (1, 0, 3, 2, 7, 6, 5, 4)


def split(x):
    high = x.astype(BF16)
    return high, (x - high.astype(F32)).astype(BF16)


def dot(a, b, ca, cb):
    return lax.dot_general(a, b, (((ca,), (cb,)), ((), ())), preferred_element_type=F32)


def total(x):
    return jnp.sum(jnp.sum(x, axis=1, keepdims=True), axis=0, keepdims=True)


def turn(x, shift):
    flat = x.reshape(-1, x.shape[-1])
    return pltpu.roll(flat, shift % x.shape[-1], 1).reshape(x.shape)


def kernel(nx, ny, layers, cx, cy, forcing, viscosity, spread, coupling, friction, mask, aggs,
           solution, residual, *scratch):
    count = nx * ny
    gx = lax.axis_index("gx")
    gy = lax.axis_index("gy")
    me = gx * ny + gy
    (levels, (basis, stored, visc, spr, misc), (hit, big_hi, big_lo, point_diag, point_cross),
     (x_out, x_in, x_send, x_recv), gathers, first_swap, right_swap, side_swap, point_swap,
     (mid_rows, col_rows)) = scratch
    tall = cx + 2 * HALO
    own = pl.ds(HALO, cx)
    slots = cy // SLOT
    lane = lax.broadcasted_iota(jnp.int32, (cx, cy), 1)
    row = lax.broadcasted_iota(jnp.int32, (cx, cy), 0)
    first_lane, last_lane = lane == 0, lane == cy - 1
    long_lane = lax.broadcasted_iota(jnp.int32, (tall, cy), 1)
    kept_lane = (long_lane < HALO) | (long_lane >= cy - HALO)

    exists, peers = [], []
    for dx, dy in STEPS:
        ok = []
        if dx:
            ok.append(gx < nx - 1 if dx > 0 else gx > 0)
        if dy:
            ok.append(gy < ny - 1 if dy > 0 else gy > 0)
        exists.append(ok[0] if len(ok) == 1 else jnp.logical_and(ok[0], ok[1]))
        peers.append((gx + dx, gy + dy))

    class Swap:
        def __init__(self, pieces, send, recv):
            self.pieces = pieces
            self.copies = [[pltpu.make_async_remote_copy(
                src_ref=src, dst_ref=dst, send_sem=send.at[d, i], recv_sem=recv.at[BACK[d], i],
                device_id=peers[d], device_id_type=MESH) for i, (src, dst) in enumerate(pieces[d])]
                for d in range(len(pieces))]

        def start(self, which=None):
            for d in range(len(self.copies)) if which is None else which:
                @pl.when(exists[d])
                def _():
                    for copy in self.copies[d]:
                        copy.start()

        def wait(self):
            for d in range(len(self.copies)):
                @pl.when(exists[d])
                def _():
                    for copy in self.copies[d]:
                        copy.wait_send()
                    for copy in self.copies[BACK[d]]:
                        copy.wait_recv()

        def clear(self):
            for d in range(len(self.copies)):
                @pl.when(jnp.logical_not(exists[d]))
                def _():
                    for _, ref in self.pieces[BACK[d]]:
                        ref[...] = jnp.zeros(ref.shape, F32)

    def edges(rows, packed, landed):
        low, high = pl.ds(0, HALO), pl.ds(cx - HALO, HALO)
        top, bottom = pl.ds(0, HALO), pl.ds(HALO + cx, HALO)
        return [
            [(src(cx - HALO), dst(0)) for src, dst in rows],
            [(src(0), dst(1)) for src, dst in rows],
            [(packed, landed.at[0, :, own])],
            [(packed, landed.at[1, :, own])],
            [(packed.at[:, high], landed.at[0, :, top])],
            [(packed.at[:, high], landed.at[1, :, top])],
            [(packed.at[:, low], landed.at[0, :, bottom])],
            [(packed.at[:, low], landed.at[1, :, bottom])],
        ]

    def ends(e):
        return pl.ds(0, HALO) if e == 0 else pl.ds(HALO + cx, HALO)

    class Packer:
        def __init__(self, out):
            self.out = out
            self.at = 0
            self.tile = None

        def add(self, value):
            s, m = divmod(self.at, slots)
            moved = pltpu.roll(value, (SLOT * m + HALO) % cy, 1)
            self.tile = moved if m == 0 else jnp.where(lane // SLOT == m, moved, self.tile)
            self.at += 1
            if m == slots - 1:
                self.flush(s)

        def flush(self, s):
            self.out[s] = self.tile
            self.tile = None

        def finish(self):
            if self.tile is not None:
                self.flush((self.at - 1) // slots)

    def unpack(landed, puts):
        south = long_lane % SLOT < HALO
        comb = None
        for i, put in enumerate(puts):
            s, m = divmod(i, slots)
            if m == 0:
                comb = jnp.where(south, landed[0, s], landed[1, s])
            put(jnp.where(kept_lane, pltpu.roll(comb, (cy - SLOT * m - HALO) % cy, 1), 0.0))

    chunks = ((0, tall // 2), (tall // 2, tall // 2))
    both = (0, 1)

    class Level:
        def __init__(self, depth, refs):
            self.depth = depth
            (self.field, self.diag, self.vert, self.side, self.cross, self.inverse, self.upper,
             self.right, self.forward) = refs

        def at(self, p, k, t, c0, cn, shift=0):
            return self.field[p, k, t, :, pl.ds(TOP + c0 + shift, cn), :]

        def sideways(self, p, k, c0, cn, tiles):
            here = pl.ds(c0, cn)
            wide = lax.broadcasted_iota(jnp.int32, (2, cn, cy), 2)
            value = [self.at(p, k, t, c0, cn) for t in both]
            up = [turn(v, cy - 1) for v in value]
            down = [turn(v, 1) for v in value]
            outs = []
            for t in tiles:
                north = jnp.where(wide == cy - 1, up[1 - t], up[t])
                south = jnp.where(wide == 0, down[1 - t], down[t])
                out = (self.side[0, k, t, here][None] * self.at(p, k, t, c0, cn, 1)
                       + self.side[1, k, t, here][None] * self.at(p, k, t, c0, cn, -1)
                       + self.side[2, k, t, here][None] * north + self.side[3, k, t, here][None] * south)
                if k == 0:
                    crossed = self.cross[t, here]
                    out = out - jnp.stack([crossed * value[t][1], crossed * value[t][0]])
                outs.append(out)
            return value, outs

        def leftover(self, p, right, emit, tiles=both, spans=chunks):
            for c0, cn in spans:
                here = pl.ds(c0, cn)
                for k in range(self.depth):
                    value, outs = self.sideways(p, k, c0, cn, tiles)
                    for i, t in enumerate(tiles):
                        out = outs[i] - self.diag[k, t, here][None] * value[t]
                        if k + 1 < self.depth:
                            out = out + self.vert[k, t, here][None] * self.at(p, k + 1, t, c0, cn)
                        if k > 0:
                            out = out + self.vert[k - 1, t, here][None] * self.at(p, k - 1, t, c0, cn)
                        emit(k, t, c0, cn, right(k, t, here) + out)

        def solve(self, source, old, p):
            for c0, cn in chunks:
                here = pl.ds(c0, cn)
                last = [None, None]
                for k in range(self.depth):
                    values = source(k, c0, cn)
                    for t in both:
                        value = values[t]
                        if k > 0:
                            value = value + self.vert[k - 1, t, here][None] * last[t]
                        last[t] = value * self.inverse[k, t, here][None]
                        self.forward[k, t, :, here] = last[t]
                for k in reversed(range(self.depth)):
                    for t in both:
                        if k + 1 < self.depth:
                            last[t] = self.forward[k, t, :, here] - self.upper[k, t, here][None] * last[t]
                        value = LINE_WEIGHT * last[t]
                        if old is not None:
                            value = value + (1.0 - LINE_WEIGHT) * self.at(old, k, t, c0, cn)
                        self.field[p, k, t, :, pl.ds(TOP + c0, cn), :] = value

        def first(self, right):
            self.solve(lambda k, c0, cn: [right(k, t, pl.ds(c0, cn)) for t in both], None, 0)

        def sweep(self, p, right):
            def source(k, c0, cn):
                outs = self.sideways(p, k, c0, cn, both)[1]
                return [right(k, t, pl.ds(c0, cn)) + outs[t] for t in both]
            self.solve(source, p, 1 - p)

        def factor(self):
            inverse = 1.0 / self.diag[0]
            self.inverse[0] = inverse
            for k in range(1, self.depth):
                ratio = -self.vert[k - 1] * inverse
                self.upper[k - 1] = ratio
                inverse = 1.0 / (self.diag[k] + self.vert[k - 1] * ratio)
                self.inverse[k] = inverse

        def after(self, right):
            self.sweep(0, right)
            self.sweep(1, right)

    half = layers // 2
    fine, middle, column = (Level(n, refs) for n, refs in zip((layers, half, 1), levels))
    for level in (fine, middle, column):
        for p in range(2):
            for k in range(level.depth):
                for t in both:
                    level.field[p, k, t, :, pl.ds(0, TOP), :] = jnp.zeros((2, TOP, cy), F32)
                    level.field[p, k, t, :, pl.ds(TOP + tall, TOP), :] = jnp.zeros((2, TOP, cy), F32)

    def rows_of(ref, at):
        return lambda start: ref.at[at + (pl.ds(start, HALO),)]

    any_k = slice(None)

    (first_pack, first_land, first_send, first_recv) = first_swap
    swap0 = Swap(edges([
        (lambda lo: forcing.at[:, :, pl.ds(lo, HALO)], lambda e: basis.at[0, :, :, 0, ends(e)]),
        (lambda lo: viscosity.at[:, pl.ds(lo, HALO)], lambda e: visc.at[:, 0, ends(e)]),
        (lambda lo: spread.at[:, pl.ds(lo, HALO)], lambda e: spr.at[:, 0, ends(e)]),
        (lambda lo: misc.at[:, 0, pl.ds(HALO + lo, HALO)], lambda e: misc.at[:, 0, ends(e)]),
    ], first_pack, first_land), first_send, first_recv)
    (right_pack, right_land, right_send, right_recv) = right_swap

    def swap_right(j):
        return Swap(edges([(lambda lo: basis.at[j, :, :, 0, pl.ds(HALO + lo, HALO)],
                            lambda e: basis.at[j, :, :, 0, ends(e)])],
                          right_pack, right_land), right_send, right_recv)

    (side_pack, side_land, side_send, side_recv) = side_swap
    swap_side = Swap(edges([
        (lambda lo: middle.field.at[1, :, 0, :, pl.ds(TOP + HALO + lo, HALO)], lambda e: mid_rows.at[e]),
        (lambda lo: column.field.at[1, 0, 0, :, pl.ds(TOP + HALO + lo, HALO)], lambda e: col_rows.at[e, 0]),
        (lambda lo: column.right.at[0, 0, :, pl.ds(HALO + lo, HALO)], lambda e: col_rows.at[e, 1]),
    ], side_pack, side_land), side_send, side_recv)
    (far_out, far_in, far_send, far_recv) = point_swap
    swap_far = Swap([[(far_out, far_in.at[d])] for d in range(8)], far_send, far_recv)

    def near_swap(p, q):
        return Swap([[(x_out.at[p], x_in.at[q, d])] for d in range(4)], x_send.at[p], x_recv.at[q])

    misc[0, 0, own] = mask[...].astype(F32)
    misc[1, 0, own] = aggs[...].astype(F32)
    misc[2, 0, own] = friction[...]
    misc[3, 0, own] = coupling[...]
    swap0.start((0, 1))
    packer = Packer(first_pack)
    for i in range(4):
        packer.add(misc[i, 0, own])
    for k in range(layers):
        packer.add(viscosity[k])
        packer.add(spread[k])
    for k in range(layers):
        for v in range(2):
            packer.add(forcing[v, k])
    packer.finish()
    swap0.start(range(2, 8))
    for j in range(1, ITERS):
        swap_right(j).clear()
    swap0.clear()
    swap_side.clear()
    swap_far.clear()
    for q in range(2):
        near_swap(0, q).clear()
    for k in range(layers):
        visc[k, 0, own] = viscosity[k]
        spr[k, 0, own] = spread[k]
        basis[0, :, k, 0, own] = forcing[:, k]

    def gather(which, slot=0):
        out, into, send, recv = gathers[which]
        into, recv = into.at[slot], recv.at[slot]
        rest = into.at[pl.ds(0, count - 1)]

        def start():
            def step(i, carry):
                target = lax.rem(me + i, count)
                pltpu.make_async_remote_copy(
                    src_ref=out, dst_ref=into.at[me], send_sem=send, recv_sem=recv,
                    device_id=(target // ny, lax.rem(target, ny)), device_id_type=MESH).start()
                return carry

            lax.fori_loop(1, count, step, 0)
            into[me] = out[...]

        def wait():
            pltpu.make_async_copy(rest, rest, recv).wait()
            pltpu.make_async_copy(rest, rest, send).wait()

        return start, wait

    wide = lax.broadcasted_iota(jnp.int32, (1, cy), 1)

    def reduce_all(parts):
        line = jnp.zeros((1, cy), F32)
        for i, part in enumerate(parts):
            line = jnp.where(wide == i, part, line)
        gathers[1][0][...] = line
        start, wait = gather(1)
        start()
        wait()
        return jnp.sum(gathers[1][1][0, :, 0, :], axis=0, keepdims=True)

    def pick(line, i):
        return jnp.sum(jnp.where(wide == i, line, 0.0), axis=1, keepdims=True)

    def put_to(ref, *at):
        def put(value):
            ref[at] = value
        return put

    swap0.wait()
    puts = [put_to(misc, i, 1) for i in range(4)]
    for k in range(layers):
        puts += [put_to(visc, k, 1), put_to(spr, k, 1)]
    for k in range(layers):
        puts += [put_to(basis, 0, v, k, 1) for v in range(2)]
    unpack(first_land, puts)

    ids_all = [misc[1, t].astype(jnp.int32) for t in both]
    ids = misc[1, 0, own].astype(jnp.int32)
    ice = [misc[0, t] for t in both]
    for t in both:
        column.field[1, 0, t, 0, pl.ds(TOP, tall), :] = ice[t]
    around = []
    ups = [turn(x, cy - 1) for x in ice]
    downs = [turn(x, 1) for x in ice]
    for t in both:
        around.append((column.field[1, 0, t, 0, pl.ds(TOP + 1, tall), :],
                       column.field[1, 0, t, 0, pl.ds(TOP - 1, tall), :],
                       jnp.where(long_lane == cy - 1, ups[1 - t], ups[t]),
                       jnp.where(long_lane == 0, downs[1 - t], downs[t])))
    for k in range(layers):
        for t in both:
            owned = spr[k, t]
            faces = 4.0 * owned
            if k + 1 < layers:
                face = 0.5 * (visc[k, t] + visc[k + 1, t]) * ice[t]
                fine.vert[k, t] = face
                faces = faces + face
            if k > 0:
                faces = faces + fine.vert[k - 1, t]
            if k == 0:
                faces = faces + misc[2, t]
            fine.diag[k, t] = ice[t] * faces + (1.0 - ice[t])
            owned = owned * ice[t]
            for d in range(4):
                fine.side[d, k, t] = owned * around[t][d]
    for t in both:
        fine.cross[t] = misc[2, t] * misc[3, t] * ice[t]
    for finer, coarser in ((fine, middle), (middle, column)):
        size = finer.depth // coarser.depth
        for k in range(coarser.depth):
            group = range(k * size, (k + 1) * size)
            diag = sum(finer.diag[j] for j in group)
            inner_faces = sum(finer.vert[j] for j in list(group)[:-1])
            coarser.diag[k] = diag - 2.0 * inner_faces
            if k + 1 < coarser.depth:
                coarser.vert[k] = finer.vert[group[-1]]
            for d in range(4):
                coarser.side[d, k] = sum(finer.side[d, j] for j in group)
        coarser.cross[...] = finer.cross[...]

    side2 = [column.side[d, 0, 0, own] for d in range(4)]
    diag2, cross2 = column.diag[0, 0, own], column.cross[0, own]
    inner = (diag2 - jnp.where(row < cx - 1, side2[0], 0.0) - jnp.where(row > 0, side2[1], 0.0)
             - jnp.where(lane < cy - 1, side2[2], 0.0) - jnp.where(lane > 0, side2[3], 0.0))
    entries = (inner, cross2, jnp.where(row == cx - 1, side2[0], 0.0), jnp.where(row == 0, side2[1], 0.0),
               jnp.where(last_lane, side2[2], 0.0), jnp.where(first_lane, side2[3], 0.0))
    eight = lax.broadcasted_iota(jnp.int32, (8, cy), 0)
    tile = jnp.zeros((8, cy), F32)
    for i, entry in enumerate(entries):
        tile = jnp.where(eight == i, total(entry), tile)
    gathers[2][0][...] = tile
    tables_start, tables_wait = gather(2)
    tables_start()
    for level in (fine, middle, column):
        level.factor()

    down = lax.broadcasted_iota(jnp.int32, (cy, cy), 0)
    across = lax.broadcasted_iota(jnp.int32, (cy, cy), 1)
    for r in range(cx):
        hit[r] = jnp.where(ids[r:r + 1, :] == down, 1.0, 0.0).astype(BF16)
    near = jnp.zeros((cy, cy), F32)
    for r in range(cx):
        here = hit[r].astype(F32)
        term = diag2[r:r + 1, :] * here
        if r + 1 < cx:
            term = term - side2[0][r:r + 1, :] * hit[r + 1].astype(F32)
        if r > 0:
            term = term - side2[1][r:r + 1, :] * hit[r - 1].astype(F32)
        term = term - jnp.where(across < cy - 1, side2[2][r:r + 1, :], 0.0) * pltpu.roll(here, cy - 1, 1)
        term = term - jnp.where(across > 0, side2[3][r:r + 1, :], 0.0) * pltpu.roll(here, 1, 1)
        high, low = split(term)
        near = near + dot(high, hit[r], 1, 1) + dot(low, hit[r], 1, 1)
    point_diag[...] = jnp.sum(jnp.where(down == across, near, 0.0), axis=0, keepdims=True)
    tables = [near]
    for d, r, e in ((0, cx - 1, HALO + cx), (1, 0, HALO - 1)):
        other = ids_all[0][e:e + 1, :]
        term = jnp.where(other == down, side2[d][r:r + 1, :], 0.0)
        high, low = split(term)
        tables.append(-(dot(high, hit[r], 1, 1) + dot(low, hit[r], 1, 1)))
    for d, q, e in ((2, cy - 1, 0), (3, 0, cy - 1)):
        other = ids_all[1][HALO:HALO + cx, e:e + 1]
        term = jnp.where(other == lane, side2[d][:, q:q + 1], 0.0)
        here = jnp.where(ids[:, q:q + 1] == lane, 1.0, 0.0)
        high, low = split(term)
        here = here.astype(BF16)
        tables.append(-(dot(high, here, 0, 0) + dot(low, here, 0, 0)))
    for i, table in enumerate(tables):
        high, low = split(table)
        big_hi[i] = high
        big_lo[i] = low

    tall4 = lax.broadcasted_iota(jnp.int32, (4 * cx, cy), 0) % cx

    def restrict_points(first, second):
        h0, l0 = split(first)
        h1, l1 = split(second)
        left = jnp.concatenate([h0, h1, l0, l1], axis=0)
        out = jnp.zeros((4 * cx, cy), F32)
        for r in range(cx):
            out = jnp.where(tall4 == r, dot(left, hit[r], 1, 1), out)
        parts = [jnp.sum(out[i * cx:(i + 1) * cx] + out[(i + 2) * cx:(i + 3) * cx], axis=0, keepdims=True)
                 for i in range(2)]
        return jnp.concatenate(parts, axis=0)

    point_cross[...] = restrict_points(cross2, cross2)
    block_row = lax.broadcasted_iota(jnp.int32, (count, cy), 0)

    def coarse_correction(j, left):
        sums = jnp.sum(left, axis=1, keepdims=True)
        gathers[0][0][...] = jnp.where(wide % 2 == 0, sums[0:1], sums[1:2])
        slot = lax.rem(j, 2)
        start, wait = gather(0, slot)
        start()
        pl.when(j == 0)(tables_wait)
        wait()
        right = gathers[0][1][slot, :, 0, :]
        diag, crossed, east, west, north, south = (gathers[2][1][0, :, i, :] for i in range(6))
        answer = COARSE_WEIGHT * right / diag
        for _ in range(CSWEEPS - 1):
            applied = diag * answer + crossed * pltpu.roll(answer, 1, 1) - (
                east * pltpu.roll(answer, count - ny, 0) + west * pltpu.roll(answer, ny, 0)
                + north * pltpu.roll(answer, count - 1, 0) + south * pltpu.roll(answer, 1, 0))
            answer = answer + COARSE_WEIGHT * (right - applied) / diag
        found = []
        for at in (me, me + ny, me - ny, me + 1, me - 1):
            line = jnp.sum(jnp.where(block_row == at, answer, 0.0), axis=0, keepdims=True)
            found.append(jnp.concatenate([line[:, 0:1], line[:, 1:2]], axis=0))
        return found

    def point_apply(xs):
        out = point_cross[...] * jnp.concatenate([xs[0][1:2], xs[0][0:1]], axis=0)
        for i, x in enumerate(xs):
            high, low = split(x)
            out = out + dot(high, big_hi[i], 1, 0) + dot(low, big_hi[i], 1, 0) + dot(high, big_lo[i], 1, 0)
        return out

    def point_cycle(j, right):
        def begin(p, x):
            x_out[p] = x
            q = lax.rem(p + j, 2)
            swap = near_swap(p, q)
            swap.start()

            def end():
                swap.wait()
                return [x] + [x_in[q, BACK[d]] for d in range(4)]
            return end

        scale = POINT_WEIGHT / point_diag[...]
        x = right * scale
        end = begin(0, x)
        packer = Packer(side_pack)
        for v in range(2):
            packer.add(column.field[1, 0, 0, v, pl.ds(TOP + HALO, cx), :])
            packer.add(column.right[0, 0, v, own])
        for k in range(half):
            for v in range(2):
                packer.add(middle.field[1, k, 0, v, pl.ds(TOP + HALO, cx), :])
        packer.finish()
        swap_side.start()
        x = x + (right - point_apply(end())) * scale
        xs = begin(1, x)()
        found = coarse_correction(j, right - point_apply(xs))
        xs = [x + y for x, y in zip(xs, found)]
        x = xs[0] + (right - point_apply(xs)) * scale
        return x + (right - point_apply(begin(0, x)())) * scale

    def spread_points(x):
        far_out[...] = x
        swap_far.start()
        swap_side.wait()
        swap_far.wait()
        parts = [[], []]
        zones = ((pl.ds(0, HALO), 1, 6, 7), (own, None, 2, 3), (pl.ds(HALO + cx, HALO), 0, 4, 5))
        short = {n: lax.broadcasted_iota(jnp.int32, (n, cy), 1) < cy // 2 for n in (HALO, cx)}

        def take(src, v, index):
            values = x if src is None else far_in[BACK[src]]
            return jnp.take_along_axis(jnp.broadcast_to(values[v:v + 1], index.shape), index, axis=1,
                                       mode="promise_in_bounds")

        for rows, straight, right, left in zones:
            index = [misc[1, t, rows].astype(jnp.int32) for t in both]
            parts[0].append(jnp.stack([take(straight, v, index[0]) for v in range(2)]))
            lanes = short[index[1].shape[0]]
            parts[1].append(jnp.stack([jnp.where(lanes, take(right, v, index[1]), take(left, v, index[1]))
                                       for v in range(2)]))
        return [jnp.concatenate(p, axis=1) for p in parts]

    def iteration(j, carry):
        def right0(k, t, here):
            return basis[j, :, k, t, here]

        def right1(k, t, here):
            return middle.right[k, t, :, here]

        def right2(k, t, here):
            return column.right[k, t, :, here]

        def collect(coarser, size):
            held = {}

            def emit(k, t, c0, cn, value):
                held[t] = held[t] + value if k % size else value
                if k % size == size - 1:
                    coarser.right[k // size, t, :, pl.ds(c0, cn)] = held[t]
            return emit

        fine.first(right0)
        fine.sweep(0, right0)
        fine.leftover(1, right0, collect(middle, 2))
        middle.first(right1)
        middle.sweep(0, right1)
        middle.leftover(1, right1, collect(column, half))
        column.first(right2)
        column.sweep(0, right2)
        kept = []
        column.leftover(1, right2, lambda k, t, c0, cn, value: kept.append(value), (0,), ((HALO, cx),))
        found = spread_points(point_cycle(j, restrict_points(kept[0][0], kept[0][1])))

        whole = pl.ds(TOP, tall)
        inside = pl.ds(TOP + HALO, cx)
        landed = []
        unpack(side_land, [landed.append] * (4 + 2 * half))
        column.field[0, 0, 0, :, whole] = found[0] + jnp.concatenate(
            [col_rows[0, 0], column.field[1, 0, 0, :, inside], col_rows[1, 0]], axis=1)
        column.field[0, 0, 1, :, whole] = found[1] + jnp.stack([landed[0], landed[2]])
        for e in range(2):
            column.right[0, 0, :, ends(e)] = col_rows[e, 1]
        column.right[0, 1] = jnp.stack([landed[1], landed[3]])
        column.after(right2)
        for k in range(half):
            middle.field[0, k, 0, :, whole] = column.field[0, 0, 0, :, whole] + jnp.concatenate(
                [mid_rows[0, k], middle.field[1, k, 0, :, inside], mid_rows[1, k]], axis=1)
            middle.field[0, k, 1, :, whole] = column.field[0, 0, 1, :, whole] + jnp.stack(
                [landed[4 + 2 * k], landed[5 + 2 * k]])
        middle.after(right1)
        for k in range(layers):
            for t in both:
                fine.field[0, k, t, :, whole] = (fine.field[1, k, t, :, whole]
                                                 + middle.field[0, k // 2, t, :, whole])
        fine.after(right0)

        packer = Packer(right_pack)

        def emit(k, t, c0, cn, value):
            basis[j + 1, :, k, 0, own] = value
            stored[j, :, k] = fine.field[0, k, 0, :, inside]
            for v in range(2):
                packer.add(value[v])

        fine.leftover(0, right0, emit, (0,), ((HALO, cx),))
        packer.finish()

        @pl.when(j < ITERS - 1)
        def _():
            swap = swap_right(j + 1)
            swap.start()
            swap.wait()
            unpack(right_land, [put_to(basis, j + 1, v, k, 1) for k in range(layers) for v in range(2)])
        return carry

    lax.fori_loop(0, ITERS, iteration, 0)

    names = [(i, j) for i in range(ITERS + 1) for j in range(i, ITERS + 1)]
    sums = {name: jnp.zeros((cx, cy), F32) for name in names}
    for k in range(layers):
        chain = [basis[i, :, k, 0, own] for i in range(ITERS + 1)]
        terms = [chain[j] - chain[j + 1] for j in range(ITERS)] + [chain[0]]
        for i, j in names:
            prod = terms[i] * terms[j]
            sums[i, j] = sums[i, j] + prod[0] + prod[1]
    line = reduce_all([total(sums[name]) for name in names])
    gram = {name: pick(line, at) for at, name in enumerate(names)}
    rows = [[gram[min(i, j), max(i, j)] for j in range(ITERS + 1)] for i in range(ITERS)]
    for a in range(ITERS):
        for i in range(a + 1, ITERS):
            share = rows[i][a] / rows[a][a]
            for c in range(a, ITERS + 1):
                rows[i][c] = rows[i][c] - share * rows[a][c]
    weights = [None] * ITERS
    for a in reversed(range(ITERS)):
        part = rows[a][ITERS]
        for c in range(a + 1, ITERS):
            part = part - rows[a][c] * weights[c]
        weights[a] = part / rows[a][a]
    for k in range(layers):
        out = weights[0] * stored[0, :, k]
        rest = forcing[:, k] - weights[0] * (basis[0, :, k, 0, own] - basis[1, :, k, 0, own])
        for j in range(1, ITERS):
            out = out + weights[j] * stored[j, :, k]
            rest = rest - weights[j] * (basis[j, :, k, 0, own] - basis[j + 1, :, k, 0, own])
        solution[:, k] = out
        residual[:, k] = rest


def solution(mesh):
    nx, ny = mesh.shape["gx"], mesh.shape["gy"]
    count = nx * ny

    def body(forcing, viscosity, spread, coupling, friction, mask, aggs):
        layers, cx, cy = forcing.shape[1:]
        dma = pltpu.SemaphoreType.DMA
        tall = cx + 2 * HALO
        half = layers // 2

        def vm(*shape, dtype=F32):
            return pltpu.VMEM(shape, dtype)

        def level(n):
            return (
                vm(2, n, 2, 2, tall + 2 * TOP, cy),
                vm(n, 2, tall, cy), vm(n, 2, tall, cy), vm(4, n, 2, tall, cy), vm(2, tall, cy),
                vm(n, 2, tall, cy), vm(n, 2, tall, cy), vm(n, 2, 2, tall, cy), vm(n, 2, 2, tall, cy),
            )

        def swap(planes, pieces):
            tiles = -(-planes * SLOT // cy)
            return (vm(tiles, cx, cy), vm(2, tiles, tall, cy), dma((8, pieces)), dma((8, pieces)))

        scratch = (
            (level(layers), level(half), level(1)),
            (vm(ITERS + 1, 2, layers, 2, tall, cy), vm(ITERS, 2, layers, cx, cy),
             vm(layers, 2, tall, cy), vm(layers, 2, tall, cy), vm(4, 2, tall, cy)),
            (vm(cx, cy, cy, dtype=BF16), vm(5, cy, cy, dtype=BF16), vm(5, cy, cy, dtype=BF16),
             vm(1, cy), vm(2, cy)),
            (vm(2, 2, cy), vm(2, 4, 2, cy), dma((2, 4, 1)), dma((2, 4, 1))),
            tuple((vm(n, cy), vm(2, count, n, cy), dma(()), dma((2,))) for n in (1, 1, 8)),
            swap(4 + 4 * layers, 4),
            swap(2 * layers, 1),
            swap(4 + 2 * half, 3),
            (vm(2, cy), vm(8, 2, cy), dma((8, 1)), dma((8, 1))),
            (vm(2, half, 2, HALO, cy), vm(2, 2, 2, HALO, cy)),
        )
        flat, tree = jax.tree.flatten(scratch)

        def run(*refs):
            kernel(nx, ny, layers, cx, cy, *refs[:9], *jax.tree.unflatten(tree, refs[9:]))

        shape = jax.ShapeDtypeStruct(forcing.shape, F32)
        whole = pl.BlockSpec(memory_space=pltpu.VMEM)
        return tuple(pl.pallas_call(
            run,
            out_shape=(shape, shape),
            in_specs=[whole] * 7,
            out_specs=(whole, whole),
            scratch_shapes=flat,
            compiler_params=pltpu.CompilerParams(has_side_effects=True, vmem_limit_bytes=60 * 1024 * 1024),
        )(forcing, viscosity, spread, coupling, friction, mask, aggs))

    return jax.shard_map(
        body,
        mesh=mesh,
        in_specs=(
            P(None, None, "gx", "gy"),
            P(None, "gx", "gy"),
            P(None, "gx", "gy"),
            P("gx", "gy"),
            P("gx", "gy"),
            P("gx", "gy"),
            P("gx", "gy"),
        ),
        out_specs=(P(None, None, "gx", "gy"), P(None, None, "gx", "gy")),
        check_vma=False,
    )
```

```python
import jax
import jax.numpy as jnp
from jax import lax
from jax.experimental import pallas as pl
from jax.experimental.pallas import tpu as pltpu
from jax.sharding import PartitionSpec as P

ITERS = 3
CSWEEPS = 4
LINE_WEIGHT = 0.8
POINT_WEIGHT = 0.7
COARSE_WEIGHT = 0.7
MESH = pl.DeviceIdType.MESH
F32 = jnp.float32
BF16 = jnp.bfloat16
TOP = 8
HALO = 8
SLOT = 2 * HALO
STEPS = ((1, 0), (-1, 0), (0, 1), (0, -1), (1, 1), (1, -1), (-1, 1), (-1, -1))
BACK = (1, 0, 3, 2, 7, 6, 5, 4)


def split(x):
    high = x.astype(BF16)
    return high, (x - high.astype(F32)).astype(BF16)


def dot(a, b, ca, cb):
    return lax.dot_general(a, b, (((ca,), (cb,)), ((), ())), preferred_element_type=F32)


def total(x):
    return jnp.sum(jnp.sum(x, axis=1, keepdims=True), axis=0, keepdims=True)


def turn(x, shift):
    flat = x.reshape(-1, x.shape[-1])
    return pltpu.roll(flat, shift % x.shape[-1], 1).reshape(x.shape)


def kernel(nx, ny, layers, cx, cy, forcing, viscosity, spread, coupling, friction, mask, aggs,
           solution, residual, *scratch):
    count = nx * ny
    gx = lax.axis_index("gx")
    gy = lax.axis_index("gy")
    me = gx * ny + gy
    (levels, (basis, stored, visc, spr, misc), (hit, big_hi, big_lo, point_diag, point_cross, own_sum),
     (x_out, x_in, x_send, x_recv), gathers, first_swap, right_swap, side_swap, point_swap,
     (mid_rows, col_rows), (near_out, near_in, near_send, near_recv)) = scratch
    tall = cx + 2 * HALO
    own = pl.ds(HALO, cx)
    slots = cy // SLOT
    lane = lax.broadcasted_iota(jnp.int32, (cx, cy), 1)
    row = lax.broadcasted_iota(jnp.int32, (cx, cy), 0)
    first_lane, last_lane = lane == 0, lane == cy - 1
    long_lane = lax.broadcasted_iota(jnp.int32, (tall, cy), 1)
    kept_lane = (long_lane < HALO) | (long_lane >= cy - HALO)

    exists, peers = [], []
    for dx, dy in STEPS:
        ok = []
        if dx:
            ok.append(gx < nx - 1 if dx > 0 else gx > 0)
        if dy:
            ok.append(gy < ny - 1 if dy > 0 else gy > 0)
        exists.append(ok[0] if len(ok) == 1 else jnp.logical_and(ok[0], ok[1]))
        peers.append((gx + dx, gy + dy))

    class Swap:
        def __init__(self, pieces, send, recv):
            self.pieces = pieces
            self.copies = [[pltpu.make_async_remote_copy(
                src_ref=src, dst_ref=dst, send_sem=send.at[d, i], recv_sem=recv.at[BACK[d], i],
                device_id=peers[d], device_id_type=MESH) for i, (src, dst) in enumerate(pieces[d])]
                for d in range(len(pieces))]

        def start(self, which=None):
            for d in range(len(self.copies)) if which is None else which:
                @pl.when(exists[d])
                def _():
                    for copy in self.copies[d]:
                        copy.start()

        def wait(self):
            for d in range(len(self.copies)):
                @pl.when(exists[d])
                def _():
                    for copy in self.copies[d]:
                        copy.wait_send()
                    for copy in self.copies[BACK[d]]:
                        copy.wait_recv()

        def clear(self):
            for d in range(len(self.copies)):
                @pl.when(jnp.logical_not(exists[d]))
                def _():
                    for _, ref in self.pieces[BACK[d]]:
                        ref[...] = jnp.zeros(ref.shape, F32)

    def edges(rows, packed, landed):
        low, high = pl.ds(0, HALO), pl.ds(cx - HALO, HALO)
        top, bottom = pl.ds(0, HALO), pl.ds(HALO + cx, HALO)
        return [
            [(src(cx - HALO), dst(0)) for src, dst in rows],
            [(src(0), dst(1)) for src, dst in rows],
            [(packed, landed.at[0, :, own])],
            [(packed, landed.at[1, :, own])],
            [(packed.at[:, high], landed.at[0, :, top])],
            [(packed.at[:, high], landed.at[1, :, top])],
            [(packed.at[:, low], landed.at[0, :, bottom])],
            [(packed.at[:, low], landed.at[1, :, bottom])],
        ]

    def ends(e):
        return pl.ds(0, HALO) if e == 0 else pl.ds(HALO + cx, HALO)

    class Packer:
        def __init__(self, out):
            self.out = out
            self.at = 0
            self.tile = None

        def add(self, value):
            s, m = divmod(self.at, slots)
            moved = pltpu.roll(value, (SLOT * m + HALO) % cy, 1)
            self.tile = moved if m == 0 else jnp.where(lane // SLOT == m, moved, self.tile)
            self.at += 1
            if m == slots - 1:
                self.flush(s)

        def flush(self, s):
            self.out[s] = self.tile
            self.tile = None

        def finish(self):
            if self.tile is not None:
                self.flush((self.at - 1) // slots)

    def unpack(landed, puts):
        south = long_lane % SLOT < HALO
        comb = None
        for i, put in enumerate(puts):
            s, m = divmod(i, slots)
            if m == 0:
                comb = jnp.where(south, landed[0, s], landed[1, s])
            put(jnp.where(kept_lane, pltpu.roll(comb, (cy - SLOT * m - HALO) % cy, 1), 0.0))

    chunks = ((0, tall // 2), (tall // 2, tall // 2))
    both = (0, 1)

    class Level:
        def __init__(self, depth, refs):
            self.depth = depth
            (self.field, self.diag, self.vert, self.side, self.cross, self.inverse, self.upper,
             self.right, self.forward) = refs

        def at(self, p, k, t, c0, cn, shift=0):
            return self.field[p, k, t, :, pl.ds(TOP + c0 + shift, cn), :]

        def sideways(self, p, k, c0, cn, tiles):
            here = pl.ds(c0, cn)
            wide = lax.broadcasted_iota(jnp.int32, (2, cn, cy), 2)
            value = [self.at(p, k, t, c0, cn) for t in both]
            up = [turn(v, cy - 1) for v in value]
            down = [turn(v, 1) for v in value]
            outs = []
            for t in tiles:
                north = jnp.where(wide == cy - 1, up[1 - t], up[t])
                south = jnp.where(wide == 0, down[1 - t], down[t])
                out = (self.side[0, k, t, here][None] * self.at(p, k, t, c0, cn, 1)
                       + self.side[1, k, t, here][None] * self.at(p, k, t, c0, cn, -1)
                       + self.side[2, k, t, here][None] * north + self.side[3, k, t, here][None] * south)
                if k == 0:
                    crossed = self.cross[t, here]
                    out = out - jnp.stack([crossed * value[t][1], crossed * value[t][0]])
                outs.append(out)
            return value, outs

        def leftover(self, p, right, emit, tiles=both, spans=chunks):
            for c0, cn in spans:
                here = pl.ds(c0, cn)
                for k in range(self.depth):
                    value, outs = self.sideways(p, k, c0, cn, tiles)
                    for i, t in enumerate(tiles):
                        out = outs[i] - self.diag[k, t, here][None] * value[t]
                        if k + 1 < self.depth:
                            out = out + self.vert[k, t, here][None] * self.at(p, k + 1, t, c0, cn)
                        if k > 0:
                            out = out + self.vert[k - 1, t, here][None] * self.at(p, k - 1, t, c0, cn)
                        emit(k, t, c0, cn, right(k, t, here) + out)

        def solve(self, source, old, p):
            for c0, cn in chunks:
                here = pl.ds(c0, cn)
                last = [None, None]
                for k in range(self.depth):
                    values = source(k, c0, cn)
                    for t in both:
                        value = values[t]
                        if k > 0:
                            value = value + self.vert[k - 1, t, here][None] * last[t]
                        last[t] = value * self.inverse[k, t, here][None]
                        self.forward[k, t, :, here] = last[t]
                for k in reversed(range(self.depth)):
                    for t in both:
                        if k + 1 < self.depth:
                            last[t] = self.forward[k, t, :, here] - self.upper[k, t, here][None] * last[t]
                        value = LINE_WEIGHT * last[t]
                        if old is not None:
                            value = value + (1.0 - LINE_WEIGHT) * self.at(old, k, t, c0, cn)
                        self.field[p, k, t, :, pl.ds(TOP + c0, cn), :] = value

        def first(self, right):
            self.solve(lambda k, c0, cn: [right(k, t, pl.ds(c0, cn)) for t in both], None, 0)

        def sweep(self, p, right):
            def source(k, c0, cn):
                outs = self.sideways(p, k, c0, cn, both)[1]
                return [right(k, t, pl.ds(c0, cn)) + outs[t] for t in both]
            self.solve(source, p, 1 - p)

        def factor(self):
            inverse = 1.0 / self.diag[0]
            self.inverse[0] = inverse
            for k in range(1, self.depth):
                ratio = -self.vert[k - 1] * inverse
                self.upper[k - 1] = ratio
                inverse = 1.0 / (self.diag[k] + self.vert[k - 1] * ratio)
                self.inverse[k] = inverse

        def after(self, right):
            self.sweep(0, right)
            self.sweep(1, right)

    half = layers // 2
    fine, middle, column = (Level(n, refs) for n, refs in zip((layers, half, 1), levels))
    for level in (fine, middle, column):
        for p in range(2):
            for k in range(level.depth):
                for t in both:
                    level.field[p, k, t, :, pl.ds(0, TOP), :] = jnp.zeros((2, TOP, cy), F32)
                    level.field[p, k, t, :, pl.ds(TOP + tall, TOP), :] = jnp.zeros((2, TOP, cy), F32)

    def rows_of(ref, at):
        return lambda start: ref.at[at + (pl.ds(start, HALO),)]

    any_k = slice(None)

    (first_pack, first_land, first_send, first_recv) = first_swap
    swap0 = Swap(edges([
        (lambda lo: viscosity.at[:, pl.ds(lo, HALO)], lambda e: visc.at[:, 0, ends(e)]),
        (lambda lo: spread.at[:, pl.ds(lo, HALO)], lambda e: spr.at[:, 0, ends(e)]),
        (lambda lo: misc.at[:, 0, pl.ds(HALO + lo, HALO)], lambda e: misc.at[:, 0, ends(e)]),
    ], first_pack, first_land), first_send, first_recv)
    (right_pack, right_land, right_send, right_recv) = right_swap

    def swap_right(j):
        return Swap(edges([(lambda lo: basis.at[j, :, :, 0, pl.ds(HALO + lo, HALO)],
                            lambda e: basis.at[j, :, :, 0, ends(e)])],
                          right_pack, right_land), right_send, right_recv)

    (side_pack, side_land, side_send, side_recv) = side_swap
    swap_side = Swap(edges([
        (lambda lo: middle.field.at[1, :, 0, :, pl.ds(TOP + HALO + lo, HALO)], lambda e: mid_rows.at[e]),
        (lambda lo: column.field.at[1, 0, 0, :, pl.ds(TOP + HALO + lo, HALO)], lambda e: col_rows.at[e, 0]),
        (lambda lo: column.right.at[0, 0, :, pl.ds(HALO + lo, HALO)], lambda e: col_rows.at[e, 1]),
    ], side_pack, side_land), side_send, side_recv)
    (far_out, far_in, far_send, far_recv) = point_swap
    swap_far = Swap([[(far_out, far_in.at[d])] for d in range(8)], far_send, far_recv)

    swap_near = Swap([[(near_out, near_in.at[d])] for d in range(4)], near_send, near_recv)

    def near_swap(p, q):
        return Swap([[(x_out.at[p], x_in.at[q, d])] for d in range(4)], x_send.at[p], x_recv.at[q])

    misc[0, 0, own] = mask[...].astype(F32)
    misc[1, 0, own] = aggs[...].astype(F32)
    misc[2, 0, own] = friction[...]
    misc[3, 0, own] = coupling[...]
    swap0.start((0, 1))
    packer = Packer(first_pack)
    for i in range(4):
        packer.add(misc[i, 0, own])
    for k in range(layers):
        packer.add(viscosity[k])
        packer.add(spread[k])
    packer.finish()
    swap0.start(range(2, 8))
    packer = Packer(right_pack)
    for k in range(layers):
        basis[0, :, k, 0, own] = forcing[:, k]
        for v in range(2):
            packer.add(forcing[v, k])
    packer.finish()
    swap_right(0).start()
    for j in range(ITERS):
        swap_right(j).clear()
    swap0.clear()
    swap_side.clear()
    swap_far.clear()
    for q in range(2):
        near_swap(0, q).clear()
    swap_near.clear()
    for k in range(layers):
        visc[k, 0, own] = viscosity[k]
        spr[k, 0, own] = spread[k]

    def gather(which, slot=0):
        out, into, send, recv = gathers[which]
        into, recv = into.at[slot], recv.at[slot]
        rest = into.at[pl.ds(0, count - 1)]

        def start():
            def step(i, carry):
                target = lax.rem(me + i, count)
                pltpu.make_async_remote_copy(
                    src_ref=out, dst_ref=into.at[me], send_sem=send, recv_sem=recv,
                    device_id=(target // ny, lax.rem(target, ny)), device_id_type=MESH).start()
                return carry

            lax.fori_loop(1, count, step, 0)
            into[me] = out[...]

        def wait():
            pltpu.make_async_copy(rest, rest, recv).wait()
            pltpu.make_async_copy(rest, rest, send).wait()

        return start, wait

    wide = lax.broadcasted_iota(jnp.int32, (1, cy), 1)

    def reduce_all(parts):
        line = jnp.zeros((1, cy), F32)
        for i, part in enumerate(parts):
            line = jnp.where(wide == i, part, line)
        gathers[1][0][...] = line
        start, wait = gather(1)
        start()
        wait()
        return jnp.sum(gathers[1][1][0, :, 0, :], axis=0, keepdims=True)

    def pick(line, i):
        return jnp.sum(jnp.where(wide == i, line, 0.0), axis=1, keepdims=True)

    def put_to(ref, *at):
        def put(value):
            ref[at] = value
        return put

    swap0.wait()
    puts = [put_to(misc, i, 1) for i in range(4)]
    for k in range(layers):
        puts += [put_to(visc, k, 1), put_to(spr, k, 1)]
    unpack(first_land, puts)

    ids_all = [misc[1, t].astype(jnp.int32) for t in both]
    ids = misc[1, 0, own].astype(jnp.int32)
    ice = [misc[0, t] for t in both]
    for t in both:
        column.field[1, 0, t, 0, pl.ds(TOP, tall), :] = ice[t]
    around = []
    ups = [turn(x, cy - 1) for x in ice]
    downs = [turn(x, 1) for x in ice]
    for t in both:
        around.append((column.field[1, 0, t, 0, pl.ds(TOP + 1, tall), :],
                       column.field[1, 0, t, 0, pl.ds(TOP - 1, tall), :],
                       jnp.where(long_lane == cy - 1, ups[1 - t], ups[t]),
                       jnp.where(long_lane == 0, downs[1 - t], downs[t])))
    for k in range(layers):
        for t in both:
            owned = spr[k, t]
            faces = 4.0 * owned
            if k + 1 < layers:
                face = 0.5 * (visc[k, t] + visc[k + 1, t]) * ice[t]
                fine.vert[k, t] = face
                faces = faces + face
            if k > 0:
                faces = faces + fine.vert[k - 1, t]
            if k == 0:
                faces = faces + misc[2, t]
            fine.diag[k, t] = ice[t] * faces + (1.0 - ice[t])
            owned = owned * ice[t]
            for d in range(4):
                fine.side[d, k, t] = owned * around[t][d]
    for t in both:
        fine.cross[t] = misc[2, t] * misc[3, t] * ice[t]
    for finer, coarser in ((fine, middle), (middle, column)):
        size = finer.depth // coarser.depth
        for k in range(coarser.depth):
            group = range(k * size, (k + 1) * size)
            diag = sum(finer.diag[j] for j in group)
            inner_faces = sum(finer.vert[j] for j in list(group)[:-1])
            coarser.diag[k] = diag - 2.0 * inner_faces
            if k + 1 < coarser.depth:
                coarser.vert[k] = finer.vert[group[-1]]
            for d in range(4):
                coarser.side[d, k] = sum(finer.side[d, j] for j in group)
        coarser.cross[...] = finer.cross[...]

    side2 = [column.side[d, 0, 0, own] for d in range(4)]
    diag2, cross2 = column.diag[0, 0, own], column.cross[0, own]
    inner = (diag2 - jnp.where(row < cx - 1, side2[0], 0.0) - jnp.where(row > 0, side2[1], 0.0)
             - jnp.where(lane < cy - 1, side2[2], 0.0) - jnp.where(lane > 0, side2[3], 0.0))
    entries = (inner, cross2, jnp.where(row == cx - 1, side2[0], 0.0), jnp.where(row == 0, side2[1], 0.0),
               jnp.where(last_lane, side2[2], 0.0), jnp.where(first_lane, side2[3], 0.0))
    eight = lax.broadcasted_iota(jnp.int32, (8, cy), 0)
    tile = jnp.zeros((8, cy), F32)
    for i, entry in enumerate(entries):
        tile = jnp.where(eight == i, total(entry), tile)
    gathers[2][0][...] = tile
    tables_start, tables_wait = gather(2)
    tables_start()
    for level in (fine, middle, column):
        level.factor()

    down = lax.broadcasted_iota(jnp.int32, (cy, cy), 0)
    across = lax.broadcasted_iota(jnp.int32, (cy, cy), 1)
    for r in range(cx):
        hit[r] = jnp.where(ids[r:r + 1, :] == down, 1.0, 0.0).astype(BF16)
    near = jnp.zeros((cy, cy), F32)
    for r in range(cx):
        here = hit[r].astype(F32)
        term = diag2[r:r + 1, :] * here
        if r + 1 < cx:
            term = term - side2[0][r:r + 1, :] * hit[r + 1].astype(F32)
        if r > 0:
            term = term - side2[1][r:r + 1, :] * hit[r - 1].astype(F32)
        term = term - jnp.where(across < cy - 1, side2[2][r:r + 1, :], 0.0) * pltpu.roll(here, cy - 1, 1)
        term = term - jnp.where(across > 0, side2[3][r:r + 1, :], 0.0) * pltpu.roll(here, 1, 1)
        high, low = split(term)
        near = near + dot(high, hit[r], 1, 1) + dot(low, hit[r], 1, 1)
    point_diag[...] = jnp.sum(jnp.where(down == across, near, 0.0), axis=0, keepdims=True)
    tables = [near]
    for d, r, e in ((0, cx - 1, HALO + cx), (1, 0, HALO - 1)):
        other = ids_all[0][e:e + 1, :]
        term = jnp.where(other == down, side2[d][r:r + 1, :], 0.0)
        high, low = split(term)
        tables.append(-(dot(high, hit[r], 1, 1) + dot(low, hit[r], 1, 1)))
    for d, q, e in ((2, cy - 1, 0), (3, 0, cy - 1)):
        other = ids_all[1][HALO:HALO + cx, e:e + 1]
        term = jnp.where(other == lane, side2[d][:, q:q + 1], 0.0)
        here = jnp.where(ids[:, q:q + 1] == lane, 1.0, 0.0)
        high, low = split(term)
        here = here.astype(BF16)
        tables.append(-(dot(high, here, 0, 0) + dot(low, here, 0, 0)))
    for i, table in enumerate(tables):
        high, low = split(table)
        big_hi[i] = high
        big_lo[i] = low

    tall4 = lax.broadcasted_iota(jnp.int32, (4 * cx, cy), 0) % cx

    def restrict_points(first, second):
        h0, l0 = split(first)
        h1, l1 = split(second)
        left = jnp.concatenate([h0, h1, l0, l1], axis=0)
        out = jnp.zeros((4 * cx, cy), F32)
        for r in range(cx):
            out = jnp.where(tall4 == r, dot(left, hit[r], 1, 1), out)
        parts = [jnp.sum(out[i * cx:(i + 1) * cx] + out[(i + 2) * cx:(i + 3) * cx], axis=0, keepdims=True)
                 for i in range(2)]
        return jnp.concatenate(parts, axis=0)

    point_cross[...] = restrict_points(cross2, cross2)
    scale = POINT_WEIGHT / point_diag[...]
    ones = jnp.ones((8, cy), BF16)
    sixteen = lax.broadcasted_iota(jnp.int32, (16, cy), 0)
    sent = jnp.where(sixteen == 5, scale * point_cross[0:1, :], 0.0)
    for i, table in enumerate(tables):
        sent = jnp.where(sixteen == i, scale * jnp.sum(table, axis=0, keepdims=True), sent)
        across_sum = (dot(ones, big_hi[i], 1, 1) + dot(ones, big_lo[i], 1, 1))[0:1, :]
        if i == 0:
            own_sum[...] = across_sum
        else:
            sent = jnp.where(sixteen == 5 + i, across_sum, sent)
    near_out[...] = sent
    swap_near.start()
    block_row = lax.broadcasted_iota(jnp.int32, (count, cy), 0)
    coarse_lane = lax.broadcasted_iota(jnp.int32, (count, cy), 1)
    shifts = (ny, count - ny, 1, count - 1)

    def coarse_begin(j, right, x):
        lines = [right - own_sum[...] * x - point_cross[...] * jnp.concatenate([x[1:2], x[0:1]], axis=0)]
        for d in range(4):
            lines.append(-near_in[BACK[d], 6 + BACK[d]:7 + BACK[d], :] * x)
        line = jnp.zeros((1, cy), F32)
        for i, part in enumerate(lines):
            sums = jnp.sum(part, axis=1, keepdims=True)
            for v in range(2):
                line = jnp.where(wide == 2 * i + v, sums[v:v + 1], line)
        gathers[0][0][...] = line
        start, wait = gather(0, lax.rem(j, 2))
        start()
        return wait

    def coarse_end(j, wait):
        pl.when(j == 0)(tables_wait)
        wait()
        came = gathers[0][1][lax.rem(j, 2), :, 0, :]
        right = came
        for d in range(4):
            right = right + pltpu.roll(pltpu.roll(came, shifts[d], 0), cy - 2 - 2 * d, 1)
        diag, crossed, east, west, north, south = (gathers[2][1][0, :, i, :] for i in range(6))
        weight = COARSE_WEIGHT / diag
        answer = right * weight
        for _ in range(CSWEEPS - 1):
            other = jnp.where(coarse_lane % 2 == 0, pltpu.roll(answer, cy - 1, 1), pltpu.roll(answer, 1, 1))
            applied = diag * answer + crossed * other - (
                east * pltpu.roll(answer, count - ny, 0) + west * pltpu.roll(answer, ny, 0)
                + north * pltpu.roll(answer, count - 1, 0) + south * pltpu.roll(answer, 1, 0))
            answer = answer + (right - applied) * weight
        hops = ((0, 0),) + STEPS[:4]
        known = {}

        def value(dx, dy):
            if (dx, dy) not in known:
                line = jnp.sum(jnp.where(block_row == me + dx * ny + dy, answer, 0.0), axis=0, keepdims=True)
                known[dx, dy] = jnp.concatenate([line[:, 0:1], line[:, 1:2]], axis=0)
            return known[dx, dy]

        found = []
        for i, (dx, dy) in enumerate(hops):
            here = value(dx, dy)
            rows = near_out if i == 0 else near_in.at[BACK[i - 1]]
            out = here - rows[5:6, :] * jnp.concatenate([here[1:2], here[0:1]], axis=0)
            for n, (ex, ey) in enumerate(hops):
                out = out - rows[n:n + 1, :] * value(dx + ex, dy + ey)
            found.append(out)
        return found

    def point_apply(xs):
        out = point_cross[...] * jnp.concatenate([xs[0][1:2], xs[0][0:1]], axis=0)
        for i, x in enumerate(xs):
            high, low = split(x)
            out = out + dot(high, big_hi[i], 1, 0) + dot(low, big_hi[i], 1, 0) + dot(high, big_lo[i], 1, 0)
        return out

    def point_cycle(j, right):
        def begin(p, x):
            x_out[p] = x
            q = lax.rem(p + j, 2)
            swap = near_swap(p, q)
            swap.start()

            def end():
                swap.wait()
                return [x] + [x_in[q, BACK[d]] for d in range(4)]
            return end

        scale = POINT_WEIGHT / point_diag[...]
        x = right * scale
        end = begin(0, x)
        packer = Packer(side_pack)
        for v in range(2):
            packer.add(column.field[1, 0, 0, v, pl.ds(TOP + HALO, cx), :])
            packer.add(column.right[0, 0, v, own])
        for k in range(half):
            for v in range(2):
                packer.add(middle.field[1, k, 0, v, pl.ds(TOP + HALO, cx), :])
        packer.finish()
        swap_side.start()
        x = x + (right - point_apply(end())) * scale
        end = begin(1, x)
        pl.when(j == 0)(swap_near.wait)
        coarse_wait = coarse_begin(j, right, x)
        x = x + (right - point_apply(end())) * scale
        xs = begin(0, x)()
        xs = [x + y for x, y in zip(xs, coarse_end(j, coarse_wait))]
        return xs[0] + (right - point_apply(xs)) * scale

    def spread_points(x):
        far_out[...] = x
        swap_far.start()
        swap_side.wait()
        swap_far.wait()
        parts = [[], []]
        zones = ((pl.ds(0, HALO), 1, 6, 7), (own, None, 2, 3), (pl.ds(HALO + cx, HALO), 0, 4, 5))
        short = {n: lax.broadcasted_iota(jnp.int32, (n, cy), 1) < cy // 2 for n in (HALO, cx)}

        def take(src, v, index):
            values = x if src is None else far_in[BACK[src]]
            return jnp.take_along_axis(jnp.broadcast_to(values[v:v + 1], index.shape), index, axis=1,
                                       mode="promise_in_bounds")

        for rows, straight, right, left in zones:
            index = [misc[1, t, rows].astype(jnp.int32) for t in both]
            parts[0].append(jnp.stack([take(straight, v, index[0]) for v in range(2)]))
            lanes = short[index[1].shape[0]]
            parts[1].append(jnp.stack([jnp.where(lanes, take(right, v, index[1]), take(left, v, index[1]))
                                       for v in range(2)]))
        return [jnp.concatenate(p, axis=1) for p in parts]

    def iteration(j, carry):
        def right0(k, t, here):
            return basis[j, :, k, t, here]

        def right1(k, t, here):
            return middle.right[k, t, :, here]

        def right2(k, t, here):
            return column.right[k, t, :, here]

        def collect(coarser, size):
            held = {}

            def emit(k, t, c0, cn, value):
                held[t] = held[t] + value if k % size else value
                if k % size == size - 1:
                    coarser.right[k // size, t, :, pl.ds(c0, cn)] = held[t]
            return emit

        swap_right(j).wait()
        unpack(right_land, [put_to(basis, j, v, k, 1) for k in range(layers) for v in range(2)])
        fine.first(right0)
        fine.sweep(0, right0)
        fine.leftover(1, right0, collect(middle, 2))
        middle.first(right1)
        middle.sweep(0, right1)
        middle.leftover(1, right1, collect(column, half))
        column.first(right2)
        column.sweep(0, right2)
        kept = []
        column.leftover(1, right2, lambda k, t, c0, cn, value: kept.append(value), (0,), ((HALO, cx),))
        found = spread_points(point_cycle(j, restrict_points(kept[0][0], kept[0][1])))

        whole = pl.ds(TOP, tall)
        inside = pl.ds(TOP + HALO, cx)
        landed = []
        unpack(side_land, [landed.append] * (4 + 2 * half))
        column.field[0, 0, 0, :, whole] = found[0] + jnp.concatenate(
            [col_rows[0, 0], column.field[1, 0, 0, :, inside], col_rows[1, 0]], axis=1)
        column.field[0, 0, 1, :, whole] = found[1] + jnp.stack([landed[0], landed[2]])
        for e in range(2):
            column.right[0, 0, :, ends(e)] = col_rows[e, 1]
        column.right[0, 1] = jnp.stack([landed[1], landed[3]])
        column.after(right2)
        for k in range(half):
            middle.field[0, k, 0, :, whole] = column.field[0, 0, 0, :, whole] + jnp.concatenate(
                [mid_rows[0, k], middle.field[1, k, 0, :, inside], mid_rows[1, k]], axis=1)
            middle.field[0, k, 1, :, whole] = column.field[0, 0, 1, :, whole] + jnp.stack(
                [landed[4 + 2 * k], landed[5 + 2 * k]])
        middle.after(right1)
        for k in range(layers):
            for t in both:
                fine.field[0, k, t, :, whole] = (fine.field[1, k, t, :, whole]
                                                 + middle.field[0, k // 2, t, :, whole])
        fine.after(right0)

        packer = Packer(right_pack)

        def emit(k, t, c0, cn, value):
            basis[j + 1, :, k, 0, own] = value
            stored[j, :, k] = fine.field[0, k, 0, :, inside]
            for v in range(2):
                packer.add(value[v])

        fine.leftover(0, right0, emit, (0,), ((HALO, cx),))
        packer.finish()

        @pl.when(j < ITERS - 1)
        def _():
            swap_right(j + 1).start()
        return carry

    lax.fori_loop(0, ITERS, iteration, 0)

    names = [(i, j) for i in range(ITERS + 1) for j in range(i, ITERS + 1)]
    sums = {name: jnp.zeros((cx, cy), F32) for name in names}
    for k in range(layers):
        chain = [basis[i, :, k, 0, own] for i in range(ITERS + 1)]
        terms = [chain[j] - chain[j + 1] for j in range(ITERS)] + [chain[0]]
        for i, j in names:
            prod = terms[i] * terms[j]
            sums[i, j] = sums[i, j] + prod[0] + prod[1]
    line = reduce_all([total(sums[name]) for name in names])
    gram = {name: pick(line, at) for at, name in enumerate(names)}
    rows = [[gram[min(i, j), max(i, j)] for j in range(ITERS + 1)] for i in range(ITERS)]
    for a in range(ITERS):
        for i in range(a + 1, ITERS):
            share = rows[i][a] / rows[a][a]
            for c in range(a, ITERS + 1):
                rows[i][c] = rows[i][c] - share * rows[a][c]
    weights = [None] * ITERS
    for a in reversed(range(ITERS)):
        part = rows[a][ITERS]
        for c in range(a + 1, ITERS):
            part = part - rows[a][c] * weights[c]
        weights[a] = part / rows[a][a]
    for k in range(layers):
        out = weights[0] * stored[0, :, k]
        rest = forcing[:, k] - weights[0] * (basis[0, :, k, 0, own] - basis[1, :, k, 0, own])
        for j in range(1, ITERS):
            out = out + weights[j] * stored[j, :, k]
            rest = rest - weights[j] * (basis[j, :, k, 0, own] - basis[j + 1, :, k, 0, own])
        solution[:, k] = out
        residual[:, k] = rest


def solution(mesh):
    nx, ny = mesh.shape["gx"], mesh.shape["gy"]
    count = nx * ny

    def body(forcing, viscosity, spread, coupling, friction, mask, aggs):
        layers, cx, cy = forcing.shape[1:]
        dma = pltpu.SemaphoreType.DMA
        tall = cx + 2 * HALO
        half = layers // 2

        def vm(*shape, dtype=F32):
            return pltpu.VMEM(shape, dtype)

        def level(n):
            return (
                vm(2, n, 2, 2, tall + 2 * TOP, cy),
                vm(n, 2, tall, cy), vm(n, 2, tall, cy), vm(4, n, 2, tall, cy), vm(2, tall, cy),
                vm(n, 2, tall, cy), vm(n, 2, tall, cy), vm(n, 2, 2, tall, cy), vm(n, 2, 2, tall, cy),
            )

        def swap(planes, pieces):
            tiles = -(-planes * SLOT // cy)
            return (vm(tiles, cx, cy), vm(2, tiles, tall, cy), dma((8, pieces)), dma((8, pieces)))

        scratch = (
            (level(layers), level(half), level(1)),
            (vm(ITERS + 1, 2, layers, 2, tall, cy), vm(ITERS, 2, layers, cx, cy),
             vm(layers, 2, tall, cy), vm(layers, 2, tall, cy), vm(4, 2, tall, cy)),
            (vm(cx, cy, cy, dtype=BF16), vm(5, cy, cy, dtype=BF16), vm(5, cy, cy, dtype=BF16),
             vm(1, cy), vm(2, cy), vm(1, cy)),
            (vm(2, 2, cy), vm(2, 4, 2, cy), dma((2, 4, 1)), dma((2, 4, 1))),
            tuple((vm(n, cy), vm(2, count, n, cy), dma(()), dma((2,))) for n in (1, 1, 8)),
            swap(4 + 2 * layers, 3),
            swap(2 * layers, 1),
            swap(4 + 2 * half, 3),
            (vm(2, cy), vm(8, 2, cy), dma((8, 1)), dma((8, 1))),
            (vm(2, half, 2, HALO, cy), vm(2, 2, 2, HALO, cy)),
            (vm(16, cy), vm(4, 16, cy), dma((4, 1)), dma((4, 1))),
        )
        flat, tree = jax.tree.flatten(scratch)

        def run(*refs):
            kernel(nx, ny, layers, cx, cy, *refs[:9], *jax.tree.unflatten(tree, refs[9:]))

        shape = jax.ShapeDtypeStruct(forcing.shape, F32)
        whole = pl.BlockSpec(memory_space=pltpu.VMEM)
        return tuple(pl.pallas_call(
            run,
            out_shape=(shape, shape),
            in_specs=[whole] * 7,
            out_specs=(whole, whole),
            scratch_shapes=flat,
            compiler_params=pltpu.CompilerParams(has_side_effects=True, vmem_limit_bytes=60 * 1024 * 1024),
        )(forcing, viscosity, spread, coupling, friction, mask, aggs))

    return jax.shard_map(
        body,
        mesh=mesh,
        in_specs=(
            P(None, None, "gx", "gy"),
            P(None, "gx", "gy"),
            P(None, "gx", "gy"),
            P("gx", "gy"),
            P("gx", "gy"),
            P("gx", "gy"),
            P("gx", "gy"),
        ),
        out_specs=(P(None, None, "gx", "gy"), P(None, None, "gx", "gy")),
        check_vma=False,
    )
```

```python
import jax
import jax.numpy as jnp
from jax import lax
from jax.experimental import pallas as pl
from jax.experimental.pallas import tpu as pltpu
from jax.sharding import PartitionSpec as P

ITERS = 3
CSWEEPS = 4
LINE_WEIGHT = 0.8
POINT_WEIGHT = 0.7
COARSE_WEIGHT = 0.7
MESH = pl.DeviceIdType.MESH
F32 = jnp.float32
BF16 = jnp.bfloat16
TOP = 8
HALO = 8
SLOT = 2 * HALO
CHUNK = 16
STEPS = ((1, 0), (-1, 0), (0, 1), (0, -1), (1, 1), (1, -1), (-1, 1), (-1, -1))
BACK = (1, 0, 3, 2, 7, 6, 5, 4)


def split(x):
    high = x.astype(BF16)
    return high, (x - high.astype(F32)).astype(BF16)


def dot(a, b, ca, cb):
    return lax.dot_general(a, b, (((ca,), (cb,)), ((), ())), preferred_element_type=F32)


def total(x):
    return jnp.sum(jnp.sum(x, axis=1, keepdims=True), axis=0, keepdims=True)


def turn(x, shift):
    flat = x.reshape(-1, x.shape[-1])
    return pltpu.roll(flat, shift % x.shape[-1], 1).reshape(x.shape)


def kernel(nx, ny, layers, cx, cy, forcing, viscosity, spread, coupling, friction, mask, aggs,
           solution, residual, *scratch):
    count = nx * ny
    gx = lax.axis_index("gx")
    gy = lax.axis_index("gy")
    me = gx * ny + gy
    (levels, (basis, stored, visc, spr, misc, ice_ext), (hit, big, point_diag, point_cross, own_sum),
     (x_out, x_in, x_send, x_recv), gathers, first_swap, right_swap, side_swap, point_swap,
     (mid_rows, col_rows), (near_out, near_in, big_near, near_send, near_recv),
     coarse_tab) = scratch
    tall = cx + 2 * HALO
    own = pl.ds(HALO, cx)
    slots = cy // SLOT
    lane = lax.broadcasted_iota(jnp.int32, (cx, cy), 1)
    row = lax.broadcasted_iota(jnp.int32, (cx, cy), 0)
    first_lane, last_lane = lane == 0, lane == cy - 1
    long_lane = lax.broadcasted_iota(jnp.int32, (tall, cy), 1)
    kept_lane = (long_lane < HALO) | (long_lane >= cy - HALO)

    exists, peers = [], []
    for dx, dy in STEPS:
        ok = []
        if dx:
            ok.append(gx < nx - 1 if dx > 0 else gx > 0)
        if dy:
            ok.append(gy < ny - 1 if dy > 0 else gy > 0)
        exists.append(ok[0] if len(ok) == 1 else jnp.logical_and(ok[0], ok[1]))
        peers.append((gx + dx, gy + dy))

    class Swap:
        def __init__(self, pieces, send, recv):
            self.pieces = pieces
            self.copies = [[pltpu.make_async_remote_copy(
                src_ref=src, dst_ref=dst, send_sem=send.at[d, i], recv_sem=recv.at[BACK[d], i],
                device_id=peers[d], device_id_type=MESH) for i, (src, dst) in enumerate(pieces[d])]
                for d in range(len(pieces))]

        def start(self, which=None):
            for d in range(len(self.copies)) if which is None else which:
                @pl.when(exists[d])
                def _():
                    for copy in self.copies[d]:
                        copy.start()

        def wait(self):
            for d in range(len(self.copies)):
                @pl.when(exists[d])
                def _():
                    for copy in self.copies[d]:
                        copy.wait_send()
                    for copy in self.copies[BACK[d]]:
                        copy.wait_recv()

        def clear(self):
            for d in range(len(self.copies)):
                @pl.when(jnp.logical_not(exists[d]))
                def _():
                    for _, ref in self.pieces[BACK[d]]:
                        ref[...] = jnp.zeros(ref.shape, F32)

    def edges(rows, packed, landed):
        low, high = pl.ds(0, HALO), pl.ds(cx - HALO, HALO)
        top, bottom = pl.ds(0, HALO), pl.ds(HALO + cx, HALO)
        return [
            [(src(cx - HALO), dst(0)) for src, dst in rows],
            [(src(0), dst(1)) for src, dst in rows],
            [(packed, landed.at[0, :, own])],
            [(packed, landed.at[1, :, own])],
            [(packed.at[:, high], landed.at[0, :, top])],
            [(packed.at[:, high], landed.at[1, :, top])],
            [(packed.at[:, low], landed.at[0, :, bottom])],
            [(packed.at[:, low], landed.at[1, :, bottom])],
        ]

    def ends(e):
        return pl.ds(0, HALO) if e == 0 else pl.ds(HALO + cx, HALO)

    class Packer:
        def __init__(self, out):
            self.out = out
            self.at = 0
            self.tile = None

        def add(self, value):
            s, m = divmod(self.at, slots)
            moved = pltpu.roll(value, (SLOT * m + HALO) % cy, 1)
            self.tile = moved if m == 0 else jnp.where(lane // SLOT == m, moved, self.tile)
            self.at += 1
            if m == slots - 1:
                self.flush(s)

        def flush(self, s):
            self.out[s] = self.tile
            self.tile = None

        def finish(self):
            if self.tile is not None:
                self.flush((self.at - 1) // slots)

    def unpack(landed, puts):
        south = long_lane % SLOT < HALO
        comb = None
        for i, put in enumerate(puts):
            s, m = divmod(i, slots)
            if m == 0:
                comb = jnp.where(south, landed[0, s], landed[1, s])
            put(jnp.where(kept_lane, pltpu.roll(comb, (cy - SLOT * m - HALO) % cy, 1), 0.0))

    chunks = [pl.ds(i * CHUNK, CHUNK) for i in range(tall // CHUNK)]
    both = (0, 1)

    class Level:
        def __init__(self, depth, refs):
            self.depth = depth
            (self.seen, self.field, self.diag, self.vert, self.side, self.cross, self.inverse, self.upper,
             self.right, self.forward, self.moved) = refs

        def put(self, p, k, t, here, value):
            self.field[p, k, t, :, here] = value
            self.seen[p, k, t, :, pl.ds(TOP + here.start, here.size)] = value * ice_ext[t, here][None]

        def sideways(self, p, k, here, tiles):
            def at(t, shift):
                return self.seen[p, k, t, :, pl.ds(TOP + here.start + shift, here.size)]

            lanes = lax.broadcasted_iota(jnp.int32, (2, here.size, cy), 2)
            value = [at(t, 0) for t in both]
            up = [turn(v, cy - 1) for v in value]
            down = [turn(v, 1) for v in value]
            outs = []
            for t in tiles:
                north = jnp.where(lanes == cy - 1, up[1 - t], up[t])
                south = jnp.where(lanes == 0, down[1 - t], down[t])
                out = self.side[k, t, here][None] * ((at(t, 1) + at(t, -1)) + (north + south))
                if k == 0:
                    crossed = self.cross[t, here]
                    out = out - jnp.stack([crossed * value[t][1], crossed * value[t][0]])
                outs.append(out)
            return outs

        def leftover(self, p, right, emit, tiles=both, spans=None):
            for here in spans or chunks:
                for k in range(self.depth):
                    outs = self.sideways(p, k, here, tiles)
                    for i, t in enumerate(tiles):
                        emit(k, t, here, (1.0 - LINE_WEIGHT) ** 2 * right(k, t, here)
                             + (outs[i] - LINE_WEIGHT * self.moved[k, t, :, here]))

        def solve(self, source, old, p, spans=None):
            for here in spans or chunks:
                last = [None, None]
                for k in range(self.depth):
                    values = source(k, here)
                    for t in both:
                        value = values[t]
                        if k > 0:
                            value = value + self.vert[k - 1, t, here][None] * last[t]
                        last[t] = value * self.inverse[k, t, here][None]
                        if k + 1 < self.depth:
                            self.forward[k, t, :, here] = last[t]
                for k in reversed(range(self.depth)):
                    for t in both:
                        if k + 1 < self.depth:
                            last[t] = self.forward[k, t, :, here] - self.upper[k, t, here][None] * last[t]
                        value = LINE_WEIGHT * last[t]
                        if old is not None:
                            value = value + (1.0 - LINE_WEIGHT) * self.field[old, k, t, :, here]
                        self.put(p, k, t, here, value)

        def first(self, right):
            self.solve(lambda k, here: [right(k, t, here) for t in both], None, 0)

        def sweep(self, p, right, keep=False, spans=None):
            def source(k, here):
                outs = self.sideways(p, k, here, both)
                if keep:
                    for t in both:
                        self.moved[k, t, :, here] = outs[t]
                return [right(k, t, here) + outs[t] for t in both]
            self.solve(source, p, 1 - p, spans)

        def factor(self):
            inverse = 1.0 / self.diag[0]
            self.inverse[0] = inverse
            for k in range(1, self.depth):
                ratio = -self.vert[k - 1] * inverse
                self.upper[k - 1] = ratio
                inverse = 1.0 / (self.diag[k] + self.vert[k - 1] * ratio)
                self.inverse[k] = inverse

        def before(self, right):
            self.first(right)
            self.sweep(0, right, True)

        def after(self, right, spans=None):
            self.sweep(0, right, spans=spans)
            self.sweep(1, right, spans=spans)

    half = layers // 2
    fine, middle, column = (Level(n, refs) for n, refs in zip((layers, half, 1), levels))
    for level in (fine, middle, column):
        for p in range(2):
            for k in range(level.depth):
                for t in both:
                    level.seen[p, k, t, :, pl.ds(0, TOP), :] = jnp.zeros((2, TOP, cy), F32)
                    level.seen[p, k, t, :, pl.ds(TOP + tall, TOP), :] = jnp.zeros((2, TOP, cy), F32)

    def rows_of(ref, at):
        return lambda start: ref.at[at + (pl.ds(start, HALO),)]

    any_k = slice(None)

    (first_pack, first_land, first_send, first_recv) = first_swap
    swap0 = Swap(edges([
        (lambda lo: viscosity.at[:, pl.ds(lo, HALO)], lambda e: visc.at[:, 0, ends(e)]),
        (lambda lo: spread.at[:, pl.ds(lo, HALO)], lambda e: spr.at[:, 0, ends(e)]),
        (lambda lo: misc.at[:, 0, pl.ds(HALO + lo, HALO)], lambda e: misc.at[:, 0, ends(e)]),
    ], first_pack, first_land), first_send, first_recv)
    (right_pack, right_land, right_send, right_recv) = right_swap

    def swap_right(j):
        return Swap(edges([(lambda lo: basis.at[j, :, :, 0, pl.ds(HALO + lo + (2 if lo else 0), HALO - 2)],
                            lambda e: basis.at[j, :, :, 0, pl.ds(2 if e == 0 else HALO + cx, HALO - 2)])],
                          right_pack, right_land), right_send, right_recv)

    (side_pack, side_land, side_send, side_recv) = side_swap
    swap_side = Swap(edges([
        (lambda lo: middle.field.at[1, :, 0, :, pl.ds(HALO + lo, HALO)], lambda e: mid_rows.at[e]),
        (lambda lo: column.field.at[1, 0, 0, :, pl.ds(HALO + lo, HALO)], lambda e: col_rows.at[e, 0]),
        (lambda lo: column.right.at[0, 0, :, pl.ds(HALO + lo, HALO)], lambda e: col_rows.at[e, 1]),
    ], side_pack, side_land), side_send, side_recv)
    (far_out, far_in, far_send, far_recv) = point_swap
    swap_far = Swap([[(far_out, far_in.at[d])] for d in range(8)], far_send, far_recv)

    swap_near = Swap([[(near_out, near_in.at[d])] for d in range(4)], near_send, near_recv)

    def near_swap(p, q):
        return Swap([[(x_out.at[p], x_in.at[q, d])] for d in range(4)], x_send.at[p], x_recv.at[q])

    misc[0, 0, own] = mask[...].astype(F32)
    misc[1, 0, own] = aggs[...].astype(F32)
    misc[2, 0, own] = friction[...]
    misc[3, 0, own] = coupling[...]
    swap0.start((0, 1))
    packer = Packer(first_pack)
    for i in range(4):
        packer.add(misc[i, 0, own])
    for k in range(layers):
        packer.add(viscosity[k])
        packer.add(spread[k])
    packer.finish()
    swap0.start(range(2, 8))
    packer = Packer(right_pack)
    for k in range(layers):
        basis[0, :, k, 0, own] = forcing[:, k]
        for v in range(2):
            packer.add(forcing[v, k])
    packer.finish()
    swap_right(0).start()
    for j in range(ITERS):
        swap_right(j).clear()
        for k in range(layers):
            basis[j, :, k, 0, 0:HALO - 6] = jnp.zeros((2, HALO - 6, cy), F32)
            basis[j, :, k, 0, tall - HALO + 6:tall] = jnp.zeros((2, HALO - 6, cy), F32)
    swap0.clear()
    swap_side.clear()
    swap_far.clear()
    for q in range(2):
        near_swap(0, q).clear()
    swap_near.clear()
    for k in range(layers):
        visc[k, 0, own] = viscosity[k]
        spr[k, 0, own] = spread[k]

    def gather(which, slot=0):
        out, into, send, recv = gathers[which]
        into, recv = into.at[slot], recv.at[slot]
        rest = into.at[pl.ds(0, count - 1)]

        def start():
            def step(i, carry):
                target = lax.rem(me + i, count)
                pltpu.make_async_remote_copy(
                    src_ref=out, dst_ref=into.at[me], send_sem=send, recv_sem=recv,
                    device_id=(target // ny, lax.rem(target, ny)), device_id_type=MESH).start()
                return carry

            lax.fori_loop(1, count, step, 0)
            into[me] = out[...]

        def wait():
            pltpu.make_async_copy(rest, rest, recv).wait()
            pltpu.make_async_copy(rest, rest, send).wait()

        return start, wait

    wide = lax.broadcasted_iota(jnp.int32, (1, cy), 1)

    def reduce_all(parts):
        line = jnp.zeros((1, cy), F32)
        for i, part in enumerate(parts):
            line = jnp.where(wide == i, part, line)
        gathers[1][0][...] = line
        start, wait = gather(1)
        start()
        wait()
        return jnp.sum(gathers[1][1][0, :, 0, :], axis=0, keepdims=True)

    def pick(line, i):
        return jnp.sum(jnp.where(wide == i, line, 0.0), axis=1, keepdims=True)

    def put_to(ref, *at):
        def put(value):
            ref[at] = value
        return put

    ids = aggs[...]
    ice_own = mask[...].astype(F32)
    down = lax.broadcasted_iota(jnp.int32, (cy, cy), 0)
    across = lax.broadcasted_iota(jnp.int32, (cy, cy), 1)
    spots = [pl.ds(r * cy, cy) for r in range(cx)]
    for r in range(cx):
        hit[:, spots[r]] = jnp.where(ids[r:r + 1, :] == down, 1.0, 0.0).astype(BF16)
    flow = sum(spread[k] for k in range(layers))
    cross2 = friction[...] * coupling[...] * ice_own
    diag2 = ice_own * (4.0 * flow + friction[...]) + layers * (1.0 - ice_own)
    flow = flow * ice_own
    ahead = jnp.where(lane < cy - 1, flow * pltpu.roll(ice_own, cy - 1, 1), 0.0)
    behind = jnp.where(lane > 0, flow * pltpu.roll(ice_own, 1, 1), 0.0)
    near = jnp.zeros((cy, cy), F32)
    for r in range(cx):
        here = hit[:, spots[r]].astype(F32)
        term = diag2[r:r + 1, :] * here
        if r + 1 < cx:
            term = term - flow[r:r + 1, :] * ice_own[r + 1:r + 2, :] * hit[:, spots[r + 1]].astype(F32)
        if r > 0:
            term = term - flow[r:r + 1, :] * ice_own[r - 1:r, :] * hit[:, spots[r - 1]].astype(F32)
        term = term - ahead[r:r + 1, :] * pltpu.roll(here, cy - 1, 1)
        term = term - behind[r:r + 1, :] * pltpu.roll(here, 1, 1)
        high, low = split(term)
        near = near + dot(high, hit[:, spots[r]], 1, 1) + dot(low, hit[:, spots[r]], 1, 1)
    point_diag[...] = jnp.sum(jnp.where(down == across, near, 0.0), axis=0, keepdims=True)
    tall4 = lax.broadcasted_iota(jnp.int32, (4 * cx, cy), 0) % cx

    def restrict_points(first, second):
        h0, l0 = split(first)
        h1, l1 = split(second)
        left = jnp.concatenate([h0, h1, l0, l1], axis=0)
        left = jnp.concatenate([jnp.where(tall4 == r, left, jnp.zeros_like(left)) for r in range(cx)], axis=1)
        out = dot(left, hit[...], 1, 1)
        parts = [jnp.sum(out[i * cx:(i + 1) * cx] + out[(i + 2) * cx:(i + 3) * cx], axis=0, keepdims=True)
                 for i in range(2)]
        return jnp.concatenate(parts, axis=0)

    point_cross[...] = restrict_points(cross2, cross2)

    swap0.wait()
    puts = [put_to(misc, i, 1) for i in range(4)]
    for k in range(layers):
        puts += [put_to(visc, k, 1), put_to(spr, k, 1)]
    unpack(first_land, puts)

    ids_all = [misc[1, t].astype(jnp.int32) for t in both]
    ice = [misc[0, t] for t in both]
    for t in both:
        ice_ext[t] = ice[t]
        column.seen[1, 0, t, 0, pl.ds(TOP, tall), :] = ice[t]
    around = []
    ups = [turn(x, cy - 1) for x in ice]
    downs = [turn(x, 1) for x in ice]
    for t in both:
        around.append((column.seen[1, 0, t, 0, pl.ds(TOP + 1, tall), :],
                       column.seen[1, 0, t, 0, pl.ds(TOP - 1, tall), :],
                       jnp.where(long_lane == cy - 1, ups[1 - t], ups[t]),
                       jnp.where(long_lane == 0, downs[1 - t], downs[t])))
    for k in range(layers):
        for t in both:
            owned = spr[k, t]
            faces = 4.0 * owned
            if k + 1 < layers:
                face = 0.5 * (visc[k, t] + visc[k + 1, t]) * ice[t]
                fine.vert[k, t] = face
                faces = faces + face
            if k > 0:
                faces = faces + fine.vert[k - 1, t]
            if k == 0:
                faces = faces + misc[2, t]
            fine.diag[k, t] = ice[t] * faces + (1.0 - ice[t])
            fine.side[k, t] = owned * ice[t]
    for t in both:
        fine.cross[t] = misc[2, t] * misc[3, t] * ice[t]
    for finer, coarser in ((fine, middle), (middle, column)):
        size = finer.depth // coarser.depth
        for k in range(coarser.depth):
            group = range(k * size, (k + 1) * size)
            diag = sum(finer.diag[j] for j in group)
            inner_faces = sum(finer.vert[j] for j in list(group)[:-1])
            coarser.diag[k] = diag - 2.0 * inner_faces
            if k + 1 < coarser.depth:
                coarser.vert[k] = finer.vert[group[-1]]
            coarser.side[k] = sum(finer.side[j] for j in group)
        coarser.cross[...] = finer.cross[...]

    side2 = [column.side[0, 0, own] * around[0][d][HALO:HALO + cx] for d in range(4)]
    inner = (diag2 - jnp.where(row < cx - 1, side2[0], 0.0) - jnp.where(row > 0, side2[1], 0.0)
             - jnp.where(lane < cy - 1, side2[2], 0.0) - jnp.where(lane > 0, side2[3], 0.0))
    entries = (inner, cross2, jnp.where(row == cx - 1, side2[0], 0.0), jnp.where(row == 0, side2[1], 0.0),
               jnp.where(last_lane, side2[2], 0.0), jnp.where(first_lane, side2[3], 0.0))
    eight = lax.broadcasted_iota(jnp.int32, (8, cy), 0)
    tile = jnp.zeros((8, cy), F32)
    for i, entry in enumerate(entries):
        tile = jnp.where(eight == i, total(entry), tile)
    gathers[2][0][...] = tile
    tables_start, tables_wait = gather(2)
    tables_start()
    for level in (fine, middle, column):
        level.factor()

    tables = [near]
    for d, r, e in ((0, cx - 1, HALO + cx), (1, 0, HALO - 1)):
        other = ids_all[0][e:e + 1, :]
        term = jnp.where(other == down, side2[d][r:r + 1, :], 0.0)
        high, low = split(term)
        tables.append(-(dot(high, hit[:, spots[r]], 1, 1) + dot(low, hit[:, spots[r]], 1, 1)))
    for d, q, e in ((2, cy - 1, 0), (3, 0, cy - 1)):
        other = ids_all[1][HALO:HALO + cx, e:e + 1]
        term = jnp.where(other == lane, side2[d][:, q:q + 1], 0.0)
        here = jnp.where(ids[:, q:q + 1] == lane, 1.0, 0.0)
        high, low = split(term)
        here = here.astype(BF16)
        tables.append(-(dot(high, here, 0, 0) + dot(low, here, 0, 0)))
    for i, table in enumerate(tables):
        big[i * cy:(i + 1) * cy, 0:cy], big[i * cy:(i + 1) * cy, cy:2 * cy] = split(table)

    scale = POINT_WEIGHT / point_diag[...]
    ones = jnp.ones((8, 2 * cy), BF16)
    sixteen = lax.broadcasted_iota(jnp.int32, (16, cy), 0)
    sent = jnp.where(sixteen == 5, scale * point_cross[0:1, :], 0.0)
    for i, table in enumerate(tables):
        sent = jnp.where(sixteen == i, scale * jnp.sum(table, axis=0, keepdims=True), sent)
        part = big[i * cy:(i + 1) * cy]
        across_sum = dot(ones, part, 1, 1)[0:1, :]
        if i == 0:
            own_sum[...] = across_sum
        else:
            sent = jnp.where(sixteen == 5 + i, across_sum, sent)
    sent = jnp.where(sixteen == 10, scale, sent)
    near_out[0:16] = sent
    edge_rows = jnp.zeros((8, cy), F32)
    for i, (r, e) in enumerate(((cx - 1, HALO + cx), (0, HALO - 1))):
        for n, line in enumerate((misc[1, 0, HALO + r:HALO + r + 1], misc[1, 0, e:e + 1], side2[i][r:r + 1])):
            edge_rows = jnp.where(eight == 3 * i + n, line, edge_rows)
    near_out[16:24] = edge_rows
    edge_cols = jnp.zeros((cx, cy), F32)
    for i, (q, e) in enumerate(((cy - 1, 0), (0, cy - 1))):
        for n, line in enumerate((misc[1, 0, own, q:q + 1], misc[1, 1, own, e:e + 1], side2[2 + i][:, q:q + 1])):
            edge_cols = jnp.where(lane == 3 * i + n, line, edge_cols)
    near_out[24:24 + cx] = edge_cols
    near_out[24 + cx:24 + cx + cy] = near
    swap_near.start()

    def build_near():
        swap_near.wait()
        down_f, lane_f = down.astype(F32), lane.astype(F32)

        def step(m, carry):
            rows, cols = near_in[m, 16:24], near_in[m, 24:24 + cx]
            found = [near_in[m, 24 + cx:24 + cx + cy]]
            for i in range(2):
                there = jnp.where(rows[3 * i:3 * i + 1] == down_f, 1.0, 0.0).astype(BF16)
                high, low = split(jnp.where(rows[3 * i + 1:3 * i + 2] == down_f, rows[3 * i + 2:3 * i + 3], 0.0))
                found.append(-(dot(high, there, 1, 1) + dot(low, there, 1, 1)))
            for i in range(2):
                there = jnp.where(cols[:, 3 * i:3 * i + 1] == lane_f, 1.0, 0.0).astype(BF16)
                high, low = split(jnp.where(cols[:, 3 * i + 1:3 * i + 2] == lane_f, cols[:, 3 * i + 2:3 * i + 3], 0.0))
                found.append(-(dot(high, there, 0, 0) + dot(low, there, 0, 0)))
            for i, table in enumerate(found):
                big_near[m, i * cy:(i + 1) * cy, 0:cy], big_near[m, i * cy:(i + 1) * cy, cy:2 * cy] = split(table)
            return carry

        lax.fori_loop(0, 4, step, 0)

    block_row = lax.broadcasted_iota(jnp.int32, (count, cy), 0)
    coarse_lane = lax.broadcasted_iota(jnp.int32, (count, cy), 1)
    shifts = (ny, count - ny, 1, count - 1)

    def coarse_begin(j, right, x):
        lines = [right - own_sum[...] * x - point_cross[...] * jnp.concatenate([x[1:2], x[0:1]], axis=0)]
        for d in range(4):
            lines.append(-near_in[BACK[d], 6 + BACK[d]:7 + BACK[d], :] * x)
        line = jnp.zeros((1, cy), F32)
        for i, part in enumerate(lines):
            sums = jnp.sum(part, axis=1, keepdims=True)
            for v in range(2):
                line = jnp.where(wide == 2 * i + v, sums[v:v + 1], line)
        gathers[0][0][0:2] = x
        gathers[0][0][2:3] = line
        start, wait = gather(0, lax.rem(j, 2))
        start()
        return wait

    def coarse_end(j, wait):
        @pl.when(j == 0)
        def _():
            tables_wait()
            for i in range(6):
                coarse_tab[i] = gathers[2][1][0, :, i, :]
            coarse_tab[6] = COARSE_WEIGHT / coarse_tab[0]
        wait()
        came = gathers[0][1][lax.rem(j, 2), :, 2, :]
        right = came
        for d in range(4):
            right = right + pltpu.roll(pltpu.roll(came, shifts[d], 0), cy - 2 - 2 * d, 1)
        diag, crossed, east, west, north, south, weight = (coarse_tab[i] for i in range(7))
        answer = right * weight
        for _ in range(CSWEEPS - 1):
            other = jnp.where(coarse_lane % 2 == 0, pltpu.roll(answer, cy - 1, 1), pltpu.roll(answer, 1, 1))
            applied = diag * answer + crossed * other - (
                east * pltpu.roll(answer, count - ny, 0) + west * pltpu.roll(answer, ny, 0)
                + north * pltpu.roll(answer, count - 1, 0) + south * pltpu.roll(answer, 1, 0))
            answer = answer + (right - applied) * weight
        hops = ((0, 0),) + STEPS[:4]
        known = {}

        def value(dx, dy):
            if (dx, dy) not in known:
                line = jnp.sum(jnp.where(block_row == me + dx * ny + dy, answer, 0.0), axis=0, keepdims=True)
                known[dx, dy] = jnp.concatenate([line[:, 0:1], line[:, 1:2]], axis=0)
            return known[dx, dy]

        found = []
        for i, (dx, dy) in enumerate(hops):
            here = value(dx, dy)
            rows = near_out if i == 0 else near_in.at[BACK[i - 1]]
            out = here - rows[5:6, :] * jnp.concatenate([here[1:2], here[0:1]], axis=0)
            for n, (ex, ey) in enumerate(hops):
                out = out - rows[n:n + 1, :] * value(dx + ex, dy + ey)
            found.append(out)
        return found

    def swapped(x):
        return jnp.concatenate([x[1:2], x[0:1]], axis=0)

    def apply_tables(table, xs):
        parts = [split(x) for x in xs]
        left = jnp.concatenate([jnp.concatenate([p[i] for p in parts], axis=1) for i in range(2)], axis=0)
        both_parts = dot(left, table[...], 1, 0)
        both_parts = both_parts[0:2] + both_parts[2:4]
        return both_parts[:, 0:cy] + both_parts[:, cy:2 * cy]

    def point_apply(xs):
        return point_cross[...] * swapped(xs[0]) + apply_tables(big, xs)

    def point_cycle(j, right):
        x_out[0] = right * (POINT_WEIGHT / point_diag[...])
        swap = near_swap(0, 0)
        swap.start()
        packer = Packer(side_pack)
        for v in range(2):
            packer.add(column.field[1, 0, 0, v, own])
            packer.add(column.right[0, 0, v, own])
        for k in range(half):
            for v in range(2):
                packer.add(middle.field[1, k, 0, v, own])
        packer.finish()
        swap_side.start()
        pl.when(j == 0)(build_near)
        scale = POINT_WEIGHT / point_diag[...]
        swap.wait()
        first = [right * scale] + [x_in[0, BACK[d]] for d in range(4)]
        x = first[0] + (right - point_apply(first)) * scale
        coarse_wait = coarse_begin(j, right, x)
        merge_side()
        found = coarse_end(j, coarse_wait)
        hops = ((0, 0),) + STEPS[:4]

        def second(dx, dy):
            return gathers[0][1][lax.rem(j, 2), lax.rem(me + dx * ny + dy + count, count), 0:2]

        xs = []
        for i, (dx, dy) in enumerate(hops):
            local = [second(dx + ex, dy + ey) for ex, ey in hops]
            if i == 0:
                moved = point_apply(local) * scale
            else:
                rows = near_in.at[BACK[i - 1]]
                moved = (rows[10:11] * apply_tables(big_near.at[BACK[i - 1]], local)
                         + rows[5:6] * swapped(local[0]))
            xs.append(local[0] + first[i] - moved + found[i])
        return xs[0] + (right - point_apply(xs)) * scale

    def merge_side():
        swap_side.wait()
        column.field[0, 0, 0] = jnp.concatenate([col_rows[0, 0], column.field[1, 0, 0, :, own], col_rows[1, 0]], axis=1)
        for e in range(2):
            column.right[0, 0, :, ends(e)] = col_rows[e, 1]
        for k in range(half):
            middle.field[0, k, 0] = jnp.concatenate([mid_rows[0, k], middle.field[1, k, 0, :, own], mid_rows[1, k]],
                                                    axis=1)
        puts = []
        for v in range(2):
            puts += [put_to(column.field, 0, 0, 1, v), put_to(column.right, 0, 1, v)]
        for k in range(half):
            puts += [put_to(middle.field, 0, k, 1, v) for v in range(2)]
        unpack(side_land, puts)

    def spread_points(x):
        far_out[...] = x
        swap_far.start()
        swap_far.wait()
        parts = [[], []]
        zones = ((pl.ds(0, HALO), 1, 6, 7), (own, None, 2, 3), (pl.ds(HALO + cx, HALO), 0, 4, 5))
        short = {n: lax.broadcasted_iota(jnp.int32, (n, cy), 1) < cy // 2 for n in (HALO, cx)}

        def take(src, v, index):
            values = x if src is None else far_in[BACK[src]]
            return jnp.take_along_axis(jnp.broadcast_to(values[v:v + 1], index.shape), index, axis=1,
                                       mode="promise_in_bounds")

        for rows, straight, right, left in zones:
            index = [misc[1, t, rows].astype(jnp.int32) for t in both]
            parts[0].append(jnp.stack([take(straight, v, index[0]) for v in range(2)]))
            lanes = short[index[1].shape[0]]
            parts[1].append(jnp.stack([jnp.where(lanes, take(right, v, index[1]), take(left, v, index[1]))
                                       for v in range(2)]))
        return [jnp.concatenate(p, axis=1) for p in parts]

    def iteration(j, carry):
        def right0(k, t, here):
            return basis[j, :, k, t, here]

        def right1(k, t, here):
            return middle.right[k, t, :, here]

        def right2(k, t, here):
            return column.right[k, t, :, here]

        def collect(coarser, size):
            held = {}

            def emit(k, t, here, value):
                held[t] = held[t] + value if k % size else value
                if k % size == size - 1:
                    coarser.right[k // size, t, :, here] = held[t]
            return emit

        swap_right(j).wait()
        unpack(right_land, [put_to(basis, j, v, k, 1) for k in range(layers) for v in range(2)])
        fine.before(right0)
        fine.leftover(1, right0, collect(middle, 2))
        middle.before(right1)
        middle.leftover(1, right1, collect(column, half))
        column.before(right2)
        kept = []
        column.leftover(1, right2, lambda k, t, here, value: kept.append(value), (0,), (own,))
        found = spread_points(point_cycle(j, restrict_points(kept[0][0], kept[0][1])))

        whole = pl.ds(0, tall)
        for t in both:
            column.put(0, 0, t, whole, found[t] + column.field[0, 0, t])
        column.after(right2)
        for k in range(half):
            for t in both:
                middle.put(0, k, t, whole, column.field[0, 0, t] + middle.field[0, k, t])
        middle.after(right1)
        for k in range(layers):
            for t in both:
                fine.put(0, k, t, whole, fine.field[1, k, t] + middle.field[0, k // 2, t])
        fine.after(right0, [pl.ds(HALO // 2 + i * 8, 8) for i in range(cx // 8 + 1)])

        packer = Packer(right_pack)

        for k in range(layers):
            here = fine.field[0, k, 0, :, own]
            stored[j, :, k] = here
            out = fine.sideways(0, k, own, (0,))[0] - fine.diag[k, 0, own][None] * here
            if k + 1 < layers:
                out = out + fine.vert[k, 0, own][None] * fine.field[0, k + 1, 0, :, own]
            if k > 0:
                out = out + fine.vert[k - 1, 0, own][None] * fine.field[0, k - 1, 0, :, own]
            value = basis[j, :, k, 0, own] + out
            basis[j + 1, :, k, 0, own] = value
            for v in range(2):
                packer.add(value[v])
        packer.finish()

        @pl.when(j < ITERS - 1)
        def _():
            swap_right(j + 1).start()
        return carry

    lax.fori_loop(0, ITERS, iteration, 0)

    names = [(i, j) for i in range(ITERS + 1) for j in range(i, ITERS + 1)]
    sums = {name: jnp.zeros((cx, cy), F32) for name in names}
    for k in range(layers):
        chain = [basis[i, :, k, 0, own] for i in range(ITERS + 1)]
        terms = [chain[j] - chain[j + 1] for j in range(ITERS)] + [chain[0]]
        for i, j in names:
            prod = terms[i] * terms[j]
            sums[i, j] = sums[i, j] + prod[0] + prod[1]
    line = reduce_all([total(sums[name]) for name in names])
    gram = {name: pick(line, at) for at, name in enumerate(names)}
    rows = [[gram[min(i, j), max(i, j)] for j in range(ITERS + 1)] for i in range(ITERS)]
    for a in range(ITERS):
        for i in range(a + 1, ITERS):
            share = rows[i][a] / rows[a][a]
            for c in range(a, ITERS + 1):
                rows[i][c] = rows[i][c] - share * rows[a][c]
    weights = [None] * ITERS
    for a in reversed(range(ITERS)):
        part = rows[a][ITERS]
        for c in range(a + 1, ITERS):
            part = part - rows[a][c] * weights[c]
        weights[a] = part / rows[a][a]
    for k in range(layers):
        out = weights[0] * stored[0, :, k]
        rest = forcing[:, k] - weights[0] * (basis[0, :, k, 0, own] - basis[1, :, k, 0, own])
        for j in range(1, ITERS):
            out = out + weights[j] * stored[j, :, k]
            rest = rest - weights[j] * (basis[j, :, k, 0, own] - basis[j + 1, :, k, 0, own])
        for v in range(2):
            solution[pl.ds((v * layers + k) * cx, cx)] = out[v]
            residual[pl.ds((v * layers + k) * cx, cx)] = rest[v]


def solution(mesh):
    nx, ny = mesh.shape["gx"], mesh.shape["gy"]
    count = nx * ny

    def body(forcing, viscosity, spread, coupling, friction, mask, aggs):
        layers, cx, cy = forcing.shape[1:]
        dma = pltpu.SemaphoreType.DMA
        tall = cx + 2 * HALO
        half = layers // 2

        def vm(*shape, dtype=F32):
            return pltpu.VMEM(shape, dtype)

        def level(n):
            return (
                vm(2, n, 2, 2, tall + 2 * TOP, cy), vm(2, n, 2, 2, tall, cy),
                vm(n, 2, tall, cy), vm(n, 2, tall, cy), vm(n, 2, tall, cy), vm(2, tall, cy),
                vm(n, 2, tall, cy), vm(n, 2, tall, cy), vm(n, 2, 2, tall, cy), vm(n, 2, 2, tall, cy),
                vm(n, 2, 2, tall, cy),
            )

        def swap(planes, pieces):
            tiles = -(-planes * SLOT // cy)
            return (vm(tiles, cx, cy), vm(2, tiles, tall, cy), dma((8, pieces)), dma((8, pieces)))

        scratch = (
            (level(layers), level(half), level(1)),
            (vm(ITERS + 1, 2, layers, 2, tall, cy), vm(ITERS, 2, layers, cx, cy),
             vm(layers, 2, tall, cy), vm(layers, 2, tall, cy), vm(4, 2, tall, cy), vm(2, tall, cy)),
            (vm(cy, cx * cy, dtype=BF16), vm(5 * cy, 2 * cy, dtype=BF16),
             vm(1, cy), vm(2, cy), vm(1, cy)),
            (vm(2, 2, cy), vm(2, 4, 2, cy), dma((2, 4, 1)), dma((2, 4, 1))),
            tuple((vm(n, cy), vm(2, count, n, cy), dma(()), dma((2,))) for n in (3, 1, 8)),
            swap(4 + 2 * layers, 3),
            swap(2 * layers, 1),
            swap(4 + 2 * half, 3),
            (vm(2, cy), vm(8, 2, cy), dma((8, 1)), dma((8, 1))),
            (vm(2, half, 2, HALO, cy), vm(2, 2, 2, HALO, cy)),
            (vm(24 + cx + cy, cy), vm(4, 24 + cx + cy, cy), vm(4, 5 * cy, 2 * cy, dtype=BF16), dma((4, 1)), dma((4, 1))),
            vm(7, count, cy),
        )
        flat, tree = jax.tree.flatten(scratch)

        def run(*refs):
            kernel(nx, ny, layers, cx, cy, *refs[:9], *jax.tree.unflatten(tree, refs[9:]))

        shape = jax.ShapeDtypeStruct((2 * layers * cx, cy), F32)
        whole = pl.BlockSpec(memory_space=pltpu.VMEM)
        outs = pl.pallas_call(
            run,
            out_shape=(shape, shape),
            in_specs=[whole] * 7,
            out_specs=(whole, whole),
            scratch_shapes=flat,
            compiler_params=pltpu.CompilerParams(has_side_effects=True, vmem_limit_bytes=60 * 1024 * 1024),
        )(forcing, viscosity, spread, coupling, friction, mask, aggs)
        return tuple(out.reshape(forcing.shape) for out in outs)

    return jax.shard_map(
        body,
        mesh=mesh,
        in_specs=(
            P(None, None, "gx", "gy"),
            P(None, "gx", "gy"),
            P(None, "gx", "gy"),
            P("gx", "gy"),
            P("gx", "gy"),
            P("gx", "gy"),
            P("gx", "gy"),
        ),
        out_specs=(P(None, None, "gx", "gy"), P(None, None, "gx", "gy")),
        check_vma=False,
    )
```

```python
import jax
import jax.numpy as jnp
from jax import lax
from jax.experimental import pallas as pl
from jax.experimental.pallas import tpu as pltpu
from jax.sharding import PartitionSpec as P

ITERS = 3
CSWEEPS = 4
LINE_WEIGHT = 0.8
POINT_WEIGHT = 0.7
COARSE_WEIGHT = 0.7
MESH = pl.DeviceIdType.MESH
F32 = jnp.float32
BF16 = jnp.bfloat16
TOP = 8
HALO = 8
CHUNK = 16
INNER = 8
STEPS = ((1, 0), (-1, 0), (0, 1), (0, -1), (1, 1), (1, -1), (-1, 1), (-1, -1))
BACK = (1, 0, 3, 2, 7, 6, 5, 4)


def split(x):
    high = x.astype(BF16)
    return high, (x - high.astype(F32)).astype(BF16)


def dot(a, b, ca, cb):
    return lax.dot_general(a, b, (((ca,), (cb,)), ((), ())), preferred_element_type=F32)


def total(x):
    return jnp.sum(jnp.sum(x, axis=1, keepdims=True), axis=0, keepdims=True)


def turn(x, shift):
    flat = x.reshape(-1, x.shape[-1])
    return pltpu.roll(flat, shift % x.shape[-1], 1).reshape(x.shape)


def kernel(nx, ny, layers, cx, cy, forcing, viscosity, spread, coupling, friction, mask, aggs,
           result, *scratch):
    count = nx * ny
    gx = lax.axis_index("gx")
    gy = lax.axis_index("gy")
    me = gx * ny + gy
    (levels, (basis, stored, visc, spr, misc, ice_ext), (hit, big, point_diag, point_cross, own_sum),
     (x_out, x_in, x_send, x_recv), gathers, first_swap, right_swap, side_swap, point_swap,
     (mid_rows, col_rows), (near_out, near_in, big_near, near_send, near_recv),
     coarse_tab, lift_side, lift_cross) = scratch
    tall = cx + 2 * HALO
    own = pl.ds(HALO, cx)
    slots = cy // HALO
    lane = lax.broadcasted_iota(jnp.int32, (cx, cy), 1)
    row = lax.broadcasted_iota(jnp.int32, (cx, cy), 0)
    first_lane, last_lane = lane == 0, lane == cy - 1
    long_lane = lax.broadcasted_iota(jnp.int32, (tall, cy), 1)
    kept_lane = (long_lane < HALO) | (long_lane >= cy - HALO)

    exists, peers = [], []
    for dx, dy in STEPS:
        ok = []
        if dx:
            ok.append(gx < nx - 1 if dx > 0 else gx > 0)
        if dy:
            ok.append(gy < ny - 1 if dy > 0 else gy > 0)
        exists.append(ok[0] if len(ok) == 1 else jnp.logical_and(ok[0], ok[1]))
        peers.append((gx + dx, gy + dy))

    class Swap:
        def __init__(self, pieces, send, recv):
            self.pieces = pieces
            self.copies = [[pltpu.make_async_remote_copy(
                src_ref=src, dst_ref=dst, send_sem=send.at[d, i], recv_sem=recv.at[BACK[d], i],
                device_id=peers[d], device_id_type=MESH) for i, (src, dst) in enumerate(pieces[d])]
                for d in range(len(pieces))]

        def start(self, which=None):
            for d in range(len(self.copies)) if which is None else which:
                @pl.when(exists[d])
                def _():
                    for copy in self.copies[d]:
                        copy.start()

        def wait(self):
            for d in range(len(self.copies)):
                @pl.when(exists[d])
                def _():
                    for copy in self.copies[d]:
                        copy.wait_send()
                    for copy in self.copies[BACK[d]]:
                        copy.wait_recv()

        def clear(self):
            for d in range(len(self.copies)):
                @pl.when(jnp.logical_not(exists[d]))
                def _():
                    for _, ref in self.pieces[BACK[d]]:
                        ref[...] = jnp.zeros(ref.shape, F32)

    def edges(rows, packed, landed):
        low, high = pl.ds(0, HALO), pl.ds(cx - HALO, HALO)
        top, bottom = pl.ds(0, HALO), pl.ds(HALO + cx, HALO)
        return [
            [(src(cx - HALO), dst(0)) for src, dst in rows],
            [(src(0), dst(1)) for src, dst in rows],
            [(packed.at[0], landed.at[0, :, own])],
            [(packed.at[1], landed.at[1, :, own])],
            [(packed.at[0, :, high], landed.at[0, :, top])],
            [(packed.at[1, :, high], landed.at[1, :, top])],
            [(packed.at[0, :, low], landed.at[0, :, bottom])],
            [(packed.at[1, :, low], landed.at[1, :, bottom])],
        ]

    def ends(e):
        return pl.ds(0, HALO) if e == 0 else pl.ds(HALO + cx, HALO)

    class Packer:
        def __init__(self, out):
            self.out = out
            self.at = 0
            self.tiles = None

        def add(self, value):
            s, m = divmod(self.at, slots)
            moved = pltpu.roll(value, (HALO * m + HALO) % cy, 1)
            self.tiles = [moved] * 2 if m == 0 else [
                jnp.where(lane // HALO == (m + i) % slots, moved, self.tiles[i]) for i in range(2)]
            self.at += 1
            if m == slots - 1:
                self.flush(s)

        def flush(self, s):
            for i in range(2):
                self.out[i, s] = self.tiles[i]
            self.tiles = None

        def finish(self):
            if self.tiles is not None:
                self.flush((self.at - 1) // slots)

    def unpack(landed, puts):
        south = long_lane // HALO % 2 == 0
        comb = None
        for i, put in enumerate(puts):
            s, m = divmod(i, slots)
            if m == 0:
                comb = [jnp.where(south, landed[e, s], landed[1 - e, s]) for e in range(2)]
            put(jnp.where(kept_lane, pltpu.roll(comb[m % 2], (2 * cy - HALO * m - HALO) % cy, 1), 0.0))

    chunks = [pl.ds(i * CHUNK, CHUNK) for i in range(tall // CHUNK)]
    both = (0, 1)

    class Level:
        def __init__(self, depth, refs):
            self.depth = depth
            (self.seen, self.field, self.diag, self.vert, self.side, self.cross, self.inverse, self.upper,
             self.right, self.forward, self.moved) = refs

        def put(self, p, k, t, here, value):
            self.field[p, k, t, :, here] = value
            self.seen[p, k, t, :, pl.ds(TOP + here.start, here.size)] = value * ice_ext[t, here][None]

        def sums(self, p, k, here, tiles):
            def at(t, shift):
                return self.seen[p, k, t, :, pl.ds(TOP + here.start + shift, here.size)]

            lanes = lax.broadcasted_iota(jnp.int32, (2, here.size, cy), 2)
            value = [at(t, 0) for t in both]
            up = [turn(v, cy - 1) for v in value]
            down = [turn(v, 1) for v in value]
            outs = []
            for t in tiles:
                north = jnp.where(lanes == cy - 1, up[1 - t], up[t])
                south = jnp.where(lanes == 0, down[1 - t], down[t])
                outs.append((at(t, 1) + at(t, -1)) + (north + south))
            return value, outs

        def sideways(self, k, here, tiles, value, outs):
            outs = [self.side[k, t, here][None] * out for t, out in zip(tiles, outs)]
            if k == 0:
                for i, t in enumerate(tiles):
                    crossed = self.cross[t, here]
                    outs[i] = outs[i] - jnp.stack([crossed * value[t][1], crossed * value[t][0]])
            return outs

        def beside(self, p, k, here, tiles):
            return self.sideways(k, here, tiles, *self.sums(p, k, here, tiles))

        def leftover(self, p, right, emit, tiles=both, spans=None):
            for here in spans or chunks:
                for k in range(self.depth):
                    outs = self.beside(p, k, here, tiles)
                    for i, t in enumerate(tiles):
                        emit(k, t, here, (1.0 - LINE_WEIGHT) ** 2 * right(k, t, here)
                             + (outs[i] - LINE_WEIGHT * self.moved[k, t, :, here]))

        def solve(self, source, finish, spans):
            for here in spans or chunks:
                last = [None, None]
                for k in range(self.depth):
                    values = source(k, here)
                    for t in both:
                        value = values[t]
                        if k > 0:
                            value = value + self.vert[k - 1, t, here][None] * last[t]
                        last[t] = value * self.inverse[k, t, here][None]
                        if k + 1 < self.depth:
                            self.forward[k, t, :, here] = last[t]
                for k in reversed(range(self.depth)):
                    for t in both:
                        if k + 1 < self.depth:
                            last[t] = self.forward[k, t, :, here] - self.upper[k, t, here][None] * last[t]
                        finish(k, t, here, LINE_WEIGHT * last[t])

        def first(self, right, spans=None):
            self.solve(lambda k, here: [right(k, t, here) for t in both],
                       lambda k, t, here, value: self.put(0, k, t, here, value), spans)

        def sweep(self, p, right, keep=False, spans=None, plain=False):
            def source(k, here):
                outs = self.beside(p, k, here, both)
                if keep:
                    for t in both:
                        self.moved[k, t, :, here] = outs[t]
                return [right(k, t, here) + outs[t] for t in both]

            def finish(k, t, here, value):
                value = value + (1.0 - LINE_WEIGHT) * self.field[p, k, t, :, here]
                if plain:
                    self.field[1 - p, k, t, :, here] = value
                else:
                    self.put(1 - p, k, t, here, value)
            self.solve(source, finish, spans)

        def factor(self):
            inverse = 1.0 / self.diag[0]
            self.inverse[0] = inverse
            for k in range(1, self.depth):
                ratio = -self.vert[k - 1] * inverse
                self.upper[k - 1] = ratio
                inverse = 1.0 / (self.diag[k] + self.vert[k - 1] * ratio)
                self.inverse[k] = inverse

        def before(self, right, spans=None):
            self.first(right, spans)
            self.sweep(0, right, True, spans)

    inside = [pl.ds(HALO // 2 + i * INNER, INNER) for i in range((cx + HALO) // INNER)]
    half = layers // 2
    fine, middle, column = (Level(n, refs) for n, refs in zip((layers, half, 1), levels))
    for level in (fine, middle, column):
        for p in range(2):
            for k in range(level.depth):
                for t in both:
                    level.seen[p, k, t, :, 0:TOP + HALO] = jnp.zeros((2, TOP + HALO, cy), F32)
                    level.seen[p, k, t, :, TOP + HALO + cx:] = jnp.zeros((2, TOP + HALO, cy), F32)

    def rows_of(ref, at):
        return lambda start: ref.at[at + (pl.ds(start, HALO),)]

    any_k = slice(None)

    (first_pack, first_land, first_send, first_recv) = first_swap
    swap0 = Swap(edges([
        (lambda lo: viscosity.at[:, pl.ds(lo, HALO)], lambda e: visc.at[:, 0, ends(e)]),
        (lambda lo: spread.at[:, pl.ds(lo, HALO)], lambda e: spr.at[:, 0, ends(e)]),
        (lambda lo: misc.at[:, 0, pl.ds(HALO + lo, HALO)], lambda e: misc.at[:, 0, ends(e)]),
    ], first_pack, first_land), first_send, first_recv)
    (right_pack, right_land, right_send, right_recv) = right_swap

    def swap_right(j):
        return Swap(edges([(lambda lo: basis.at[j, :, :, 0, pl.ds(HALO + lo + (2 if lo else 0), HALO - 2)],
                            lambda e: basis.at[j, :, :, 0, pl.ds(2 if e == 0 else HALO + cx, HALO - 2)])],
                          right_pack, right_land), right_send, right_recv)

    (side_pack, side_land, side_send, side_recv) = side_swap
    swap_side = Swap(edges([
        (lambda lo: middle.field.at[1, :, 0, :, pl.ds(HALO + lo, HALO)], lambda e: mid_rows.at[e]),
        (lambda lo: column.field.at[1, 0, 0, :, pl.ds(HALO + lo, HALO)], lambda e: col_rows.at[e, 0]),
        (lambda lo: column.right.at[0, 0, :, pl.ds(HALO + lo, HALO)], lambda e: col_rows.at[e, 1]),
    ], side_pack, side_land), side_send, side_recv)
    (far_out, far_in, far_send, far_recv) = point_swap
    swap_far = Swap([[(far_out, far_in.at[d])] for d in range(8)], far_send, far_recv)

    swap_near = Swap([[(near_out, near_in.at[d])] for d in range(4)], near_send, near_recv)

    def near_swap(p, q):
        return Swap([[(x_out.at[p], x_in.at[q, d])] for d in range(4)], x_send.at[p], x_recv.at[q])

    misc[0, 0, own] = mask[...].astype(F32)
    misc[1, 0, own] = aggs[...].astype(F32)
    misc[2, 0, own] = friction[...]
    misc[3, 0, own] = coupling[...]
    swap0.start((0, 1))
    packer = Packer(first_pack)
    for i in range(4):
        packer.add(misc[i, 0, own])
    for k in range(layers):
        packer.add(viscosity[k])
        packer.add(spread[k])
    packer.finish()
    swap0.start(range(2, 8))
    packer = Packer(right_pack)
    for k in range(layers):
        basis[0, :, k, 0, own] = forcing[:, k]
        for v in range(2):
            packer.add(forcing[v, k])
    packer.finish()
    swap_right(0).start()
    for j in range(ITERS):
        swap_right(j).clear()
        for k in range(layers):
            basis[j, :, k, 0, 0:HALO - 6] = jnp.zeros((2, HALO - 6, cy), F32)
            basis[j, :, k, 0, tall - HALO + 6:tall] = jnp.zeros((2, HALO - 6, cy), F32)
    swap0.clear()
    swap_side.clear()
    swap_far.clear()
    for q in range(2):
        near_swap(0, q).clear()
    swap_near.clear()
    for k in range(layers):
        visc[k, 0, own] = viscosity[k]
        spr[k, 0, own] = spread[k]

    def gather(which, slot=0):
        out, into, send, recv = gathers[which]
        into, recv = into.at[slot], recv.at[slot]
        rest = into.at[pl.ds(0, count - 1)]

        def start():
            def step(i, carry):
                target = lax.rem(me + i, count)
                pltpu.make_async_remote_copy(
                    src_ref=out, dst_ref=into.at[me], send_sem=send, recv_sem=recv,
                    device_id=(target // ny, lax.rem(target, ny)), device_id_type=MESH).start()
                return carry

            lax.fori_loop(1, count, step, 0)
            into[me] = out[...]

        def wait():
            pltpu.make_async_copy(rest, rest, recv).wait()
            pltpu.make_async_copy(rest, rest, send).wait()

        return start, wait

    wide = lax.broadcasted_iota(jnp.int32, (1, cy), 1)

    def reduce_all(parts):
        line = jnp.zeros((1, cy), F32)
        for i, part in enumerate(parts):
            line = jnp.where(wide == i, part, line)
        gathers[1][0][...] = line
        start, wait = gather(1)
        start()
        wait()
        return jnp.sum(gathers[1][1][0, :, 0, :], axis=0, keepdims=True)

    def pick(line, i):
        return jnp.sum(jnp.where(wide == i, line, 0.0), axis=1, keepdims=True)

    def put_to(ref, *at):
        def put(value):
            ref[at] = value
        return put

    ids = aggs[...]
    ice_own = mask[...].astype(F32)
    down = lax.broadcasted_iota(jnp.int32, (cy, cy), 0)
    across = lax.broadcasted_iota(jnp.int32, (cy, cy), 1)
    spots = [pl.ds(r * cy, cy) for r in range(cx)]
    for r in range(cx):
        hit[:, spots[r]] = jnp.where(ids[r:r + 1, :] == down, 1.0, 0.0).astype(BF16)
    flow = sum(spread[k] for k in range(layers))
    cross2 = friction[...] * coupling[...] * ice_own
    diag2 = ice_own * (4.0 * flow + friction[...]) + layers * (1.0 - ice_own)
    flow = flow * ice_own
    ahead = jnp.where(lane < cy - 1, flow * pltpu.roll(ice_own, cy - 1, 1), 0.0)
    behind = jnp.where(lane > 0, flow * pltpu.roll(ice_own, 1, 1), 0.0)
    near = jnp.zeros((cy, cy), F32)
    for r in range(cx):
        here = hit[:, spots[r]].astype(F32)
        term = diag2[r:r + 1, :] * here
        if r + 1 < cx:
            term = term - flow[r:r + 1, :] * ice_own[r + 1:r + 2, :] * hit[:, spots[r + 1]].astype(F32)
        if r > 0:
            term = term - flow[r:r + 1, :] * ice_own[r - 1:r, :] * hit[:, spots[r - 1]].astype(F32)
        term = term - ahead[r:r + 1, :] * pltpu.roll(here, cy - 1, 1)
        term = term - behind[r:r + 1, :] * pltpu.roll(here, 1, 1)
        high, low = split(term)
        near = near + dot(high, hit[:, spots[r]], 1, 1) + dot(low, hit[:, spots[r]], 1, 1)
    point_diag[...] = jnp.sum(jnp.where(down == across, near, 0.0), axis=0, keepdims=True)
    tall4 = lax.broadcasted_iota(jnp.int32, (4 * cx, cy), 0) % cx

    def restrict_points(first, second):
        h0, l0 = split(first)
        h1, l1 = split(second)
        left = jnp.concatenate([h0, h1, l0, l1], axis=0)
        left = jnp.concatenate([jnp.where(tall4 == r, left, jnp.zeros_like(left)) for r in range(cx)], axis=1)
        out = dot(left, hit[...], 1, 1)
        parts = [jnp.sum(out[i * cx:(i + 1) * cx] + out[(i + 2) * cx:(i + 3) * cx], axis=0, keepdims=True)
                 for i in range(2)]
        return jnp.concatenate(parts, axis=0)

    point_cross[...] = restrict_points(cross2, cross2)

    swap0.wait()
    puts = [put_to(misc, i, 1) for i in range(4)]
    for k in range(layers):
        puts += [put_to(visc, k, 1), put_to(spr, k, 1)]
    unpack(first_land, puts)

    ids_all = [misc[1, t].astype(jnp.int32) for t in both]
    ice = [misc[0, t] for t in both]
    for t in both:
        ice_ext[t] = ice[t]
        column.seen[1, 0, t, 0, pl.ds(TOP, tall), :] = ice[t]
    around = []
    ups = [turn(x, cy - 1) for x in ice]
    downs = [turn(x, 1) for x in ice]
    for t in both:
        around.append((column.seen[1, 0, t, 0, pl.ds(TOP + 1, tall), :],
                       column.seen[1, 0, t, 0, pl.ds(TOP - 1, tall), :],
                       jnp.where(long_lane == cy - 1, ups[1 - t], ups[t]),
                       jnp.where(long_lane == 0, downs[1 - t], downs[t])))
    for k in range(layers):
        for t in both:
            owned = spr[k, t]
            faces = 4.0 * owned
            if k + 1 < layers:
                face = 0.5 * (visc[k, t] + visc[k + 1, t]) * ice[t]
                fine.vert[k, t] = face
                faces = faces + face
            if k > 0:
                faces = faces + fine.vert[k - 1, t]
            if k == 0:
                faces = faces + misc[2, t]
            fine.diag[k, t] = ice[t] * faces + (1.0 - ice[t])
            fine.side[k, t] = owned * ice[t]
    for t in both:
        fine.cross[t] = misc[2, t] * misc[3, t] * ice[t]
    for finer, coarser in ((fine, middle), (middle, column)):
        size = finer.depth // coarser.depth
        for k in range(coarser.depth):
            group = range(k * size, (k + 1) * size)
            diag = sum(finer.diag[j] for j in group)
            inner_faces = sum(finer.vert[j] for j in list(group)[:-1])
            coarser.diag[k] = diag - 2.0 * inner_faces
            if k + 1 < coarser.depth:
                coarser.vert[k] = finer.vert[group[-1]]
            coarser.side[k] = sum(finer.side[j] for j in group)
        coarser.cross[...] = finer.cross[...]

    side2 = [column.side[0, 0, own] * around[0][d][HALO:HALO + cx] for d in range(4)]
    inner = (diag2 - jnp.where(row < cx - 1, side2[0], 0.0) - jnp.where(row > 0, side2[1], 0.0)
             - jnp.where(lane < cy - 1, side2[2], 0.0) - jnp.where(lane > 0, side2[3], 0.0))
    entries = (inner, cross2, jnp.where(row == cx - 1, side2[0], 0.0), jnp.where(row == 0, side2[1], 0.0),
               jnp.where(last_lane, side2[2], 0.0), jnp.where(first_lane, side2[3], 0.0))
    eight = lax.broadcasted_iota(jnp.int32, (8, cy), 0)
    tile = jnp.zeros((8, cy), F32)
    for i, entry in enumerate(entries):
        tile = jnp.where(eight == i, total(entry), tile)
    gathers[2][0][...] = tile
    tables_start, tables_wait = gather(2)
    tables_start()
    for level in (fine, middle, column):
        level.factor()

    tables = [near]
    for d, r, e in ((0, cx - 1, HALO + cx), (1, 0, HALO - 1)):
        other = ids_all[0][e:e + 1, :]
        term = jnp.where(other == down, side2[d][r:r + 1, :], 0.0)
        high, low = split(term)
        tables.append(-(dot(high, hit[:, spots[r]], 1, 1) + dot(low, hit[:, spots[r]], 1, 1)))
    for d, q, e in ((2, cy - 1, 0), (3, 0, cy - 1)):
        other = ids_all[1][HALO:HALO + cx, e:e + 1]
        term = jnp.where(other == lane, side2[d][:, q:q + 1], 0.0)
        here = jnp.where(ids[:, q:q + 1] == lane, 1.0, 0.0)
        high, low = split(term)
        here = here.astype(BF16)
        tables.append(-(dot(high, here, 0, 0) + dot(low, here, 0, 0)))
    for i, table in enumerate(tables):
        big[i * cy:(i + 1) * cy, 0:cy], big[i * cy:(i + 1) * cy, cy:2 * cy] = split(table)

    scale = POINT_WEIGHT / point_diag[...]
    ones = jnp.ones((8, 2 * cy), BF16)
    sixteen = lax.broadcasted_iota(jnp.int32, (16, cy), 0)
    sent = jnp.where(sixteen == 5, scale * point_cross[0:1, :], 0.0)
    for i, table in enumerate(tables):
        sent = jnp.where(sixteen == i, scale * jnp.sum(table, axis=0, keepdims=True), sent)
        part = big[i * cy:(i + 1) * cy]
        across_sum = dot(ones, part, 1, 1)[0:1, :]
        if i == 0:
            own_sum[...] = across_sum
        else:
            sent = jnp.where(sixteen == 5 + i, across_sum, sent)
    sent = jnp.where(sixteen == 10, scale, sent)
    near_out[0:16] = sent
    edge_rows = jnp.zeros((8, cy), F32)
    for i, (r, e) in enumerate(((cx - 1, HALO + cx), (0, HALO - 1))):
        for n, line in enumerate((misc[1, 0, HALO + r:HALO + r + 1], misc[1, 0, e:e + 1], side2[i][r:r + 1])):
            edge_rows = jnp.where(eight == 3 * i + n, line, edge_rows)
    near_out[16:24] = edge_rows
    edge_cols = jnp.zeros((cx, cy), F32)
    for i, (q, e) in enumerate(((cy - 1, 0), (0, cy - 1))):
        for n, line in enumerate((misc[1, 0, own, q:q + 1], misc[1, 1, own, e:e + 1], side2[2 + i][:, q:q + 1])):
            edge_cols = jnp.where(lane == 3 * i + n, line, edge_cols)
    near_out[24:24 + cx] = edge_cols
    near_out[24 + cx:24 + cx + cy] = near
    swap_near.start()

    def build_near():
        swap_near.wait()
        down_f, lane_f = down.astype(F32), lane.astype(F32)

        def step(m, carry):
            rows, cols = near_in[m, 16:24], near_in[m, 24:24 + cx]
            found = [near_in[m, 24 + cx:24 + cx + cy]]
            for i in range(2):
                there = jnp.where(rows[3 * i:3 * i + 1] == down_f, 1.0, 0.0).astype(BF16)
                high, low = split(jnp.where(rows[3 * i + 1:3 * i + 2] == down_f, rows[3 * i + 2:3 * i + 3], 0.0))
                found.append(-(dot(high, there, 1, 1) + dot(low, there, 1, 1)))
            for i in range(2):
                there = jnp.where(cols[:, 3 * i:3 * i + 1] == lane_f, 1.0, 0.0).astype(BF16)
                high, low = split(jnp.where(cols[:, 3 * i + 1:3 * i + 2] == lane_f, cols[:, 3 * i + 2:3 * i + 3], 0.0))
                found.append(-(dot(high, there, 0, 0) + dot(low, there, 0, 0)))
            for i, table in enumerate(found):
                big_near[m, i * cy:(i + 1) * cy, 0:cy], big_near[m, i * cy:(i + 1) * cy, cy:2 * cy] = split(table)
            return carry

        lax.fori_loop(0, 4, step, 0)

    block_row = lax.broadcasted_iota(jnp.int32, (count, cy), 0)
    shifts = (ny, count - ny, 1, count - 1)

    def coarse_begin(j, right, x):
        lines = [right - own_sum[...] * x - point_cross[...] * jnp.concatenate([x[1:2], x[0:1]], axis=0)]
        for d in range(4):
            lines.append(-near_in[BACK[d], 6 + BACK[d]:7 + BACK[d], :] * x)
        line = jnp.zeros((1, cy), F32)
        for i, part in enumerate(lines):
            sums = jnp.sum(part, axis=1, keepdims=True)
            for v in range(2):
                line = jnp.where(wide == 2 * i + v, sums[v:v + 1], line)
        gathers[0][0][0:2] = x
        gathers[0][0][2:3] = line
        start, wait = gather(0, lax.rem(j, 2))
        start()
        return wait

    def coarse_end(j, wait):
        @pl.when(j == 0)
        def _():
            tables_wait()
            for i in range(6):
                coarse_tab[i] = gathers[2][1][0, :, i, :]
            coarse_tab[6] = COARSE_WEIGHT / coarse_tab[0]
        wait()
        came = gathers[0][1][lax.rem(j, 2), :, 2, :]
        moved = [pltpu.roll(came, shifts[d], 0) for d in range(4)]
        right = []
        for v in range(2):
            part = came if v == 0 else pltpu.roll(came, cy - v, 1)
            for d in range(4):
                part = part + pltpu.roll(moved[d], cy - 2 - 2 * d - v, 1)
            right.append(part)
        diag, crossed, east, west, north, south, weight = (coarse_tab[i] for i in range(7))
        answer = [part * weight for part in right]
        for _ in range(CSWEEPS - 1):
            old = answer
            answer = []
            for v in range(2):
                applied = diag * old[v] + crossed * old[1 - v] - (
                    east * pltpu.roll(old[v], count - ny, 0) + west * pltpu.roll(old[v], ny, 0)
                    + north * pltpu.roll(old[v], count - 1, 0) + south * pltpu.roll(old[v], 1, 0))
                answer.append(old[v] + (right[v] - applied) * weight)
        hops = ((0, 0),) + STEPS[:4]
        known = {}

        def value(dx, dy):
            if (dx, dy) not in known:
                here = block_row == me + dx * ny + dy
                known[dx, dy] = jnp.concatenate(
                    [jnp.sum(jnp.where(here, part, 0.0), axis=0, keepdims=True)[:, 0:1] for part in answer], axis=0)
            return known[dx, dy]

        found = []
        for i, (dx, dy) in enumerate(hops):
            here = value(dx, dy)
            rows = near_out if i == 0 else near_in.at[BACK[i - 1]]
            out = here - rows[5:6, :] * jnp.concatenate([here[1:2], here[0:1]], axis=0)
            for n, (ex, ey) in enumerate(hops):
                out = out - rows[n:n + 1, :] * value(dx + ex, dy + ey)
            found.append(out)
        return found

    def build_lifts():
        for t in both:
            for out, source in ((lift_side, lambda k: middle.side[k, t]), (lift_cross, lambda k: middle.cross[t] if k == 0 else 0.0)):
                last = 0.0
                for k in range(half):
                    value = source(k)
                    if k > 0:
                        value = value + middle.vert[k - 1, t] * last
                    last = value * middle.inverse[k, t]
                    out[k, t] = last
                out[half - 1, t] = LINE_WEIGHT * last
                for k in reversed(range(half - 1)):
                    last = out[k, t] - middle.upper[k, t] * last
                    out[k, t] = LINE_WEIGHT * last

    def swapped(x):
        return jnp.concatenate([x[1:2], x[0:1]], axis=0)

    def apply_tables(table, xs):
        parts = [split(x) for x in xs]
        left = jnp.concatenate([jnp.concatenate([p[i] for p in parts], axis=1) for i in range(2)], axis=0)
        both_parts = dot(left, table[...], 1, 0)
        both_parts = both_parts[0:2] + both_parts[2:4]
        return both_parts[:, 0:cy] + both_parts[:, cy:2 * cy]

    def point_apply(xs):
        return point_cross[...] * swapped(xs[0]) + apply_tables(big, xs)

    def point_cycle(j, right, merge):
        x_out[0] = right * (POINT_WEIGHT / point_diag[...])
        swap = near_swap(0, 0)
        swap.start()
        packer = Packer(side_pack)
        for v in range(2):
            packer.add(column.field[1, 0, 0, v, own])
            packer.add(column.right[0, 0, v, own])
        for k in range(half):
            for v in range(2):
                packer.add(middle.field[1, k, 0, v, own])
        packer.finish()
        swap_side.start()
        pl.when(j == 0)(build_near)
        pl.when(j == 0)(build_lifts)
        scale = POINT_WEIGHT / point_diag[...]
        swap.wait()
        first = [right * scale] + [x_in[0, BACK[d]] for d in range(4)]
        x = first[0] + (right - point_apply(first)) * scale
        coarse_wait = coarse_begin(j, right, x)
        merge()
        found = coarse_end(j, coarse_wait)
        hops = ((0, 0),) + STEPS[:4]

        def second(dx, dy):
            return gathers[0][1][lax.rem(j, 2), lax.rem(me + dx * ny + dy + count, count), 0:2]

        xs = []
        for i, (dx, dy) in enumerate(hops):
            local = [second(dx + ex, dy + ey) for ex, ey in hops]
            if i == 0:
                moved = point_apply(local) * scale
            else:
                rows = near_in.at[BACK[i - 1]]
                moved = (rows[10:11] * apply_tables(big_near.at[BACK[i - 1]], local)
                         + rows[5:6] * swapped(local[0]))
            xs.append(local[0] + first[i] - moved + found[i])
        return xs[0] + (right - point_apply(xs)) * scale

    def mid_put(k, v):
        def put(value):
            middle.field[0, k, 1, v] = value
            middle.seen[0, k, 1, v, TOP:TOP + tall] = value * ice_ext[1]
        return put

    whole = pl.ds(0, tall)

    def merge_side(right0, right1):
        swap_side.wait()
        column.field[0, 0, 0] = jnp.concatenate([col_rows[0, 0], column.field[1, 0, 0, :, own], col_rows[1, 0]], axis=1)
        for e in range(2):
            column.right[0, 0, :, ends(e)] = col_rows[e, 1]
        for k in range(half):
            middle.put(0, k, 0, whole, jnp.concatenate(
                [mid_rows[0, k], middle.field[1, k, 0, :, own], mid_rows[1, k]], axis=1))
        puts = []
        for v in range(2):
            puts += [put_to(column.field, 0, 0, 1, v), put_to(column.right, 0, 1, v)]
        for k in range(half):
            puts += [mid_put(k, v) for v in range(2)]
        unpack(side_land, puts)
        middle.sweep(0, right1, spans=inside, plain=True)
        fine.sweep(1, right0, spans=inside, plain=True)

    def spread_points(x):
        far_out[...] = x
        swap_far.start()
        swap_far.wait()
        parts = [[], []]
        zones = ((pl.ds(0, HALO), 1, 6, 7), (own, None, 2, 3), (pl.ds(HALO + cx, HALO), 0, 4, 5))
        short = {n: lax.broadcasted_iota(jnp.int32, (n, cy), 1) < cy // 2 for n in (HALO, cx)}

        def take(src, v, index):
            values = x if src is None else far_in[BACK[src]]
            return jnp.take_along_axis(jnp.broadcast_to(values[v:v + 1], index.shape), index, axis=1,
                                       mode="promise_in_bounds")

        for rows, straight, right, left in zones:
            index = [misc[1, t, rows].astype(jnp.int32) for t in both]
            parts[0].append(jnp.stack([take(straight, v, index[0]) for v in range(2)]))
            lanes = short[index[1].shape[0]]
            parts[1].append(jnp.stack([jnp.where(lanes, take(right, v, index[1]), take(left, v, index[1]))
                                       for v in range(2)]))
        return [jnp.concatenate(p, axis=1) for p in parts]

    def iteration(j, carry):
        def right0(k, t, here):
            return basis[j, :, k, t, here]

        def right1(k, t, here):
            return middle.right[k, t, :, here]

        def right2(k, t, here):
            return column.right[k, t, :, here]

        def collect(coarser, size):
            held = {}

            def emit(k, t, here, value):
                held[t] = held[t] + value if k % size else value
                if k % size == size - 1:
                    coarser.right[k // size, t, :, here] = held[t]
            return emit

        swap_right(j).wait()
        unpack(right_land, [put_to(basis, j, v, k, 1) for k in range(layers) for v in range(2)])
        fine.before(right0)
        fine.leftover(1, right0, collect(middle, 2), spans=inside)
        middle.before(right1, inside)
        middle.leftover(1, right1, collect(column, half), spans=inside)
        column.before(right2, inside)
        kept = []
        column.leftover(1, right2, lambda k, t, here, value: kept.append(value), (0,), (own,))
        found = spread_points(point_cycle(j, restrict_points(kept[0][0], kept[0][1]),
                                          lambda: merge_side(right0, right1)))

        for t in both:
            column.put(0, 0, t, whole, found[t] + column.field[0, 0, t])
        column.sweep(0, right2)
        column.sweep(1, right2)
        for here in inside:
            outs = column.sums(0, 0, here, both)[1]
            for t in both:
                value = column.field[0, 0, t, :, here]
                part = (1.0 - LINE_WEIGHT) * value
                other = jnp.stack([value[1], value[0]])
                for k in range(half):
                    middle.put(0, k, t, here, (middle.field[1, k, t, :, here] + part)
                               + (lift_side[k, t, here][None] * outs[t] - lift_cross[k, t, here][None] * other))
        middle.sweep(0, right1, spans=inside)
        held = []

        def lifted(k, here):
            if k % 2 == 0:
                held[:] = middle.sums(1, k // 2, here, both)
            return fine.sideways(k, here, both, *held)

        def lift(k, t, here, value):
            fine.put(1, k, t, here, (fine.field[0, k, t, :, here] + value)
                     + (1.0 - LINE_WEIGHT) * middle.field[1, k // 2, t, :, here])

        fine.solve(lifted, lift, inside)
        fine.sweep(1, right0, spans=inside)

        packer = Packer(right_pack)

        for k in range(layers):
            here = fine.field[0, k, 0, :, own]
            stored[j, :, k] = here
            out = fine.beside(0, k, own, (0,))[0] - fine.diag[k, 0, own][None] * here
            if k + 1 < layers:
                out = out + fine.vert[k, 0, own][None] * fine.field[0, k + 1, 0, :, own]
            if k > 0:
                out = out + fine.vert[k - 1, 0, own][None] * fine.field[0, k - 1, 0, :, own]
            value = basis[j, :, k, 0, own] + out
            basis[j + 1, :, k, 0, own] = value
            for v in range(2):
                packer.add(value[v])
        packer.finish()

        @pl.when(j < ITERS - 1)
        def _():
            swap_right(j + 1).start()
        return carry

    lax.fori_loop(0, ITERS, iteration, 0)

    names = [(i, j) for i in range(ITERS + 1) for j in range(i, ITERS + 1)]
    sums = {name: jnp.zeros((cx, cy), F32) for name in names}
    for k in range(layers):
        chain = [basis[i, :, k, 0, own] for i in range(ITERS + 1)]
        terms = [chain[j] - chain[j + 1] for j in range(ITERS)] + [chain[0]]
        for i, j in names:
            prod = terms[i] * terms[j]
            sums[i, j] = sums[i, j] + prod[0] + prod[1]
    line = reduce_all([total(sums[name]) for name in names])
    gram = {name: pick(line, at) for at, name in enumerate(names)}
    rows = [[gram[min(i, j), max(i, j)] for j in range(ITERS + 1)] for i in range(ITERS)]
    for a in range(ITERS):
        for i in range(a + 1, ITERS):
            share = rows[i][a] / rows[a][a]
            for c in range(a, ITERS + 1):
                rows[i][c] = rows[i][c] - share * rows[a][c]
    weights = [None] * ITERS
    for a in reversed(range(ITERS)):
        part = rows[a][ITERS]
        for c in range(a + 1, ITERS):
            part = part - rows[a][c] * weights[c]
        weights[a] = part / rows[a][a]
    for k in range(layers):
        out = weights[0] * stored[0, :, k]
        rest = forcing[:, k] - weights[0] * (basis[0, :, k, 0, own] - basis[1, :, k, 0, own])
        for j in range(1, ITERS):
            out = out + weights[j] * stored[j, :, k]
            rest = rest - weights[j] * (basis[j, :, k, 0, own] - basis[j + 1, :, k, 0, own])
        for v in range(2):
            result[pl.ds((v * layers + k) * cx, cx)] = out[v]
            result[pl.ds((2 * layers + v * layers + k) * cx, cx)] = rest[v]


def solution(mesh):
    nx, ny = mesh.shape["gx"], mesh.shape["gy"]
    count = nx * ny

    def body(forcing, viscosity, spread, coupling, friction, mask, aggs):
        layers, cx, cy = forcing.shape[1:]
        dma = pltpu.SemaphoreType.DMA
        tall = cx + 2 * HALO
        half = layers // 2

        def vm(*shape, dtype=F32):
            return pltpu.VMEM(shape, dtype)

        def level(n):
            return (
                vm(2, n, 2, 2, tall + 2 * TOP, cy), vm(2, n, 2, 2, tall, cy),
                vm(n, 2, tall, cy), vm(n, 2, tall, cy), vm(n, 2, tall, cy), vm(2, tall, cy),
                vm(n, 2, tall, cy), vm(n, 2, tall, cy), vm(n, 2, 2, tall, cy), vm(n, 2, 2, tall, cy),
                vm(n, 2, 2, tall, cy),
            )

        def swap(planes, pieces):
            tiles = -(-planes * HALO // cy)
            return (vm(2, tiles, cx, cy), vm(2, tiles, tall, cy), dma((8, pieces)), dma((8, pieces)))

        scratch = (
            (level(layers), level(half), level(1)),
            (vm(ITERS + 1, 2, layers, 2, tall, cy), vm(ITERS, 2, layers, cx, cy),
             vm(layers, 2, tall, cy), vm(layers, 2, tall, cy), vm(4, 2, tall, cy), vm(2, tall, cy)),
            (vm(cy, cx * cy, dtype=BF16), vm(5 * cy, 2 * cy, dtype=BF16),
             vm(1, cy), vm(2, cy), vm(1, cy)),
            (vm(2, 2, cy), vm(2, 4, 2, cy), dma((2, 4, 1)), dma((2, 4, 1))),
            tuple((vm(n, cy), vm(2, count, n, cy), dma(()), dma((2,))) for n in (3, 1, 8)),
            swap(4 + 2 * layers, 3),
            swap(2 * layers, 1),
            swap(4 + 2 * half, 3),
            (vm(2, cy), vm(8, 2, cy), dma((8, 1)), dma((8, 1))),
            (vm(2, half, 2, HALO, cy), vm(2, 2, 2, HALO, cy)),
            (vm(24 + cx + cy, cy), vm(4, 24 + cx + cy, cy), vm(4, 5 * cy, 2 * cy, dtype=BF16), dma((4, 1)), dma((4, 1))),
            vm(7, count, cy), vm(half, 2, tall, cy), vm(half, 2, tall, cy),
        )
        flat, tree = jax.tree.flatten(scratch)

        def run(*refs):
            kernel(nx, ny, layers, cx, cy, *refs[:8], *jax.tree.unflatten(tree, refs[8:]))

        shape = jax.ShapeDtypeStruct((4 * layers * cx, cy), F32)
        whole = pl.BlockSpec(memory_space=pltpu.VMEM)
        outs = pl.pallas_call(
            run,
            out_shape=shape,
            in_specs=[whole] * 7,
            out_specs=whole,
            scratch_shapes=flat,
            compiler_params=pltpu.CompilerParams(has_side_effects=True, vmem_limit_bytes=60 * 1024 * 1024),
        )(forcing, viscosity, spread, coupling, friction, mask, aggs)
        return tuple(out.reshape(forcing.shape) for out in jnp.split(outs, 2))

    return jax.shard_map(
        body,
        mesh=mesh,
        in_specs=(
            P(None, None, "gx", "gy"),
            P(None, "gx", "gy"),
            P(None, "gx", "gy"),
            P("gx", "gy"),
            P("gx", "gy"),
            P("gx", "gy"),
            P("gx", "gy"),
        ),
        out_specs=(P(None, None, "gx", "gy"), P(None, None, "gx", "gy")),
        check_vma=False,
    )
```

```python
import jax
import jax.numpy as jnp
from jax import lax
from jax.experimental import pallas as pl
from jax.experimental.pallas import tpu as pltpu
from jax.sharding import PartitionSpec as P

ITERS = 3
CSWEEPS = 4
LINE_WEIGHT = 0.8
POINT_WEIGHT = 0.7
COARSE_WEIGHT = 0.7
MESH = pl.DeviceIdType.MESH
F32 = jnp.float32
BF16 = jnp.bfloat16
TOP = 8
HALO = 8
REACH = 6
CHUNK = 16
INNER = 8
STEPS = ((1, 0), (-1, 0), (0, 1), (0, -1), (1, 1), (1, -1), (-1, 1), (-1, -1))
BACK = (1, 0, 3, 2, 7, 6, 5, 4)


def split(x):
    high = x.astype(BF16)
    return high, (x - high.astype(F32)).astype(BF16)


def dot(a, b, ca, cb):
    return lax.dot_general(a, b, (((ca,), (cb,)), ((), ())), preferred_element_type=F32)


def total(x):
    return jnp.sum(jnp.sum(x, axis=1, keepdims=True), axis=0, keepdims=True)


def turn(x, shift):
    flat = x.reshape(-1, x.shape[-1])
    return pltpu.roll(flat, shift % x.shape[-1], 1).reshape(x.shape)


def kernel(nx, ny, layers, cx, cy, forcing, viscosity, spread, coupling, friction, mask, aggs,
           result, *scratch):
    count = nx * ny
    gx = lax.axis_index("gx")
    gy = lax.axis_index("gy")
    me = gx * ny + gy
    (levels, (basis, stored, visc, spr, misc, ice_ext), (hit, big, point_diag, point_cross, own_sum),
     (x_out, x_in, x_send, x_recv), gathers, first_swap, right_swap, side_swap, point_swap,
     (mid_rows, col_rows), (near_out, near_in, big_near, near_send, near_recv),
     coarse_tab, lift_side, lift_cross) = scratch
    tall = cx + 2 * HALO
    half = layers // 2
    own = pl.ds(HALO, cx)
    lane = lax.broadcasted_iota(jnp.int32, (cx, cy), 1)
    row = lax.broadcasted_iota(jnp.int32, (cx, cy), 0)
    first_lane, last_lane = lane == 0, lane == cy - 1
    long_lane = lax.broadcasted_iota(jnp.int32, (tall, cy), 1)

    exists, peers = [], []
    for dx, dy in STEPS:
        ok = []
        if dx:
            ok.append(gx < nx - 1 if dx > 0 else gx > 0)
        if dy:
            ok.append(gy < ny - 1 if dy > 0 else gy > 0)
        exists.append(ok[0] if len(ok) == 1 else jnp.logical_and(ok[0], ok[1]))
        peers.append((gx + dx, gy + dy))

    class Swap:
        def __init__(self, pieces, send, recv):
            self.pieces = pieces
            self.copies = [[pltpu.make_async_remote_copy(
                src_ref=src, dst_ref=dst, send_sem=send.at[d, i], recv_sem=recv.at[BACK[d], i],
                device_id=peers[d], device_id_type=MESH) for i, (src, dst) in enumerate(pieces[d])]
                for d in range(len(pieces))]

        def start(self, which=None):
            for d in range(len(self.copies)) if which is None else which:
                @pl.when(exists[d])
                def _():
                    for copy in self.copies[d]:
                        copy.start()

        def wait(self):
            for d in range(len(self.copies)):
                @pl.when(exists[d])
                def _():
                    for copy in self.copies[d]:
                        copy.wait_send()
                    for copy in self.copies[BACK[d]]:
                        copy.wait_recv()

        def clear(self):
            for d in range(len(self.copies)):
                @pl.when(jnp.logical_not(exists[d]))
                def _():
                    for _, ref in self.pieces[BACK[d]]:
                        ref[...] = jnp.zeros(ref.shape, F32)

    def edges(rows, packed, landed, reach=HALO):
        low, high = pl.ds(0, reach), pl.ds(cx - reach, reach)
        top, bottom = pl.ds(HALO - reach, reach), pl.ds(HALO + cx, reach)
        return [
            [(src(cx - HALO), dst(0)) for src, dst in rows],
            [(src(0), dst(1)) for src, dst in rows],
            [(packed.at[0], landed.at[0, :, own])],
            [(packed.at[1], landed.at[1, :, own])],
            [(packed.at[0, :, high], landed.at[0, :, top])],
            [(packed.at[1, :, high], landed.at[1, :, top])],
            [(packed.at[0, :, low], landed.at[0, :, bottom])],
            [(packed.at[1, :, low], landed.at[1, :, bottom])],
        ]

    def ends(e):
        return pl.ds(0, HALO) if e == 0 else pl.ds(HALO + cx, HALO)

    def slots_of(width):
        return cy // width if cy % width == 0 else (cy - width) // width // 2 * 2

    class Packer:
        def __init__(self, out, width=HALO):
            self.out = out
            self.width = width
            self.slots = slots_of(width)
            self.at = 0
            self.tiles = None

        def add(self, value):
            s, m = divmod(self.at, self.slots)
            w = self.width
            moved = pltpu.roll(value, (w * m + w) % cy, 1)
            if m == 0:
                self.tiles = [moved] * 2
            else:
                for i in range(2):
                    low = (m + i) * w % cy
                    self.tiles[i] = jnp.where((lane >= low) & (lane < low + w), moved, self.tiles[i])
            self.at += 1
            if m == self.slots - 1:
                self.flush(s)

        def flush(self, s):
            for i in range(2):
                self.out[i, s] = self.tiles[i]
            self.tiles = None

        def finish(self):
            if self.tiles is not None:
                self.flush((self.at - 1) // self.slots)

    def unpack(landed, puts, w=HALO):
        south = long_lane // w % 2 == 0
        kept = (long_lane < w) | (long_lane >= cy - w)
        slots = slots_of(w)
        comb = None
        for i, put in enumerate(puts):
            s, m = divmod(i, slots)
            if m == 0:
                comb = [jnp.where(south, landed[e, s], landed[1 - e, s]) for e in range(2)]
            put(jnp.where(kept, pltpu.roll(comb[m % 2], (2 * cy - w * m - w) % cy, 1), 0.0))

    chunks = [pl.ds(i * CHUNK, CHUNK) for i in range(tall // CHUNK)]
    both = (0, 1)

    class Level:
        def __init__(self, depth, refs):
            self.depth = depth
            (self.seen, self.field, self.diag, self.vert, self.side, self.cross, self.inverse, self.upper,
             self.right, self.forward, self.moved) = refs

        def put(self, p, k, t, here, value):
            self.field[p, k, t, :, here] = value
            self.seen[p, k, t, :, pl.ds(TOP + here.start, here.size)] = value * ice_ext[t, here][None]

        def sums(self, p, k, here, tiles):
            def at(t, shift):
                return self.seen[p, k, t, :, pl.ds(TOP + here.start + shift, here.size)]

            lanes = lax.broadcasted_iota(jnp.int32, (2, here.size, cy), 2)
            value = [at(t, 0) for t in both]
            up = [turn(v, cy - 1) for v in value]
            down = [turn(v, 1) for v in value]
            outs = []
            for t in tiles:
                north = jnp.where(lanes == cy - 1, up[1 - t], up[t])
                south = jnp.where(lanes == 0, down[1 - t], down[t])
                outs.append((at(t, 1) + at(t, -1)) + (north + south))
            return value, outs

        def sideways(self, k, here, tiles, value, outs):
            outs = [self.side[k, t, here][None] * out for t, out in zip(tiles, outs)]
            if k == 0:
                for i, t in enumerate(tiles):
                    crossed = self.cross[t, here]
                    outs[i] = outs[i] - jnp.stack([crossed * value[t][1], crossed * value[t][0]])
            return outs

        def beside(self, p, k, here, tiles):
            return self.sideways(k, here, tiles, *self.sums(p, k, here, tiles))

        def leftover(self, p, right, emit, tiles=both, spans=None):
            for here in spans or chunks:
                for k in range(self.depth):
                    outs = self.beside(p, k, here, tiles)
                    for i, t in enumerate(tiles):
                        emit(k, t, here, (1.0 - LINE_WEIGHT) ** 2 * right(k, t, here)
                             + (outs[i] - LINE_WEIGHT * self.moved[k, t, :, here]))

        def solve(self, source, finish, spans):
            for here in spans or chunks:
                last = [None, None]
                for k in range(self.depth):
                    values = source(k, here)
                    for t in both:
                        value = values[t]
                        if k > 0:
                            value = value + self.vert[k - 1, t, here][None] * last[t]
                        last[t] = value * self.inverse[k, t, here][None]
                        if k + 1 < self.depth:
                            self.forward[k, t, :, here] = last[t]
                for k in reversed(range(self.depth)):
                    for t in both:
                        if k + 1 < self.depth:
                            last[t] = self.forward[k, t, :, here] - self.upper[k, t, here][None] * last[t]
                        finish(k, t, here, LINE_WEIGHT * last[t])

        def first(self, right, spans=None):
            self.solve(lambda k, here: [right(k, t, here) for t in both],
                       lambda k, t, here, value: self.put(0, k, t, here, value), spans)

        def sweep(self, p, right, keep=False, spans=None, plain=False):
            def source(k, here):
                outs = self.beside(p, k, here, both)
                if keep:
                    for t in both:
                        self.moved[k, t, :, here] = outs[t]
                return [right(k, t, here) + outs[t] for t in both]

            def finish(k, t, here, value):
                value = value + (1.0 - LINE_WEIGHT) * self.field[p, k, t, :, here]
                if plain:
                    self.field[1 - p, k, t, :, here] = value
                else:
                    self.put(1 - p, k, t, here, value)
            self.solve(source, finish, spans)

        def factor(self):
            inverse = 1.0 / self.diag[0]
            self.inverse[0] = inverse
            for k in range(1, self.depth):
                ratio = -self.vert[k - 1] * inverse
                self.upper[k - 1] = ratio
                inverse = 1.0 / (self.diag[k] + self.vert[k - 1] * ratio)
                self.inverse[k] = inverse

        def before(self, right, spans=None):
            self.first(right, spans)
            self.sweep(0, right, True, spans)

    inside = [pl.ds(HALO // 2 + i * INNER, INNER) for i in range((cx + HALO) // INNER)]
    fine, middle, column = (Level(n, refs) for n, refs in zip((layers, half, 1), levels))
    for level in (fine, middle, column):
        for p in range(2):
            for k in range(level.depth):
                for t in both:
                    level.seen[p, k, t, :, 0:TOP + HALO] = jnp.zeros((2, TOP + HALO, cy), F32)
                    level.seen[p, k, t, :, TOP + HALO + cx:] = jnp.zeros((2, TOP + HALO, cy), F32)

    def tail(lo, offset):
        return pl.ds(offset + lo + (HALO - REACH if lo else 0), REACH)

    def near_ends(e):
        return pl.ds(HALO - REACH if e == 0 else HALO + cx, REACH)

    (first_pack, first_land, first_send, first_recv) = first_swap
    swap0 = Swap(edges([
        (lambda lo: viscosity.at[:, tail(lo, 0)], lambda e: visc.at[:, 0, near_ends(e)]),
        (lambda lo: spread.at[:, tail(lo, 0)], lambda e: spr.at[:, 0, near_ends(e)]),
        (lambda lo: misc.at[:, 0, pl.ds(HALO + lo, HALO)], lambda e: misc.at[:, 0, ends(e)]),
    ], first_pack, first_land), first_send, first_recv)
    (right_pack, right_land, right_send, right_recv) = right_swap

    side_tiles = right_pack.shape[1] // 2

    def swap_right(j):
        def part(h):
            span, tiles = pl.ds(h * half, half), pl.ds(h * side_tiles, side_tiles)
            return Swap(edges([(lambda lo: basis.at[j, :, span, 0, tail(lo, HALO)],
                                lambda e: basis.at[j, :, span, 0, near_ends(e)])],
                              right_pack.at[:, tiles], right_land.at[:, tiles], REACH),
                        right_send.at[h], right_recv.at[h])
        return [part(h) for h in range(2)]

    (side_pack, side_land, side_send, side_recv) = side_swap
    swap_side = Swap(edges([
        (lambda lo: middle.field.at[1, :, 0, :, pl.ds(HALO + lo, HALO)], lambda e: mid_rows.at[e]),
        (lambda lo: column.field.at[1, 0, 0, :, pl.ds(HALO + lo, HALO)], lambda e: col_rows.at[e, 0]),
        (lambda lo: column.right.at[0, 0, :, pl.ds(HALO + lo, HALO)], lambda e: col_rows.at[e, 1]),
    ], side_pack, side_land), side_send, side_recv)
    (far_out, far_in, far_send, far_recv) = point_swap
    swap_far = Swap([[(far_out, far_in.at[d])] for d in range(8)], far_send, far_recv)

    swap_near = Swap([[(near_out, near_in.at[d])] for d in range(4)], near_send, near_recv)

    def near_swap(p, q):
        return Swap([[(x_out.at[p], x_in.at[q, d])] for d in range(4)], x_send.at[p], x_recv.at[q])

    misc[0, 0, own] = mask[...].astype(F32)
    misc[1, 0, own] = aggs[...].astype(F32)
    misc[2, 0, own] = friction[...]
    misc[3, 0, own] = coupling[...]
    swap0.start((0, 1))
    packer = Packer(first_pack)
    for i in range(4):
        packer.add(misc[i, 0, own])
    for k in range(layers):
        packer.add(viscosity[k])
        packer.add(spread[k])
    packer.finish()
    swap0.start(range(2, 8))
    for h in range(2):
        packer = Packer(right_pack.at[:, pl.ds(h * side_tiles, side_tiles)], REACH)
        for k in range(h * half, h * half + half):
            basis[0, :, k, 0, own] = forcing[:, k]
            for v in range(2):
                packer.add(forcing[v, k])
        packer.finish()
    for part in swap_right(0):
        part.start()
    for j in range(ITERS):
        for part in swap_right(j):
            part.clear()
        for k in range(layers):
            basis[j, :, k, 0, 0:HALO - REACH] = jnp.zeros((2, HALO - REACH, cy), F32)
            basis[j, :, k, 0, HALO + cx + REACH:tall] = jnp.zeros((2, HALO - REACH, cy), F32)
    for k in range(layers):
        for ref in (visc, spr):
            ref[k, 0, 0:HALO - REACH] = jnp.zeros((HALO - REACH, cy), F32)
            ref[k, 0, HALO + cx + REACH:tall] = jnp.zeros((HALO - REACH, cy), F32)
    for e in range(2):
        for n in range(right_land.shape[1]):
            right_land[e, n, 0:HALO - REACH] = jnp.zeros((HALO - REACH, cy), F32)
            right_land[e, n, HALO + cx + REACH:tall] = jnp.zeros((HALO - REACH, cy), F32)
    swap0.clear()
    swap_side.clear()
    swap_far.clear()
    for q in range(2):
        near_swap(0, q).clear()
    swap_near.clear()
    for k in range(layers):
        visc[k, 0, own] = viscosity[k]
        spr[k, 0, own] = spread[k]

    def gather(which, slot=0):
        out, into, send, recv = gathers[which]
        into, recv = into.at[slot], recv.at[slot]
        rest = into.at[pl.ds(0, count - 1)]

        def start():
            def step(i, carry):
                target = lax.rem(me + i, count)
                pltpu.make_async_remote_copy(
                    src_ref=out, dst_ref=into.at[me], send_sem=send, recv_sem=recv,
                    device_id=(target // ny, lax.rem(target, ny)), device_id_type=MESH).start()
                return carry

            lax.fori_loop(1, count, step, 0)
            into[me] = out[...]

        def wait():
            pltpu.make_async_copy(rest, rest, recv).wait()
            pltpu.make_async_copy(rest, rest, send).wait()

        return start, wait

    wide = lax.broadcasted_iota(jnp.int32, (1, cy), 1)

    def reduce_all(parts):
        line = jnp.zeros((1, cy), F32)
        for i, part in enumerate(parts):
            line = jnp.where(wide == i, part, line)
        gathers[1][0][...] = line
        start, wait = gather(1)
        start()
        wait()
        return jnp.sum(gathers[1][1][0, :, 0, :], axis=0, keepdims=True)

    def pick(line, i):
        return jnp.sum(jnp.where(wide == i, line, 0.0), axis=1, keepdims=True)

    def put_to(ref, *at):
        def put(value):
            ref[at] = value
        return put

    ids = aggs[...]
    ice_own = mask[...].astype(F32)
    down = lax.broadcasted_iota(jnp.int32, (cy, cy), 0)
    across = lax.broadcasted_iota(jnp.int32, (cy, cy), 1)
    spots = [pl.ds(r * cy, cy) for r in range(cx)]
    for r in range(cx):
        hit[:, spots[r]] = jnp.where(ids[r:r + 1, :] == down, 1.0, 0.0).astype(BF16)
    flow = sum(spread[k] for k in range(layers))
    cross2 = friction[...] * coupling[...] * ice_own
    diag2 = ice_own * (4.0 * flow + friction[...]) + layers * (1.0 - ice_own)
    flow = flow * ice_own
    ahead = jnp.where(lane < cy - 1, flow * pltpu.roll(ice_own, cy - 1, 1), 0.0)
    behind = jnp.where(lane > 0, flow * pltpu.roll(ice_own, 1, 1), 0.0)
    near = jnp.zeros((cy, cy), F32)
    for r in range(cx):
        here = hit[:, spots[r]].astype(F32)
        term = diag2[r:r + 1, :] * here
        if r + 1 < cx:
            term = term - flow[r:r + 1, :] * ice_own[r + 1:r + 2, :] * hit[:, spots[r + 1]].astype(F32)
        if r > 0:
            term = term - flow[r:r + 1, :] * ice_own[r - 1:r, :] * hit[:, spots[r - 1]].astype(F32)
        term = term - ahead[r:r + 1, :] * pltpu.roll(here, cy - 1, 1)
        term = term - behind[r:r + 1, :] * pltpu.roll(here, 1, 1)
        high, low = split(term)
        near = near + dot(high, hit[:, spots[r]], 1, 1) + dot(low, hit[:, spots[r]], 1, 1)
    point_diag[...] = jnp.sum(jnp.where(down == across, near, 0.0), axis=0, keepdims=True)
    tall4 = lax.broadcasted_iota(jnp.int32, (4 * cx, cy), 0) % cx

    def restrict_points(first, second):
        h0, l0 = split(first)
        h1, l1 = split(second)
        left = jnp.concatenate([h0, h1, l0, l1], axis=0)
        left = jnp.concatenate([jnp.where(tall4 == r, left, jnp.zeros_like(left)) for r in range(cx)], axis=1)
        out = dot(left, hit[...], 1, 1)
        parts = [jnp.sum(out[i * cx:(i + 1) * cx] + out[(i + 2) * cx:(i + 3) * cx], axis=0, keepdims=True)
                 for i in range(2)]
        return jnp.concatenate(parts, axis=0)

    point_cross[...] = restrict_points(cross2, cross2)

    swap0.wait()
    puts = [put_to(misc, i, 1) for i in range(4)]
    for k in range(layers):
        puts += [put_to(visc, k, 1), put_to(spr, k, 1)]
    unpack(first_land, puts)

    ids_all = [misc[1, t].astype(jnp.int32) for t in both]
    ice = [misc[0, t] for t in both]
    for t in both:
        ice_ext[t] = ice[t]
        column.seen[1, 0, t, 0, pl.ds(TOP, tall), :] = ice[t]
    around = []
    ups = [turn(x, cy - 1) for x in ice]
    downs = [turn(x, 1) for x in ice]
    for t in both:
        around.append((column.seen[1, 0, t, 0, pl.ds(TOP + 1, tall), :],
                       column.seen[1, 0, t, 0, pl.ds(TOP - 1, tall), :],
                       jnp.where(long_lane == cy - 1, ups[1 - t], ups[t]),
                       jnp.where(long_lane == 0, downs[1 - t], downs[t])))
    for k in range(layers):
        for t in both:
            owned = spr[k, t]
            faces = 4.0 * owned
            if k + 1 < layers:
                face = 0.5 * (visc[k, t] + visc[k + 1, t]) * ice[t]
                fine.vert[k, t] = face
                faces = faces + face
            if k > 0:
                faces = faces + fine.vert[k - 1, t]
            if k == 0:
                faces = faces + misc[2, t]
            fine.diag[k, t] = ice[t] * faces + (1.0 - ice[t])
            fine.side[k, t] = owned * ice[t]
    for t in both:
        fine.cross[t] = misc[2, t] * misc[3, t] * ice[t]
    for finer, coarser in ((fine, middle), (middle, column)):
        size = finer.depth // coarser.depth
        for k in range(coarser.depth):
            group = range(k * size, (k + 1) * size)
            diag = sum(finer.diag[j] for j in group)
            inner_faces = sum(finer.vert[j] for j in list(group)[:-1])
            coarser.diag[k] = diag - 2.0 * inner_faces
            if k + 1 < coarser.depth:
                coarser.vert[k] = finer.vert[group[-1]]
            coarser.side[k] = sum(finer.side[j] for j in group)
        coarser.cross[...] = finer.cross[...]

    side2 = [column.side[0, 0, own] * around[0][d][HALO:HALO + cx] for d in range(4)]
    inner = (diag2 - jnp.where(row < cx - 1, side2[0], 0.0) - jnp.where(row > 0, side2[1], 0.0)
             - jnp.where(lane < cy - 1, side2[2], 0.0) - jnp.where(lane > 0, side2[3], 0.0))
    entries = (inner, cross2, jnp.where(row == cx - 1, side2[0], 0.0), jnp.where(row == 0, side2[1], 0.0),
               jnp.where(last_lane, side2[2], 0.0), jnp.where(first_lane, side2[3], 0.0))
    eight = lax.broadcasted_iota(jnp.int32, (8, cy), 0)
    tile = jnp.zeros((8, cy), F32)
    for i, entry in enumerate(entries):
        tile = jnp.where(eight == i, total(entry), tile)
    gathers[2][0][...] = tile
    tables_start, tables_wait = gather(2)
    tables_start()
    for level in (fine, middle, column):
        level.factor()

    tables = [near]
    for d, r, e in ((0, cx - 1, HALO + cx), (1, 0, HALO - 1)):
        other = ids_all[0][e:e + 1, :]
        term = jnp.where(other == down, side2[d][r:r + 1, :], 0.0)
        high, low = split(term)
        tables.append(-(dot(high, hit[:, spots[r]], 1, 1) + dot(low, hit[:, spots[r]], 1, 1)))
    for d, q, e in ((2, cy - 1, 0), (3, 0, cy - 1)):
        other = ids_all[1][HALO:HALO + cx, e:e + 1]
        term = jnp.where(other == lane, side2[d][:, q:q + 1], 0.0)
        here = jnp.where(ids[:, q:q + 1] == lane, 1.0, 0.0)
        high, low = split(term)
        here = here.astype(BF16)
        tables.append(-(dot(high, here, 0, 0) + dot(low, here, 0, 0)))
    for i, table in enumerate(tables):
        big[i * cy:(i + 1) * cy, 0:cy], big[i * cy:(i + 1) * cy, cy:2 * cy] = split(table)

    scale = POINT_WEIGHT / point_diag[...]
    ones = jnp.ones((8, 2 * cy), BF16)
    sixteen = lax.broadcasted_iota(jnp.int32, (16, cy), 0)
    sent = jnp.where(sixteen == 5, scale * point_cross[0:1, :], 0.0)
    for i, table in enumerate(tables):
        sent = jnp.where(sixteen == i, scale * jnp.sum(table, axis=0, keepdims=True), sent)
        part = big[i * cy:(i + 1) * cy]
        across_sum = dot(ones, part, 1, 1)[0:1, :]
        if i == 0:
            own_sum[...] = across_sum
        else:
            sent = jnp.where(sixteen == 5 + i, across_sum, sent)
    sent = jnp.where(sixteen == 10, scale, sent)
    near_out[0:16] = sent
    edge_rows = jnp.zeros((8, cy), F32)
    for i, (r, e) in enumerate(((cx - 1, HALO + cx), (0, HALO - 1))):
        for n, line in enumerate((misc[1, 0, HALO + r:HALO + r + 1], misc[1, 0, e:e + 1], side2[i][r:r + 1])):
            edge_rows = jnp.where(eight == 3 * i + n, line, edge_rows)
    near_out[16:24] = edge_rows
    edge_cols = jnp.zeros((cx, cy), F32)
    for i, (q, e) in enumerate(((cy - 1, 0), (0, cy - 1))):
        for n, line in enumerate((misc[1, 0, own, q:q + 1], misc[1, 1, own, e:e + 1], side2[2 + i][:, q:q + 1])):
            edge_cols = jnp.where(lane == 3 * i + n, line, edge_cols)
    near_out[24:24 + cx] = edge_cols
    near_out[24 + cx:24 + cx + cy] = near
    swap_near.start()

    def build_near():
        swap_near.wait()
        down_f, lane_f = down.astype(F32), lane.astype(F32)

        def step(m, carry):
            rows, cols = near_in[m, 16:24], near_in[m, 24:24 + cx]
            found = [near_in[m, 24 + cx:24 + cx + cy]]
            for i in range(2):
                there = jnp.where(rows[3 * i:3 * i + 1] == down_f, 1.0, 0.0).astype(BF16)
                high, low = split(jnp.where(rows[3 * i + 1:3 * i + 2] == down_f, rows[3 * i + 2:3 * i + 3], 0.0))
                found.append(-(dot(high, there, 1, 1) + dot(low, there, 1, 1)))
            for i in range(2):
                there = jnp.where(cols[:, 3 * i:3 * i + 1] == lane_f, 1.0, 0.0).astype(BF16)
                high, low = split(jnp.where(cols[:, 3 * i + 1:3 * i + 2] == lane_f, cols[:, 3 * i + 2:3 * i + 3], 0.0))
                found.append(-(dot(high, there, 0, 0) + dot(low, there, 0, 0)))
            for i, table in enumerate(found):
                big_near[m, i * cy:(i + 1) * cy, 0:cy], big_near[m, i * cy:(i + 1) * cy, cy:2 * cy] = split(table)
            return carry

        lax.fori_loop(0, 4, step, 0)

    block_row = lax.broadcasted_iota(jnp.int32, (count, cy), 0)
    shifts = (ny, count - ny, 1, count - 1)

    def coarse_begin(j, right, x):
        lines = [right - own_sum[...] * x - point_cross[...] * jnp.concatenate([x[1:2], x[0:1]], axis=0)]
        for d in range(4):
            lines.append(-near_in[BACK[d], 6 + BACK[d]:7 + BACK[d], :] * x)
        line = jnp.zeros((1, cy), F32)
        for i, part in enumerate(lines):
            sums = jnp.sum(part, axis=1, keepdims=True)
            for v in range(2):
                line = jnp.where(wide == 2 * i + v, sums[v:v + 1], line)
        gathers[0][0][0:2] = x
        gathers[0][0][2:3] = line
        start, wait = gather(0, lax.rem(j, 2))
        start()
        return wait

    def coarse_end(j, wait):
        @pl.when(j == 0)
        def _():
            tables_wait()
            for i in range(6):
                coarse_tab[i] = gathers[2][1][0, :, i, :]
            coarse_tab[6] = COARSE_WEIGHT / coarse_tab[0]
        wait()
        came = gathers[0][1][lax.rem(j, 2), :, 2, :]
        moved = [pltpu.roll(came, shifts[d], 0) for d in range(4)]
        right = []
        for v in range(2):
            part = came if v == 0 else pltpu.roll(came, cy - v, 1)
            for d in range(4):
                part = part + pltpu.roll(moved[d], cy - 2 - 2 * d - v, 1)
            right.append(part)
        diag, crossed, east, west, north, south, weight = (coarse_tab[i] for i in range(7))
        answer = [part * weight for part in right]
        for _ in range(CSWEEPS - 1):
            old = answer
            answer = []
            for v in range(2):
                applied = diag * old[v] + crossed * old[1 - v] - (
                    east * pltpu.roll(old[v], count - ny, 0) + west * pltpu.roll(old[v], ny, 0)
                    + north * pltpu.roll(old[v], count - 1, 0) + south * pltpu.roll(old[v], 1, 0))
                answer.append(old[v] + (right[v] - applied) * weight)
        hops = ((0, 0),) + STEPS[:4]
        known = {}

        def value(dx, dy):
            if (dx, dy) not in known:
                here = block_row == me + dx * ny + dy
                known[dx, dy] = jnp.concatenate(
                    [jnp.sum(jnp.where(here, part, 0.0), axis=0, keepdims=True)[:, 0:1] for part in answer], axis=0)
            return known[dx, dy]

        found = []
        for i, (dx, dy) in enumerate(hops):
            here = value(dx, dy)
            rows = near_out if i == 0 else near_in.at[BACK[i - 1]]
            out = here - rows[5:6, :] * jnp.concatenate([here[1:2], here[0:1]], axis=0)
            for n, (ex, ey) in enumerate(hops):
                out = out - rows[n:n + 1, :] * value(dx + ex, dy + ey)
            found.append(out)
        return found

    def build_lifts():
        for t in both:
            for out, source in ((lift_side, lambda k: middle.side[k, t]), (lift_cross, lambda k: middle.cross[t] if k == 0 else 0.0)):
                last = 0.0
                for k in range(half):
                    value = source(k)
                    if k > 0:
                        value = value + middle.vert[k - 1, t] * last
                    last = value * middle.inverse[k, t]
                    out[k, t] = last
                out[half - 1, t] = LINE_WEIGHT * last
                for k in reversed(range(half - 1)):
                    last = out[k, t] - middle.upper[k, t] * last
                    out[k, t] = LINE_WEIGHT * last

    def swapped(x):
        return jnp.concatenate([x[1:2], x[0:1]], axis=0)

    def apply_tables(table, xs):
        parts = [split(x) for x in xs]
        left = jnp.concatenate([jnp.concatenate([p[i] for p in parts], axis=1) for i in range(2)], axis=0)
        both_parts = dot(left, table[...], 1, 0)
        both_parts = both_parts[0:2] + both_parts[2:4]
        return both_parts[:, 0:cy] + both_parts[:, cy:2 * cy]

    def point_apply(xs):
        return point_cross[...] * swapped(xs[0]) + apply_tables(big, xs)

    def point_cycle(j, right, merge):
        x_out[0] = right * (POINT_WEIGHT / point_diag[...])
        swap = near_swap(0, 0)
        swap.start()
        packer = Packer(side_pack)
        for v in range(2):
            packer.add(column.field[1, 0, 0, v, own])
            packer.add(column.right[0, 0, v, own])
        for k in range(half):
            for v in range(2):
                packer.add(middle.field[1, k, 0, v, own])
        packer.finish()
        swap_side.start()
        pl.when(j == 0)(build_near)
        pl.when(j == 0)(build_lifts)
        scale = POINT_WEIGHT / point_diag[...]
        swap.wait()
        first = [right * scale] + [x_in[0, BACK[d]] for d in range(4)]
        x = first[0] + (right - point_apply(first)) * scale
        coarse_wait = coarse_begin(j, right, x)
        merge()
        found = coarse_end(j, coarse_wait)
        hops = ((0, 0),) + STEPS[:4]

        def second(dx, dy):
            return gathers[0][1][lax.rem(j, 2), lax.rem(me + dx * ny + dy + count, count), 0:2]

        xs = []
        for i, (dx, dy) in enumerate(hops):
            local = [second(dx + ex, dy + ey) for ex, ey in hops]
            if i == 0:
                moved = point_apply(local) * scale
            else:
                rows = near_in.at[BACK[i - 1]]
                moved = (rows[10:11] * apply_tables(big_near.at[BACK[i - 1]], local)
                         + rows[5:6] * swapped(local[0]))
            xs.append(local[0] + first[i] - moved + found[i])
        return xs[0] + (right - point_apply(xs)) * scale

    def mid_put(k, v):
        def put(value):
            middle.field[0, k, 1, v] = value
            middle.seen[0, k, 1, v, TOP:TOP + tall] = value * ice_ext[1]
        return put

    whole = pl.ds(0, tall)

    def merge_side(right0, right1):
        swap_side.wait()
        column.field[0, 0, 0] = jnp.concatenate([col_rows[0, 0], column.field[1, 0, 0, :, own], col_rows[1, 0]], axis=1)
        for e in range(2):
            column.right[0, 0, :, ends(e)] = col_rows[e, 1]
        for k in range(half):
            middle.put(0, k, 0, whole, jnp.concatenate(
                [mid_rows[0, k], middle.field[1, k, 0, :, own], mid_rows[1, k]], axis=1))
        puts = []
        for v in range(2):
            puts += [put_to(column.field, 0, 0, 1, v), put_to(column.right, 0, 1, v)]
        for k in range(half):
            puts += [mid_put(k, v) for v in range(2)]
        unpack(side_land, puts)
        middle.sweep(0, right1, spans=inside, plain=True)
        fine.sweep(1, right0, spans=inside, plain=True)

    def spread_points(x):
        far_out[...] = x
        swap_far.start()
        swap_far.wait()
        parts = [[], []]
        zones = ((pl.ds(0, HALO), 1, 6, 7), (own, None, 2, 3), (pl.ds(HALO + cx, HALO), 0, 4, 5))
        short = {n: lax.broadcasted_iota(jnp.int32, (n, cy), 1) < cy // 2 for n in (HALO, cx)}

        def take(src, v, index):
            values = x if src is None else far_in[BACK[src]]
            return jnp.take_along_axis(jnp.broadcast_to(values[v:v + 1], index.shape), index, axis=1,
                                       mode="promise_in_bounds")

        for rows, straight, right, left in zones:
            index = [misc[1, t, rows].astype(jnp.int32) for t in both]
            parts[0].append(jnp.stack([take(straight, v, index[0]) for v in range(2)]))
            lanes = short[index[1].shape[0]]
            parts[1].append(jnp.stack([jnp.where(lanes, take(right, v, index[1]), take(left, v, index[1]))
                                       for v in range(2)]))
        return [jnp.concatenate(p, axis=1) for p in parts]

    def iteration(j, carry):
        def right0(k, t, here):
            return basis[j, :, k, t, here]

        def right1(k, t, here):
            return middle.right[k, t, :, here]

        def right2(k, t, here):
            return column.right[k, t, :, here]

        def collect(coarser, size):
            held = {}

            def emit(k, t, here, value):
                held[t] = held[t] + value if k % size else value
                if k % size == size - 1:
                    coarser.right[k // size, t, :, here] = held[t]
            return emit

        for h, part in enumerate(swap_right(j)):
            part.wait()
            unpack(right_land.at[:, pl.ds(h * side_tiles, side_tiles)],
                   [put_to(basis, j, v, h * half + k, 1) for k in range(half) for v in range(2)], REACH)
        fine.before(right0)
        fine.leftover(1, right0, collect(middle, 2), spans=inside)
        middle.before(right1, inside)
        middle.leftover(1, right1, collect(column, half), spans=inside)
        column.before(right2, inside)
        kept = []
        column.leftover(1, right2, lambda k, t, here, value: kept.append(value), (0,), (own,))
        found = spread_points(point_cycle(j, restrict_points(kept[0][0], kept[0][1]),
                                          lambda: merge_side(right0, right1)))

        for t in both:
            column.put(0, 0, t, whole, found[t] + column.field[0, 0, t])
        column.sweep(0, right2)
        column.sweep(1, right2)
        for here in inside:
            outs = column.sums(0, 0, here, both)[1]
            for t in both:
                value = column.field[0, 0, t, :, here]
                part = (1.0 - LINE_WEIGHT) * value
                other = jnp.stack([value[1], value[0]])
                for k in range(half):
                    middle.put(0, k, t, here, (middle.field[1, k, t, :, here] + part)
                               + (lift_side[k, t, here][None] * outs[t] - lift_cross[k, t, here][None] * other))
        middle.sweep(0, right1, spans=inside)
        held = []

        def lifted(k, here):
            if k % 2 == 0:
                held[:] = middle.sums(1, k // 2, here, both)
            return fine.sideways(k, here, both, *held)

        def lift(k, t, here, value):
            fine.put(1, k, t, here, (fine.field[0, k, t, :, here] + value)
                     + (1.0 - LINE_WEIGHT) * middle.field[1, k // 2, t, :, here])

        fine.solve(lifted, lift, inside)
        fine.sweep(1, right0, spans=inside)

        packer = Packer(right_pack, REACH)
        parts = swap_right(j + 1)
        for k in range(layers):
            here = fine.field[0, k, 0, :, own]
            stored[j, :, k] = here
            out = fine.beside(0, k, own, (0,))[0] - fine.diag[k, 0, own][None] * here
            if k + 1 < layers:
                out = out + fine.vert[k, 0, own][None] * fine.field[0, k + 1, 0, :, own]
            if k > 0:
                out = out + fine.vert[k - 1, 0, own][None] * fine.field[0, k - 1, 0, :, own]
            value = basis[j, :, k, 0, own] + out
            basis[j + 1, :, k, 0, own] = value
            for v in range(2):
                packer.add(value[v])
            if k % half == half - 1:
                packer.finish()
                packer = Packer(right_pack.at[:, pl.ds(side_tiles, side_tiles)], REACH)
                pl.when(j < ITERS - 1)(parts[k // half].start)
        return carry

    lax.fori_loop(0, ITERS, iteration, 0)

    names = [(i, j) for i in range(ITERS + 1) for j in range(i, ITERS + 1)]
    sums = {name: jnp.zeros((cx, cy), F32) for name in names}
    for k in range(layers):
        chain = [basis[i, :, k, 0, own] for i in range(ITERS + 1)]
        terms = [chain[j] - chain[j + 1] for j in range(ITERS)] + [chain[0]]
        for i, j in names:
            prod = terms[i] * terms[j]
            sums[i, j] = sums[i, j] + prod[0] + prod[1]
    line = reduce_all([total(sums[name]) for name in names])
    gram = {name: pick(line, at) for at, name in enumerate(names)}
    rows = [[gram[min(i, j), max(i, j)] for j in range(ITERS + 1)] for i in range(ITERS)]
    for a in range(ITERS):
        for i in range(a + 1, ITERS):
            share = rows[i][a] / rows[a][a]
            for c in range(a, ITERS + 1):
                rows[i][c] = rows[i][c] - share * rows[a][c]
    weights = [None] * ITERS
    for a in reversed(range(ITERS)):
        part = rows[a][ITERS]
        for c in range(a + 1, ITERS):
            part = part - rows[a][c] * weights[c]
        weights[a] = part / rows[a][a]
    for k in range(layers):
        out = weights[0] * stored[0, :, k]
        rest = forcing[:, k] - weights[0] * (basis[0, :, k, 0, own] - basis[1, :, k, 0, own])
        for j in range(1, ITERS):
            out = out + weights[j] * stored[j, :, k]
            rest = rest - weights[j] * (basis[j, :, k, 0, own] - basis[j + 1, :, k, 0, own])
        for v in range(2):
            result[pl.ds((v * layers + k) * cx, cx)] = out[v]
            result[pl.ds((2 * layers + v * layers + k) * cx, cx)] = rest[v]


def solution(mesh):
    nx, ny = mesh.shape["gx"], mesh.shape["gy"]
    count = nx * ny

    def body(forcing, viscosity, spread, coupling, friction, mask, aggs):
        layers, cx, cy = forcing.shape[1:]
        dma = pltpu.SemaphoreType.DMA
        tall = cx + 2 * HALO
        half = layers // 2

        def vm(*shape, dtype=F32):
            return pltpu.VMEM(shape, dtype)

        def level(n):
            return (
                vm(2, n, 2, 2, tall + 2 * TOP, cy), vm(2, n, 2, 2, tall, cy),
                vm(n, 2, tall, cy), vm(n, 2, tall, cy), vm(n, 2, tall, cy), vm(2, tall, cy),
                vm(n, 2, tall, cy), vm(n, 2, tall, cy), vm(n, 2, 2, tall, cy), vm(n, 2, 2, tall, cy),
                vm(n, 2, 2, tall, cy),
            )

        def swap(planes, pieces, slots=cy // HALO):
            tiles = -(-planes // slots)
            return (vm(2, tiles, cx, cy), vm(2, tiles, tall, cy), dma((8, pieces)), dma((8, pieces)))

        def wide_swap(planes, slots):
            tiles = -(-planes // slots) * 2
            return (vm(2, tiles, cx, cy), vm(2, tiles, tall, cy), dma((2, 8, 1)), dma((2, 8, 1)))

        scratch = (
            (level(layers), level(half), level(1)),
            (vm(ITERS + 1, 2, layers, 2, tall, cy), vm(ITERS, 2, layers, cx, cy),
             vm(layers, 2, tall, cy), vm(layers, 2, tall, cy), vm(4, 2, tall, cy), vm(2, tall, cy)),
            (vm(cy, cx * cy, dtype=BF16), vm(5 * cy, 2 * cy, dtype=BF16),
             vm(1, cy), vm(2, cy), vm(1, cy)),
            (vm(2, 2, cy), vm(2, 4, 2, cy), dma((2, 4, 1)), dma((2, 4, 1))),
            tuple((vm(n, cy), vm(2, count, n, cy), dma(()), dma((2,))) for n in (3, 1, 8)),
            swap(4 + 2 * layers, 3),
            wide_swap(2 * half, (cy - REACH) // REACH // 2 * 2),
            swap(4 + 2 * half, 3),
            (vm(2, cy), vm(8, 2, cy), dma((8, 1)), dma((8, 1))),
            (vm(2, half, 2, HALO, cy), vm(2, 2, 2, HALO, cy)),
            (vm(24 + cx + cy, cy), vm(4, 24 + cx + cy, cy), vm(4, 5 * cy, 2 * cy, dtype=BF16), dma((4, 1)), dma((4, 1))),
            vm(7, count, cy), vm(half, 2, tall, cy), vm(half, 2, tall, cy),
        )
        flat, tree = jax.tree.flatten(scratch)

        def run(*refs):
            kernel(nx, ny, layers, cx, cy, *refs[:8], *jax.tree.unflatten(tree, refs[8:]))

        shape = jax.ShapeDtypeStruct((4 * layers * cx, cy), F32)
        whole = pl.BlockSpec(memory_space=pltpu.VMEM)
        outs = pl.pallas_call(
            run,
            out_shape=shape,
            in_specs=[whole] * 7,
            out_specs=whole,
            scratch_shapes=flat,
            compiler_params=pltpu.CompilerParams(has_side_effects=True, vmem_limit_bytes=60 * 1024 * 1024),
        )(forcing, viscosity, spread, coupling, friction, mask, aggs)
        return tuple(out.reshape(forcing.shape) for out in jnp.split(outs, 2))

    return jax.shard_map(
        body,
        mesh=mesh,
        in_specs=(
            P(None, None, "gx", "gy"),
            P(None, "gx", "gy"),
            P(None, "gx", "gy"),
            P("gx", "gy"),
            P("gx", "gy"),
            P("gx", "gy"),
            P("gx", "gy"),
        ),
        out_specs=(P(None, None, "gx", "gy"), P(None, None, "gx", "gy")),
        check_vma=False,
    )
```
